8 devices in a mesh: dp: 2 (over z, y), tp: 4 (over x, core).
Axes of the slice: x: 2, y: 2, z: 1, core: 2. Of those that a mesh axis runs over, the one named last changes fastest.
Arguments:
- x: bfloat16 [1024, 2048], P('dp'), parts along dimension 0
- k_cache: bfloat16 [1024, 32, 16, 128], P('dp', None, 'tp'), parts along dimension 0
- v_cache: bfloat16 [1024, 32, 16, 128], P('dp', None, 'tp'), parts along dimension 0
- positions: int32 [1024], P('dp'), parts along dimension 0
- att_ids: int32 [1024, 2], P('dp'), parts along dimension 0
- mlp_ids: int32 [1024, 2], P('dp'), parts along dimension 0
- norm_att: float32 [2048], replicated
- w_kv: bfloat16 [2048, 16, 256], P(None, 'tp')
- router_att: bfloat16 [2048, 8], replicated
- w_query: bfloat16 [8, 2048, 2048], P(None, None, 'tp')
- w_out: bfloat16 [8, 2048, 2048], P(None, 'tp')
- norm_mlp: float32 [2048], replicated
- router_mlp: bfloat16 [2048, 8], replicated
- w_gate: bfloat16 [8, 2048, 5632], P('tp')
- w_up: bfloat16 [8, 2048, 5632], P('tp')
- w_down: bfloat16 [8, 5632, 2048], P('tp')
Outputs:
- output 1: bfloat16 [1024, 2048], P('dp'), parts along dimension 0
- output 2: bfloat16 [1024, 32, 16, 128], P('dp', None, 'tp'), parts along dimension 0
- output 3: bfloat16 [1024, 32, 16, 128], P('dp', None, 'tp'), parts along dimension 0
There are 2 independent parts. The reference program is written for one: setup_inputs(seed, part) draws one part's arguments, and reference() takes and returns one part's arrays. A program takes and returns all parts, laid end to end along the dimension named above; an argument that names none is the same for every part.
All inputs are finite; a program needn't handle non-finite values.
Results may differ from the reference program's by a relative error of at most 0.012235.
Values are sent between devices in bfloat16 or wider.
A program may use at most 1 GiB of HBM per device.

```python
import jax
import jax.numpy as jnp
from jax import lax

HIDDEN = 2048
KV_HEADS = 16
HEAD_DIM = 128
ATT_EXPERTS = 8
MLP_EXPERTS = 8
FFN_WIDTH = 5632
TOKENS = 512
CACHE_LEN = 32

QUERY_WIDTH = KV_HEADS * HEAD_DIM
NORM_EPS = 1e-6
ROPE_BASE = 10000.0


def draw_pair(base_key, experts, skewed):
    key_first, key_offset, key_hot, key_share, key_coin = jax.random.split(base_key, 5)
    first_pick = jax.random.randint(key_first, (TOKENS,), 0, experts)
    if skewed:
        hot_id = jax.random.randint(key_hot, (), 0, experts)
        hot_share = jax.random.randint(key_share, (), 40, 61)
        coin_flip = jax.random.randint(key_coin, (TOKENS,), 0, 100)
        first_pick = jnp.where(coin_flip < hot_share, hot_id, first_pick)
    offset = jax.random.randint(key_offset, (TOKENS,), 1, experts)
    token_index = jnp.arange(TOKENS)
    forced = (token_index < experts) & (token_index != first_pick)
    second_pick = jnp.where(forced, token_index, (first_pick + offset) % experts)
    return jnp.stack([first_pick, second_pick], axis=1).astype(jnp.int32)


def draw_positions(base_key):
    positions = jax.random.randint(base_key, (TOKENS,), CACHE_LEN // 4, CACHE_LEN)
    return positions.at[0].set(CACHE_LEN - 1).at[1].set(CACHE_LEN // 4).astype(jnp.int32)


def setup_inputs(seed: int = 0, part: int = 0) -> dict:
    shared_keys = jax.random.split(jax.random.key(seed), 10)
    part_keys = jax.random.split(jax.random.fold_in(jax.random.key(seed + 1), part), 6)
    cache_shape = (TOKENS, CACHE_LEN, KV_HEADS, HEAD_DIM)
    x = jax.random.normal(part_keys[0], (TOKENS, HIDDEN), jnp.float32).astype(jnp.bfloat16)
    k_cache = jax.random.normal(part_keys[1], cache_shape, jnp.float32).astype(jnp.bfloat16)
    value_mean = jax.random.normal(part_keys[2], (TOKENS, 1, KV_HEADS, HEAD_DIM), jnp.float32)
    value_noise = jax.random.normal(part_keys[3], cache_shape, jnp.float32)
    v_cache = (0.8 * value_mean + 0.6 * value_noise).astype(jnp.bfloat16)
    positions = draw_positions(part_keys[4])
    choice_keys = jax.random.split(part_keys[5], 2)
    att_ids = draw_pair(choice_keys[0], ATT_EXPERTS, False)
    mlp_ids = draw_pair(choice_keys[1], MLP_EXPERTS, True)
    norm_att = 1.0 + 0.3 * jax.random.normal(shared_keys[0], (HIDDEN,), jnp.float32)
    w_kv = (jax.random.normal(shared_keys[1], (HIDDEN, KV_HEADS, 2 * HEAD_DIM), jnp.float32) * HIDDEN ** -0.5).astype(jnp.bfloat16)
    router_att = (jax.random.normal(shared_keys[2], (HIDDEN, ATT_EXPERTS), jnp.float32) * 0.5 * HIDDEN ** -0.5).astype(jnp.bfloat16)
    w_query = (jax.random.normal(shared_keys[3], (ATT_EXPERTS, HIDDEN, QUERY_WIDTH), jnp.float32) * HIDDEN ** -0.5).astype(jnp.bfloat16)
    w_out = (jax.random.normal(shared_keys[4], (ATT_EXPERTS, QUERY_WIDTH, HIDDEN), jnp.float32) * QUERY_WIDTH ** -0.5).astype(jnp.bfloat16)
    norm_mlp = 1.0 + 0.3 * jax.random.normal(shared_keys[5], (HIDDEN,), jnp.float32)
    router_mlp = (jax.random.normal(shared_keys[6], (HIDDEN, MLP_EXPERTS), jnp.float32) * 0.5 * HIDDEN ** -0.5).astype(jnp.bfloat16)
    w_gate = (jax.random.normal(shared_keys[7], (MLP_EXPERTS, HIDDEN, FFN_WIDTH), jnp.float32) * HIDDEN ** -0.5).astype(jnp.bfloat16)
    w_up = (jax.random.normal(shared_keys[8], (MLP_EXPERTS, HIDDEN, FFN_WIDTH), jnp.float32) * HIDDEN ** -0.5).astype(jnp.bfloat16)
    w_down = (jax.random.normal(shared_keys[9], (MLP_EXPERTS, FFN_WIDTH, HIDDEN), jnp.float32) * FFN_WIDTH ** -0.5).astype(jnp.bfloat16)
    return {'x': x, 'k_cache': k_cache, 'v_cache': v_cache, 'positions': positions, 'att_ids': att_ids, 'mlp_ids': mlp_ids, 'norm_att': norm_att, 'w_kv': w_kv, 'router_att': router_att, 'w_query': w_query, 'w_out': w_out, 'norm_mlp': norm_mlp, 'router_mlp': router_mlp, 'w_gate': w_gate, 'w_up': w_up, 'w_down': w_down}


def rms_norm(x, gain):
    values = x.astype(jnp.float32)
    inv_rms = lax.rsqrt(jnp.mean(values * values, axis=-1, keepdims=True) + NORM_EPS)
    return (values * inv_rms * gain).astype(jnp.bfloat16)


def rope_tables(positions):
    half_dim = HEAD_DIM // 2
    inv_freq = ROPE_BASE ** (-(jnp.arange(half_dim, dtype=jnp.float32) * 2.0 / HEAD_DIM))
    angles = positions.astype(jnp.float32)[:, None] * inv_freq[None, :]
    return jnp.cos(angles), jnp.sin(angles)


def apply_rope(vectors, cos_table, sin_table):
    half_dim = vectors.shape[-1] // 2
    first_half = vectors[..., :half_dim]
    second_half = vectors[..., half_dim:]
    return jnp.concatenate([first_half * cos_table - second_half * sin_table, second_half * cos_table + first_half * sin_table], axis=-1)


def reference(x, k_cache, v_cache, positions, att_ids, mlp_ids, norm_att, w_kv, router_att, w_query, w_out, norm_mlp, router_mlp, w_gate, w_up, w_down):
    hidden = rms_norm(x, norm_att)
    kv_new = jnp.dot(hidden, w_kv.reshape(HIDDEN, KV_HEADS * 2 * HEAD_DIM), preferred_element_type=jnp.float32).reshape(TOKENS, KV_HEADS, 2 * HEAD_DIM)
    cos_table, sin_table = rope_tables(positions)
    key_new = apply_rope(kv_new[:, :, :HEAD_DIM], cos_table[:, None, :], sin_table[:, None, :]).astype(jnp.bfloat16)
    value_new = kv_new[:, :, HEAD_DIM:].astype(jnp.bfloat16)
    slot_index = jnp.arange(CACHE_LEN)
    at_slot = (slot_index[None, :] == positions[:, None])[:, :, None, None]
    keys_all = jnp.where(at_slot, key_new[:, None, :, :], k_cache)
    values_all = jnp.where(at_slot, value_new[:, None, :, :], v_cache)
    att_logits = jnp.dot(hidden, router_att, preferred_element_type=jnp.float32)
    att_gates = jax.nn.softmax(jnp.take_along_axis(att_logits, att_ids, axis=1), axis=-1)
    query_all = jnp.einsum('bd,edc->bec', hidden.astype(jnp.float32), w_query.astype(jnp.float32))
    query_sel = jnp.take_along_axis(query_all, att_ids[:, :, None], axis=1).reshape(TOKENS, 2, KV_HEADS, HEAD_DIM)
    query_rot = apply_rope(query_sel, cos_table[:, None, None, :], sin_table[:, None, None, :]).astype(jnp.bfloat16)
    scores = jnp.einsum('bknd,bsnd->bkns', query_rot.astype(jnp.float32), keys_all.astype(jnp.float32)) * HEAD_DIM ** -0.5
    visible = (slot_index[None, :] <= positions[:, None])[:, None, None, :]
    weights = jax.nn.softmax(jnp.where(visible, scores, -1e30), axis=-1).astype(jnp.bfloat16)
    attended = jnp.einsum('bkns,bsnd->bknd', weights.astype(jnp.float32), values_all.astype(jnp.float32)).astype(jnp.bfloat16).reshape(TOKENS, 2, QUERY_WIDTH)
    att_onehot = (att_ids[:, :, None] == jnp.arange(ATT_EXPERTS)[None, None, :]).astype(jnp.float32)
    out_slots = jnp.einsum('bke,bkc->bec', att_onehot, attended.astype(jnp.float32))
    projected = jnp.einsum('bec,ecd->bed', out_slots, w_out.astype(jnp.float32))
    att_dense = jnp.einsum('bke,bk->be', att_onehot, att_gates)
    att_sum = jnp.einsum('be,bed->bd', att_dense, projected)
    x_mid = (x.astype(jnp.float32) + att_sum).astype(jnp.bfloat16)
    normed = rms_norm(x_mid, norm_mlp)
    mlp_logits = jnp.dot(normed, router_mlp, preferred_element_type=jnp.float32)
    mlp_gates = jax.nn.softmax(jnp.take_along_axis(mlp_logits, mlp_ids, axis=1), axis=-1)
    mlp_onehot = (mlp_ids[:, :, None] == jnp.arange(MLP_EXPERTS)[None, None, :]).astype(jnp.float32)
    mlp_dense = jnp.einsum('bke,bk->be', mlp_onehot, mlp_gates)

    def expert_step(running_sum, expert_inputs):
        gate_mat, up_mat, down_mat, weight_col = expert_inputs
        gate_val = jnp.dot(normed, gate_mat, preferred_element_type=jnp.float32)
        up_val = jnp.dot(normed, up_mat, preferred_element_type=jnp.float32)
        activation = (jax.nn.silu(gate_val) * up_val).astype(jnp.bfloat16)
        down_out = jnp.dot(activation, down_mat, preferred_element_type=jnp.float32)
        return running_sum + weight_col[:, None] * down_out, None

    mlp_sum, _ = lax.scan(expert_step, jnp.zeros((TOKENS, HIDDEN), jnp.float32), (w_gate, w_up, w_down, mlp_dense.T))
    x_out = (x_mid.astype(jnp.float32) + mlp_sum).astype(jnp.bfloat16)
    return x_out, keys_all, values_all
```

```python
import functools

import jax
import jax.numpy as jnp
from jax import lax
from jax.experimental import pallas as pl
from jax.experimental.pallas import tpu as pltpu
from jax.sharding import PartitionSpec as P

NORM_EPS = 1e-6
ROPE_BASE = 10000.0
F32 = jnp.float32
BF16 = jnp.bfloat16
NEG = -1e30
MESH = pl.DeviceIdType.MESH
VMEM_LIMIT = 62 * 1024 * 1024

TOKENS = 512
HIDDEN = 2048
HEADS = 4
HEAD_DIM = 128
SLOTS = 32
QUERY_COLS = HEADS * HEAD_DIM
EXPERTS = 8
FFN = 5632
LOCAL = 2

BLOCK = 32
RING = 8
BLOCKS = TOKENS // BLOCK
GROUP = 8
WQ_RING = 3

COL = 256
ROWS = 256
STEPS = HIDDEN // COL
CHUNKS = STEPS // 2 * (TOKENS // ROWS)

FT = 512
F_TILES = FFN // FT
MLP_STEPS = LOCAL * F_TILES
W_RING = 4
RB = 128


def dot(a, b):
    return jnp.dot(a, b, preferred_element_type=F32)


def iota(shape, dim):
    return lax.broadcasted_iota(jnp.int32, shape, dim)


def norm_rows(x_ref, gain_ref, out_ref):
    def body(i, carry):
        rows = pl.ds(pl.multiple_of(i * 32, 32), 32)
        values = x_ref[rows, :].astype(F32)
        inv = lax.rsqrt(jnp.mean(values * values, axis=-1, keepdims=True) + NORM_EPS)
        out_ref[rows, :] = (values * inv * gain_ref[...]).astype(BF16)
        return carry
    lax.fori_loop(0, TOKENS // 32, body, 0)


def pair_gates(logits, id0, id1):
    lane = iota(logits.shape, 1)
    first = jnp.sum(jnp.where(lane == id0, logits, 0.0), axis=1, keepdims=True)
    second = jnp.sum(jnp.where(lane == id1, logits, 0.0), axis=1, keepdims=True)
    top = jnp.maximum(first, second)
    e0 = jnp.exp(first - top)
    e1 = jnp.exp(second - top)
    total = e0 + e1
    return e0 / total, e1 / total


def attend_kernel(pos_ref, x_ref, gain_ref, cos_ref, sin_ref, ids_ref, router_ref, wkv_hbm, wq_hbm, kc_hbm, vc_hbm,
                  ko_hbm, vo_hbm, o_ref, gates_ref,
                  hid, wkv, wq, kbuf, vbuf, qsel, qrow, knew, vnew, orow,
                  wkv_sem, wq_sem, kin_sem, vin_sem, kout_sem, vout_sem):
    def block_of(ref, b):
        return ref.at[pl.ds(pl.multiple_of(b * BLOCK, BLOCK), BLOCK)]

    def load(b):
        slot = lax.rem(b, RING)
        return (pltpu.make_async_copy(block_of(kc_hbm, b), kbuf.at[slot], kin_sem.at[slot]),
                pltpu.make_async_copy(block_of(vc_hbm, b), vbuf.at[slot], vin_sem.at[slot]))

    def save(b):
        slot = lax.rem(b, RING)
        return (pltpu.make_async_copy(kbuf.at[slot], block_of(ko_hbm, b), kout_sem.at[slot]),
                pltpu.make_async_copy(vbuf.at[slot], block_of(vo_hbm, b), vout_sem.at[slot]))

    def load_wq(e):
        slot = lax.rem(e, WQ_RING)
        return pltpu.make_async_copy(wq_hbm.at[e], wq.at[slot], wq_sem.at[slot])

    kv_copy = pltpu.make_async_copy(wkv_hbm, wkv, wkv_sem)
    kv_copy.start()
    for e in range(WQ_RING):
        load_wq(jnp.int32(e)).start()
    for b in range(RING):
        for copy in load(jnp.int32(b)):
            copy.start()

    norm_rows(x_ref, gain_ref, hid)
    id0 = ids_ref[:, 0:1]
    id1 = ids_ref[:, 1:2]
    logits = dot(hid[...], router_ref[...])
    g0, g1 = pair_gates(logits, id0, id1)
    lane8 = iota((TOKENS, EXPERTS), 1)
    gates_ref[...] = jnp.where(lane8 == id0, g0, 0.0) + jnp.where(lane8 == id1, g1, 0.0)

    kv_copy.wait()

    def kv_body(m, carry):
        rows = pl.ds(pl.multiple_of(m * ROWS, ROWS), ROWS)
        kv = dot(hid[rows, :], wkv[...])
        cos = cos_ref[rows, :]
        sin = sin_ref[rows, :]
        for h in range(HEADS):
            k = kv[:, h * 256:h * 256 + 128]
            v = kv[:, h * 256 + 128:h * 256 + 256]
            k = k * cos + pltpu.roll(k, 64, 1) * sin
            knew[rows, h, :] = k
            knew[rows, h + 4, :] = k
            vnew[rows, h, :] = v
            vnew[rows, h + 4, :] = v
        return carry
    lax.fori_loop(0, TOKENS // ROWS, kv_body, 0)

    def q_body(e, carry):
        load_wq(e).wait()
        slot = lax.rem(e, WQ_RING)

        def m_body(m, c):
            rows = pl.ds(pl.multiple_of(m * ROWS, ROWS), ROWS)
            q = dot(hid[rows, :], wq[slot])
            for k in range(2):
                picked = ids_ref[rows, k:k + 1] == e
                qsel[k, rows, :] = jnp.where(picked, q, qsel[k, rows, :])
            return c
        lax.fori_loop(0, TOKENS // ROWS, m_body, 0)

        @pl.when(e + WQ_RING < EXPERTS)
        def _():
            load_wq(e + WQ_RING).start()
        return carry
    lax.fori_loop(0, EXPERTS, q_body, 0)

    def rope_body(m, carry):
        rows = pl.ds(pl.multiple_of(m * 128, 128), 128)
        cos = cos_ref[rows, :]
        sin = sin_ref[rows, :]
        for k in range(2):
            for h in range(HEADS):
                q = qsel[k, rows, h * 128:(h + 1) * 128]
                qrow[rows, k * HEADS + h, :] = q * cos + pltpu.roll(q, 64, 1) * sin
        return carry
    lax.fori_loop(0, TOKENS // 128, rope_body, 0)

    scale = HEAD_DIM ** -0.5
    sub16 = iota((16, HEAD_DIM), 0) >> 2
    row8 = iota((8, 128), 0)
    lane = iota((8, 128), 1)
    same_head = (lane & 3) == (row8 & 3)
    slot_of = lane >> 2

    def block_body(b, carry):
        slot = lax.rem(b, RING)
        for copy in load(b):
            copy.wait()

        def group_body(g, c):
            local = [g * GROUP + j for j in range(GROUP)]
            tokens = [b * BLOCK + t for t in local]
            places = [pos_ref[t] for t in tokens]
            for j in range(GROUP):
                rows = pl.ds(pl.multiple_of((places[j] >> 2) * 16, 16), 16)
                put = sub16 == (places[j] & 3)
                for new, buf in ((knew, kbuf), (vnew, vbuf)):
                    n8 = new[tokens[j]]
                    n16 = jnp.concatenate([n8, n8], axis=0)
                    old = buf[slot, local[j], rows, :].astype(F32)
                    buf[slot, local[j], rows, :] = jnp.where(put, n16, old).astype(BF16)
            probs = []
            for j in range(GROUP):
                q = qrow[tokens[j]].astype(BF16)
                s = lax.dot_general(q, kbuf[slot, local[j]], (((1,), (1,)), ((), ())), preferred_element_type=F32) * scale
                s = jnp.where(same_head & (slot_of <= places[j]), s, NEG)
                e = jnp.exp(s - jnp.max(s, axis=1, keepdims=True))
                probs.append((e / jnp.sum(e, axis=1, keepdims=True)).astype(BF16))
            for j in range(GROUP):
                orow[local[j]] = dot(probs[j], vbuf[slot, local[j]])
            return c
        lax.fori_loop(0, BLOCK // GROUP, group_body, 0)
        rows = pl.ds(pl.multiple_of(b * BLOCK, BLOCK), BLOCK)
        for r in range(8):
            o_ref[rows, r * 128:(r + 1) * 128] = orow[:, r, :].astype(BF16)
        for copy in save(b):
            copy.start()

        @pl.when(b >= 2)
        def _():
            for copy in save(b - 2):
                copy.wait()

            @pl.when(b - 2 + RING < BLOCKS)
            def _():
                for copy in load(b - 2 + RING):
                    copy.start()
        return carry
    lax.fori_loop(0, BLOCKS, block_body, 0)
    for b in (BLOCKS - 2, BLOCKS - 1):
        for copy in save(jnp.int32(b)):
            copy.wait()


def attend(positions, x, gain, cos, sin, ids, router, w_kv, w_query, k_cache, v_cache):
    any_spec = pl.BlockSpec(memory_space=pl.ANY)
    vmem = pl.BlockSpec(memory_space=pltpu.VMEM)
    smem = pl.BlockSpec(memory_space=pltpu.SMEM)
    cache = jax.ShapeDtypeStruct(k_cache.shape, BF16)
    return pl.pallas_call(
        attend_kernel,
        name='attend',
        out_shape=(cache, cache, jax.ShapeDtypeStruct((TOKENS, 2 * QUERY_COLS), BF16), jax.ShapeDtypeStruct((TOKENS, EXPERTS), F32)),
        in_specs=[smem] + [vmem] * 6 + [any_spec] * 4,
        out_specs=(any_spec, any_spec, vmem, vmem),
        scratch_shapes=[
            pltpu.VMEM((TOKENS, HIDDEN), BF16),
            pltpu.VMEM((HIDDEN, HEADS * 256), BF16),
            pltpu.VMEM((WQ_RING, HIDDEN, QUERY_COLS), BF16),
            pltpu.VMEM((RING, BLOCK, SLOTS * HEADS, HEAD_DIM), BF16),
            pltpu.VMEM((RING, BLOCK, SLOTS * HEADS, HEAD_DIM), BF16),
            pltpu.VMEM((2, TOKENS, QUERY_COLS), F32),
            pltpu.VMEM((TOKENS, 8, HEAD_DIM), F32),
            pltpu.VMEM((TOKENS, 8, HEAD_DIM), F32),
            pltpu.VMEM((TOKENS, 8, HEAD_DIM), F32),
            pltpu.VMEM((BLOCK, 8, HEAD_DIM), F32),
            pltpu.SemaphoreType.DMA,
            pltpu.SemaphoreType.DMA((WQ_RING,)),
            pltpu.SemaphoreType.DMA((RING,)),
            pltpu.SemaphoreType.DMA((RING,)),
            pltpu.SemaphoreType.DMA((RING,)),
            pltpu.SemaphoreType.DMA((RING,)),
        ],
        compiler_params=pltpu.CompilerParams(vmem_limit_bytes=VMEM_LIMIT),
    )(positions, x, gain, cos, sin, ids, router, w_kv, w_query, k_cache, v_cache)


def reduce_columns(load_step, wait_step, partial, base_ref, out_ref, send1, recv1, own, recv2, fin, recv3, s1, r1, s2, r2, s3, r3):
    me = lax.axis_index('tp')
    core = lax.rem(me, 2)
    sibling = me + 1 - 2 * core
    partner = lax.rem(me + 2, 4)
    barrier = pltpu.get_barrier_semaphore()
    for peer in (sibling, partner):
        pl.semaphore_signal(barrier, inc=1, device_id={'tp': peer}, device_id_type=MESH)
    pl.semaphore_wait(barrier, 2)

    def column(s):
        half = lax.rem(core + 1 + s, 2)
        return pl.multiple_of((half * (STEPS // 2) + lax.div(s, 2)) * COL, COL)

    def remote(src, dst, c, send, recv, peer):
        return pltpu.make_async_remote_copy(src_ref=src.at[c], dst_ref=dst.at[c], send_sem=send.at[c], recv_sem=recv.at[c],
                                            device_id={'tp': peer}, device_id_type=MESH)

    def to_sibling(c):
        return remote(send1, recv1, c, s1, r1, sibling)

    def to_partner(c):
        return remote(own, recv2, c, s2, r2, partner)

    def share(c):
        return remote(fin, recv3, c, s3, r3, sibling)

    def step_body(i, carry):
        for parity in range(2):
            s = 2 * i + parity
            wait_step(s, column(s))

            def row_body(m, c):
                rows = pl.ds(pl.multiple_of(m * ROWS, ROWS), ROWS)
                chunk = 2 * i + m
                acc = partial(s, rows)
                if parity == 0:
                    send1[chunk] = acc.astype(BF16)
                    to_sibling(chunk).start()
                else:
                    to_sibling(chunk).wait_recv()
                    own[chunk] = (acc + recv1[chunk].astype(F32)).astype(BF16)
                    to_partner(chunk).start()
                return c
            lax.fori_loop(0, TOKENS // ROWS, row_body, 0)
            load_step(s, column)
        return carry
    lax.fori_loop(0, STEPS // 2, step_body, 0)

    def place(c, half):
        rows = pl.ds(pl.multiple_of(lax.rem(c, 2) * ROWS, ROWS), ROWS)
        cols = pl.ds(pl.multiple_of((half * (STEPS // 2) + lax.div(c, 2)) * COL, COL), COL)
        return rows, cols

    def final_body(c, carry):
        to_partner(c).wait_recv()
        rows, cols = place(c, core)
        total = own[c].astype(F32) + recv2[c].astype(F32)
        value = (base_ref[rows, cols].astype(F32) + total).astype(BF16)
        fin[c] = value
        out_ref[rows, cols] = value
        share(c).start()
        return carry
    lax.fori_loop(0, CHUNKS, final_body, 0)

    def gather_body(c, carry):
        share(c).wait_recv()
        rows, cols = place(c, 1 - core)
        out_ref[rows, cols] = recv3[c]
        return carry
    lax.fori_loop(0, CHUNKS, gather_body, 0)

    def drain_body(c, carry):
        to_sibling(c).wait_send()
        to_partner(c).wait_send()
        share(c).wait_send()
        return carry
    lax.fori_loop(0, CHUNKS, drain_body, 0)


CHUNK_SCRATCH = [pltpu.VMEM((CHUNKS, ROWS, COL), BF16)] * 6 + [pltpu.SemaphoreType.DMA((CHUNKS,))] * 6
OUT_RING = 3


def out_kernel(o_ref, ids_ref, gates_ref, x_ref, w_hbm, out_ref, spread, wbuf, w_sem, *chunk_refs):
    me = lax.axis_index('tp')
    core = lax.rem(me, 2)

    def copy_of(s, col):
        slot = lax.rem(s, OUT_RING)
        return pltpu.make_async_copy(w_hbm.at[:, :, pl.ds(col, COL)], wbuf.at[slot], w_sem.at[slot])

    for s in range(OUT_RING):
        half = lax.rem(core + 1 + s, 2)
        copy_of(jnp.int32(s), pl.multiple_of((half * (STEPS // 2) + s // 2) * COL, COL)).start()

    def spread_body(m, carry):
        rows = pl.ds(pl.multiple_of(m * 128, 128), 128)
        first = o_ref[rows, :QUERY_COLS].astype(F32)
        second = o_ref[rows, QUERY_COLS:].astype(F32)
        for e in range(EXPERTS):
            picked = jnp.where(ids_ref[rows, 0:1] == e, first, 0.0)
            picked = jnp.where(ids_ref[rows, 1:2] == e, second, picked)
            spread[e, rows, :] = picked.astype(BF16)
        return carry
    lax.fori_loop(0, TOKENS // 128, spread_body, 0)

    def load_step(s, column):
        @pl.when(s + OUT_RING < STEPS)
        def _():
            copy_of(s + OUT_RING, column(s + OUT_RING)).start()

    def wait_step(s, col):
        copy_of(s, col).wait()

    def partial(s, rows):
        slot = lax.rem(s, OUT_RING)
        acc = jnp.zeros((ROWS, COL), F32)
        for e in range(EXPERTS):
            acc = acc + gates_ref[rows, e:e + 1] * dot(spread[e, rows, :], wbuf[slot, e])
        return acc

    reduce_columns(load_step, wait_step, partial, x_ref, out_ref, *chunk_refs)


def out_project(o, ids, gates, x, w_out):
    vmem = pl.BlockSpec(memory_space=pltpu.VMEM)
    return pl.pallas_call(
        out_kernel,
        name='out_project',
        out_shape=jax.ShapeDtypeStruct((TOKENS, HIDDEN), BF16),
        in_specs=[vmem] * 4 + [pl.BlockSpec(memory_space=pl.ANY)],
        out_specs=vmem,
        scratch_shapes=[
            pltpu.VMEM((EXPERTS, TOKENS, QUERY_COLS), BF16),
            pltpu.VMEM((OUT_RING, EXPERTS, QUERY_COLS, COL), BF16),
            pltpu.SemaphoreType.DMA((OUT_RING,)),
        ] + CHUNK_SCRATCH,
        compiler_params=pltpu.CompilerParams(vmem_limit_bytes=VMEM_LIMIT, collective_id=0, has_side_effects=True),
    )(o, ids, gates, x, w_out)


def gate_up_kernel(x_ref, gain_ref, router_ref, ids_ref, idst_ref, wg_hbm, wu_hbm, a_hbm, gates_ref,
                   unorm, picked, scatter, gathered, wg, wu, act, abuf, wg_sem, wu_sem, a_sem):
    first_id = lax.axis_index('tp') * LOCAL

    def load(s):
        e = lax.div(s, F_TILES)
        cols = pl.ds(pl.multiple_of(lax.rem(s, F_TILES) * FT, FT), FT)
        slot = lax.rem(s, W_RING)
        return (pltpu.make_async_copy(wg_hbm.at[e, :, cols], wg.at[slot], wg_sem.at[slot]),
                pltpu.make_async_copy(wu_hbm.at[e, :, cols], wu.at[slot], wu_sem.at[slot]))

    def save(s):
        e = lax.div(s, F_TILES)
        cols = pl.ds(pl.multiple_of(lax.rem(s, F_TILES) * FT, FT), FT)
        slot = lax.rem(s, 2)
        return pltpu.make_async_copy(abuf.at[slot], a_hbm.at[e, :, cols], a_sem.at[slot])

    for s in range(W_RING):
        for copy in load(jnp.int32(s)):
            copy.start()

    norm_rows(x_ref, gain_ref, unorm)
    id0 = ids_ref[:, 0:1]
    id1 = ids_ref[:, 1:2]
    logits = dot(unorm[...], router_ref[...])
    g0, g1 = pair_gates(logits, id0, id1)
    lane8 = iota((TOKENS, EXPERTS), 1)
    local8 = lane8 + first_id
    gates_ref[...] = jnp.where(local8 == id0, g0, 0.0) + jnp.where(local8 == id1, g1, 0.0)

    before = iota((TOKENS, TOKENS), 0)
    after = iota((TOKENS, TOKENS), 1)
    lower = jnp.where(after < before, 1.0, 0.0).astype(BF16)
    upper = jnp.where(before < after, 1.0, 0.0).astype(BF16)
    lane_id = iota((TOKENS, 128), 1) + first_id
    mask_col = jnp.where((lane_id == id0) | (lane_id == id1), 1.0, 0.0)
    rank_col = dot(lower, mask_col.astype(BF16))
    sub_id = iota((8, TOKENS), 0) + first_id
    mask_row = jnp.where((sub_id == idst_ref[0:1, :]) | (sub_id == idst_ref[1:2, :]), 1.0, 0.0)
    rank_row = dot(mask_row.astype(BF16), upper)
    counts = []
    for e in range(LOCAL):
        counts.append(jnp.sum(mask_row[e:e + 1, :]).astype(jnp.int32))
        where_col = jnp.where(mask_col[:, e:e + 1] > 0.0, rank_col[:, e:e + 1], -1.0)
        where_row = jnp.where(mask_row[e:e + 1, :] > 0.0, rank_row[e:e + 1, :], -1.0)
        scatter[e] = jnp.where(after.astype(F32) == where_col, 1.0, 0.0).astype(BF16)
        picked[e] = jnp.where(before.astype(F32) == where_row, 1.0, 0.0).astype(BF16)
    blocks = [lax.div(n + (RB - 1), RB) for n in counts]

    for e in range(LOCAL):
        def gather_body(rb, carry):
            rows = pl.ds(pl.multiple_of(rb * RB, RB), RB)
            gathered[e, rows, :] = dot(picked[e, rows, :], unorm[...]).astype(BF16)
            return carry
        lax.fori_loop(0, blocks[e], gather_body, 0)
    act[...] = jnp.zeros_like(act)

    def step_body(s, carry):
        e = lax.div(s, F_TILES)
        slot = lax.rem(s, W_RING)
        for copy in load(s):
            copy.wait()

        def row_body(rb, c):
            rows = pl.ds(pl.multiple_of(rb * RB, RB), RB)
            gate = dot(gathered[e, rows, :], wg[slot])
            up = dot(gathered[e, rows, :], wu[slot])
            act[rows, :] = (gate * (1.0 / (1.0 + jnp.exp(-gate))) * up).astype(BF16)
            return c
        lax.fori_loop(0, jnp.where(e == 0, blocks[0], blocks[1]), row_body, 0)

        @pl.when(s + W_RING < MLP_STEPS)
        def _():
            for copy in load(s + W_RING):
                copy.start()

        @pl.when(s >= 2)
        def _():
            save(s - 2).wait()
        out_slot = lax.rem(s, 2)

        def scatter_body(m, c):
            rows = pl.ds(pl.multiple_of(m * ROWS, ROWS), ROWS)
            abuf[out_slot, rows, :] = dot(scatter[e, rows, :], act[...]).astype(BF16)
            return c
        lax.fori_loop(0, TOKENS // ROWS, scatter_body, 0)
        save(s).start()
        return carry
    lax.fori_loop(0, MLP_STEPS, step_body, 0)
    for s in (MLP_STEPS - 2, MLP_STEPS - 1):
        save(jnp.int32(s)).wait()


def gate_up(x_mid, gain, router, ids, ids_t, w_gate, w_up):
    any_spec = pl.BlockSpec(memory_space=pl.ANY)
    vmem = pl.BlockSpec(memory_space=pltpu.VMEM)
    return pl.pallas_call(
        gate_up_kernel,
        name='gate_up',
        out_shape=(jax.ShapeDtypeStruct((LOCAL, TOKENS, FFN), BF16), jax.ShapeDtypeStruct((TOKENS, EXPERTS), F32)),
        in_specs=[vmem] * 5 + [any_spec] * 2,
        out_specs=(any_spec, vmem),
        scratch_shapes=[
            pltpu.VMEM((TOKENS, HIDDEN), BF16),
            pltpu.VMEM((LOCAL, TOKENS, TOKENS), BF16),
            pltpu.VMEM((LOCAL, TOKENS, TOKENS), BF16),
            pltpu.VMEM((LOCAL, TOKENS, HIDDEN), BF16),
            pltpu.VMEM((W_RING, HIDDEN, FT), BF16),
            pltpu.VMEM((W_RING, HIDDEN, FT), BF16),
            pltpu.VMEM((TOKENS, FT), BF16),
            pltpu.VMEM((2, TOKENS, FT), BF16),
            pltpu.SemaphoreType.DMA((W_RING,)),
            pltpu.SemaphoreType.DMA((W_RING,)),
            pltpu.SemaphoreType.DMA((2,)),
        ],
        compiler_params=pltpu.CompilerParams(vmem_limit_bytes=VMEM_LIMIT),
    )(x_mid, gain, router, ids, ids_t, w_gate, w_up)


DOWN_RING = 2


def down_kernel(gates_ref, x_ref, a_hbm, w_hbm, out_ref, abuf, wbuf, a_sem, w_sem, *chunk_refs):
    me = lax.axis_index('tp')
    core = lax.rem(me, 2)

    def copies(s, col):
        slot = lax.rem(s, DOWN_RING)
        return [pltpu.make_async_copy(w_hbm.at[e, :, pl.ds(col, COL)], wbuf.at[slot, e], w_sem.at[slot, e]) for e in range(LOCAL)]

    a_copies = [pltpu.make_async_copy(a_hbm.at[e], abuf.at[e], a_sem.at[e]) for e in range(LOCAL)]
    for copy in a_copies:
        copy.start()
    for s in range(DOWN_RING):
        half = lax.rem(core + 1 + s, 2)
        for copy in copies(jnp.int32(s), pl.multiple_of((half * (STEPS // 2) + s // 2) * COL, COL)):
            copy.start()
    for copy in a_copies:
        copy.wait()

    def load_step(s, column):
        @pl.when(s + DOWN_RING < STEPS)
        def _():
            for copy in copies(s + DOWN_RING, column(s + DOWN_RING)):
                copy.start()

    def wait_step(s, col):
        for copy in copies(s, col):
            copy.wait()

    def partial(s, rows):
        slot = lax.rem(s, DOWN_RING)
        acc = gates_ref[rows, 0:1] * dot(abuf[0, rows, :], wbuf[slot, 0])
        return acc + gates_ref[rows, 1:2] * dot(abuf[1, rows, :], wbuf[slot, 1])

    reduce_columns(load_step, wait_step, partial, x_ref, out_ref, *chunk_refs)


def down_project(gates, x_mid, act, w_down):
    vmem = pl.BlockSpec(memory_space=pltpu.VMEM)
    any_spec = pl.BlockSpec(memory_space=pl.ANY)
    return pl.pallas_call(
        down_kernel,
        name='down_project',
        out_shape=jax.ShapeDtypeStruct((TOKENS, HIDDEN), BF16),
        in_specs=[vmem] * 2 + [any_spec] * 2,
        out_specs=vmem,
        scratch_shapes=[
            pltpu.VMEM((LOCAL, TOKENS, FFN), BF16),
            pltpu.VMEM((DOWN_RING, LOCAL, FFN, COL), BF16),
            pltpu.SemaphoreType.DMA((LOCAL,)),
            pltpu.SemaphoreType.DMA((DOWN_RING, LOCAL)),
        ] + CHUNK_SCRATCH,
        compiler_params=pltpu.CompilerParams(vmem_limit_bytes=VMEM_LIMIT, collective_id=1, has_side_effects=True),
    )(gates, x_mid, act, w_down)


def rope_rows(positions):
    half = HEAD_DIM // 2
    inv_freq = ROPE_BASE ** (-(jnp.arange(half, dtype=F32) * 2.0 / HEAD_DIM))
    inv_freq = jnp.concatenate([inv_freq, inv_freq])
    sign = jnp.concatenate([-jnp.ones(half, F32), jnp.ones(half, F32)])
    angles = positions.astype(F32)[:, None] * inv_freq[None, :]
    return jnp.cos(angles), jnp.sin(angles) * sign


def solution(mesh):
    def local_step(x, k_cache, v_cache, positions, att_ids, mlp_ids, norm_att, w_kv, router_att, w_query, w_out, norm_mlp, router_mlp, w_gate, w_up, w_down):
        cos, sin = rope_rows(positions)
        flat = (TOKENS, SLOTS * HEADS, HEAD_DIM)
        k_new, v_new, o, att_gates = attend(
            positions, x, norm_att.reshape(1, HIDDEN), cos, sin, att_ids, router_att,
            w_kv.reshape(HIDDEN, HEADS * 256), w_query, k_cache.reshape(flat), v_cache.reshape(flat))
        x_mid = out_project(o, att_ids, att_gates, x, w_out)
        act, mlp_gates = gate_up(x_mid, norm_mlp.reshape(1, HIDDEN), router_mlp, mlp_ids, mlp_ids.T, w_gate, w_up)
        x_out = down_project(mlp_gates, x_mid, act, w_down)
        return x_out, k_new.reshape(k_cache.shape), v_new.reshape(v_cache.shape)

    token_spec = P('dp', None)
    cache_spec = P('dp', None, 'tp', None)
    expert_spec = P('tp', None, None)
    in_specs = (token_spec, cache_spec, cache_spec, P('dp'), token_spec, token_spec, P(), P(None, 'tp', None), P(), P(None, None, 'tp'), P(None, 'tp', None), P(), P(), expert_spec, expert_spec, expert_spec)
    out_specs = (token_spec, cache_spec, cache_spec)
    return jax.shard_map(local_step, mesh=mesh, in_specs=in_specs, out_specs=out_specs, check_vma=False)
```

```python
import functools

import jax
import jax.numpy as jnp
import numpy as np
from jax import lax
from jax.experimental import pallas as pl
from jax.experimental.pallas import tpu as pltpu
from jax.sharding import PartitionSpec as P

NORM_EPS = 1e-6
ROPE_BASE = 10000.0
F32 = jnp.float32
BF16 = jnp.bfloat16
NEG = -1e30
MESH = pl.DeviceIdType.MESH
VMEM_LIMIT = 62 * 1024 * 1024

TOKENS = 512
HIDDEN = 2048
HEADS = 4
HEAD_DIM = 128
SLOTS = 32
QUERY_COLS = HEADS * HEAD_DIM
EXPERTS = 8
FFN = 5632
LOCAL = 2

BLOCK = 32
RING = 8
BLOCKS = TOKENS // BLOCK
GROUP = 8
WQ_RING = 3

COL = 256
ROWS = 256
STEPS = HIDDEN // COL
CHUNKS = STEPS // 2 * (TOKENS // ROWS)

FT = 512
F_TILES = FFN // FT
MLP_STEPS = LOCAL * F_TILES
W_RING = 5
RB = 128


def dot(a, b):
    return jnp.dot(a, b, preferred_element_type=F32)


def iota(shape, dim):
    return lax.broadcasted_iota(jnp.int32, shape, dim)


def norm_rows(x_ref, gain_ref, out_ref):
    def body(i, carry):
        rows = pl.ds(pl.multiple_of(i * 32, 32), 32)
        values = x_ref[rows, :].astype(F32)
        inv = lax.rsqrt(jnp.mean(values * values, axis=-1, keepdims=True) + NORM_EPS)
        out_ref[rows, :] = (values * inv * gain_ref[...]).astype(BF16)
        return carry
    lax.fori_loop(0, TOKENS // 32, body, 0)


def pair_gates(logits, id0, id1):
    lane = iota(logits.shape, 1)
    first = jnp.sum(jnp.where(lane == id0, logits, 0.0), axis=1, keepdims=True)
    second = jnp.sum(jnp.where(lane == id1, logits, 0.0), axis=1, keepdims=True)
    top = jnp.maximum(first, second)
    e0 = jnp.exp(first - top)
    e1 = jnp.exp(second - top)
    total = e0 + e1
    return e0 / total, e1 / total


def turn(rows):
    sub = iota((8, TOKENS), 0)
    stacked = jnp.zeros((8, TOKENS), F32)
    for i, row in enumerate(rows):
        stacked = jnp.where(sub == i, row.astype(F32), stacked)
    return jnp.transpose(stacked).astype(jnp.int32)


def dot_nt(a, b):
    return lax.dot_general(a, b, (((1,), (1,)), ((), ())), preferred_element_type=F32)


def attend_kernel(pos_ref, x_ref, gain_ref, table_ref, posrow_ref, idst_ref, router_ref, wkv_hbm, wq_hbm, kc_hbm, vc_hbm,
                  ko_hbm, vo_hbm, o_ref, gates_ref, ids_ref,
                  hid, wraw, wtmp, wkv, wq, kbuf, vbuf, qsel, qrow, knv, orow, probs, cos_s, sin_s,
                  wkv_sem, wq_sem, kin_sem, vin_sem, kout_sem, vout_sem):
    def block_of(ref, b):
        return ref.at[pl.ds(pl.multiple_of(b * BLOCK, BLOCK), BLOCK)]

    def load(b):
        slot = lax.rem(b, RING)
        return (pltpu.make_async_copy(block_of(kc_hbm, b), kbuf.at[slot], kin_sem.at[slot]),
                pltpu.make_async_copy(block_of(vc_hbm, b), vbuf.at[slot], vin_sem.at[slot]))

    def save(b):
        slot = lax.rem(b, RING)
        return (pltpu.make_async_copy(kbuf.at[slot], block_of(ko_hbm, b), kout_sem.at[slot]),
                pltpu.make_async_copy(vbuf.at[slot], block_of(vo_hbm, b), vout_sem.at[slot]))

    def load_wq(e):
        slot = lax.rem(e, WQ_RING)
        return pltpu.make_async_copy(wq_hbm.at[e], wq.at[slot], wq_sem.at[slot])

    kv_copy = pltpu.make_async_copy(wkv_hbm, wraw, wkv_sem)
    kv_copy.start()
    for e in range(WQ_RING):
        load_wq(jnp.int32(e)).start()

    norm_rows(x_ref, gain_ref, hid)
    ids = turn((idst_ref[0:1, :], idst_ref[1:2, :], posrow_ref[...]))
    ids_ref[...] = ids
    id0 = ids[:, 0:1]
    id1 = ids[:, 1:2]
    lane128 = iota((TOKENS, 128), 1)
    chosen = ((lane128 & 31) == ids[:, 2:3]) & (lane128 < 3 * SLOTS)
    trig = dot(jnp.where(chosen, 1.0, 0.0).astype(BF16), table_ref[...])
    cos_s[...] = trig[:, :HEAD_DIM]
    sin_s[...] = trig[:, HEAD_DIM:]
    logits = dot_nt(hid[...], router_ref[...])
    g0, g1 = pair_gates(logits, id0, id1)
    lane8 = iota((TOKENS, EXPERTS), 1)
    gates_ref[...] = jnp.where(lane8 == id0, g0, 0.0) + jnp.where(lane8 == id1, g1, 0.0)

    kv_copy.wait()

    def sort_body(i, carry):
        raw = wraw[pl.ds(pl.multiple_of(i * 1024, 1024), 1024), :].astype(F32)
        wtmp[...] = raw.reshape(128, 8, 128)
        rows = pl.ds(pl.multiple_of(i * 128, 128), 128)
        for j in range(8):
            wkv[rows, j * 128:(j + 1) * 128] = wtmp[:, j, :].astype(BF16)
        return carry
    lax.fori_loop(0, HIDDEN // 128, sort_body, 0)

    def kv_body(m, carry):
        rows = pl.ds(pl.multiple_of(m * ROWS, ROWS), ROWS)
        kv = dot(hid[rows, :], wkv[...])
        cos = cos_s[rows, :]
        sin = sin_s[rows, :]
        for h in range(HEADS):
            k = kv[:, h * 128:(h + 1) * 128]
            knv[rows, h, :] = k * cos + pltpu.roll(k, 64, 1) * sin
            knv[rows, h + 4, :] = kv[:, (h + 4) * 128:(h + 5) * 128]
        return carry
    lax.fori_loop(0, TOKENS // ROWS, kv_body, 0)

    def q_body(e, carry):
        for copy in load(e):
            copy.start()
        load_wq(e).wait()
        slot = lax.rem(e, WQ_RING)

        def m_body(m, c):
            rows = pl.ds(pl.multiple_of(m * ROWS, ROWS), ROWS)
            q = dot(hid[rows, :], wq[slot])
            for k in range(2):
                picked = ids_ref[rows, k:k + 1] == e
                qsel[k, rows, :] = jnp.where(picked, q, qsel[k, rows, :])
            return c
        lax.fori_loop(0, TOKENS // ROWS, m_body, 0)

        @pl.when(e + WQ_RING < EXPERTS)
        def _():
            load_wq(e + WQ_RING).start()
        return carry
    lax.fori_loop(0, EXPERTS, q_body, 0)

    def rope_body(m, carry):
        rows = pl.ds(pl.multiple_of(m * 128, 128), 128)
        cos = cos_s[rows, :]
        sin = sin_s[rows, :]
        for k in range(2):
            for h in range(HEADS):
                q = qsel[k, rows, h * 128:(h + 1) * 128]
                qrow[rows, k * HEADS + h, :] = q * cos + pltpu.roll(q, 64, 1) * sin
        return carry
    lax.fori_loop(0, TOKENS // 128, rope_body, 0)

    scale = HEAD_DIM ** -0.5
    sub16 = iota((16, HEAD_DIM), 0) >> 2
    row8 = iota((8, 128), 0)
    lane = iota((8, 128), 1)
    low = row8 < 4
    same_head = (lane & 3) == (row8 & 3)
    slot_of = lane >> 2

    def block_body(i, carry):
        b = jnp.minimum(i, BLOCKS - 1)
        prev = jnp.maximum(i - 1, 0)
        slot = lax.rem(b, RING)
        prev_slot = lax.rem(prev, RING)
        side = lax.rem(i, 2)

        @pl.when(i < BLOCKS)
        def _():
            for copy in load(b):
                copy.wait()
        places = [pos_ref[b * BLOCK + t] for t in range(BLOCK)]

        def patch(t):
            rows = pl.ds(pl.multiple_of((places[t] >> 2) * 16, 16), 16)
            put = sub16 == (places[t] & 3)
            both = knv[b * BLOCK + t]
            swapped = pltpu.roll(both, 4, 0)
            for n8, buf in ((jnp.where(low, both, swapped), kbuf), (jnp.where(low, swapped, both), vbuf)):
                n16 = jnp.concatenate([n8, n8], axis=0)
                old = buf[slot, t, rows, :].astype(F32)
                buf[slot, t, rows, :] = jnp.where(put, n16, old).astype(BF16)

        def score(t):
            s = dot_nt(qrow[b * BLOCK + t].astype(BF16), kbuf[slot, t]) * scale
            s = jnp.where(same_head & (slot_of <= places[t]), s, NEG)
            e = jnp.exp(s - jnp.max(s, axis=1, keepdims=True))
            probs[side, t] = e / jnp.sum(e, axis=1, keepdims=True)

        def mix(t):
            orow[t] = dot(probs[1 - side, t].astype(BF16), vbuf[prev_slot, t])

        half = BLOCK // 2
        first, second = range(half), range(half, BLOCK)
        for t in first:
            patch(t)
        for t in first:
            score(t)
        for t in second:
            patch(t)
        for t in first:
            mix(t)
        for t in second:
            score(t)
        for t in second:
            mix(t)
        rows = pl.ds(pl.multiple_of(prev * BLOCK, BLOCK), BLOCK)
        for r in range(8):
            o_ref[rows, r * 128:(r + 1) * 128] = orow[:, r, :].astype(BF16)

        @pl.when(i >= 1)
        def _():
            for copy in save(prev):
                copy.start()

        @pl.when(i >= 3)
        def _():
            for copy in save(i - 3):
                copy.wait()

            @pl.when(i - 3 + RING < BLOCKS)
            def _():
                for copy in load(i - 3 + RING):
                    copy.start()
        return carry
    lax.fori_loop(0, BLOCKS + 1, block_body, 0)
    for b in (BLOCKS - 2, BLOCKS - 1):
        for copy in save(jnp.int32(b)):
            copy.wait()


def attend(positions, x, gain, table, pos_row, ids_t, router_t, w_kv, w_query, k_cache, v_cache):
    any_spec = pl.BlockSpec(memory_space=pl.ANY)
    vmem = pl.BlockSpec(memory_space=pltpu.VMEM)
    smem = pl.BlockSpec(memory_space=pltpu.SMEM)
    cache = jax.ShapeDtypeStruct(k_cache.shape, BF16)
    return pl.pallas_call(
        attend_kernel,
        name='attend',
        out_shape=(cache, cache, jax.ShapeDtypeStruct((TOKENS, 2 * QUERY_COLS), BF16),
                   jax.ShapeDtypeStruct((TOKENS, EXPERTS), F32), jax.ShapeDtypeStruct((TOKENS, EXPERTS), jnp.int32)),
        in_specs=[smem] + [vmem] * 6 + [any_spec] * 4,
        out_specs=(any_spec, any_spec, vmem, vmem, vmem),
        scratch_shapes=[
            pltpu.VMEM((TOKENS, HIDDEN), BF16),
            pltpu.VMEM((HIDDEN * 8, 128), BF16),
            pltpu.VMEM((128, 8, 128), F32),
            pltpu.VMEM((HIDDEN, HEADS * 256), BF16),
            pltpu.VMEM((WQ_RING, HIDDEN, QUERY_COLS), BF16),
            pltpu.VMEM((RING, BLOCK, SLOTS * HEADS, HEAD_DIM), BF16),
            pltpu.VMEM((RING, BLOCK, SLOTS * HEADS, HEAD_DIM), BF16),
            pltpu.VMEM((2, TOKENS, QUERY_COLS), F32),
            pltpu.VMEM((TOKENS, 8, HEAD_DIM), F32),
            pltpu.VMEM((TOKENS, 8, HEAD_DIM), F32),
            pltpu.VMEM((BLOCK, 8, HEAD_DIM), F32),
            pltpu.VMEM((2, BLOCK, 8, HEAD_DIM), F32),
            pltpu.VMEM((TOKENS, HEAD_DIM), F32),
            pltpu.VMEM((TOKENS, HEAD_DIM), F32),
            pltpu.SemaphoreType.DMA,
            pltpu.SemaphoreType.DMA((WQ_RING,)),
            pltpu.SemaphoreType.DMA((RING,)),
            pltpu.SemaphoreType.DMA((RING,)),
            pltpu.SemaphoreType.DMA((RING,)),
            pltpu.SemaphoreType.DMA((RING,)),
        ],
        compiler_params=pltpu.CompilerParams(vmem_limit_bytes=VMEM_LIMIT),
    )(positions, x, gain, table, pos_row, ids_t, router_t, w_kv, w_query, k_cache, v_cache)


def reduce_columns(load_step, wait_step, partial, base_hbm, out_ref, base_ref, base_sem, send1, recv1, own, recv2, fin, recv3, s1, r1, s2, r2, s3, r3):
    me = lax.axis_index('tp')
    core = lax.rem(me, 2)
    sibling = me + 1 - 2 * core
    partner = lax.rem(me + 2, 4)
    base_copy = pltpu.make_async_copy(base_hbm, base_ref, base_sem)
    base_copy.start()
    barrier = pltpu.get_barrier_semaphore()
    for peer in (sibling, partner):
        pl.semaphore_signal(barrier, inc=1, device_id={'tp': peer}, device_id_type=MESH)
    pl.semaphore_wait(barrier, 2)

    def column(s):
        half = lax.rem(core + 1 + s, 2)
        return pl.multiple_of((half * (STEPS // 2) + lax.div(s, 2)) * COL, COL)

    def remote(src, dst, c, send, recv, peer):
        return pltpu.make_async_remote_copy(src_ref=src.at[c], dst_ref=dst.at[c], send_sem=send.at[c], recv_sem=recv.at[c],
                                            device_id={'tp': peer}, device_id_type=MESH)

    def to_sibling(c):
        return remote(send1, recv1, c, s1, r1, sibling)

    def to_partner(c):
        return remote(own, recv2, c, s2, r2, partner)

    def share(c):
        return remote(fin, recv3, c, s3, r3, sibling)

    def step_body(i, carry):
        for parity in range(2):
            s = 2 * i + parity
            wait_step(s, column(s))

            def row_body(m, c):
                rows = pl.ds(pl.multiple_of(m * ROWS, ROWS), ROWS)
                chunk = 2 * i + m
                acc = partial(s, rows)
                if parity == 0:
                    send1[chunk] = acc.astype(BF16)
                    to_sibling(chunk).start()
                else:
                    to_sibling(chunk).wait_recv()
                    own[chunk] = (acc + recv1[chunk].astype(F32)).astype(BF16)
                    to_partner(chunk).start()
                return c
            lax.fori_loop(0, TOKENS // ROWS, row_body, 0)
            load_step(s, column)
        return carry
    lax.fori_loop(0, STEPS // 2, step_body, 0)
    base_copy.wait()

    def place(c, half):
        rows = pl.ds(pl.multiple_of(lax.rem(c, 2) * ROWS, ROWS), ROWS)
        cols = pl.ds(pl.multiple_of((half * (STEPS // 2) + lax.div(c, 2)) * COL, COL), COL)
        return rows, cols

    def final_body(c, carry):
        to_partner(c).wait_recv()
        rows, cols = place(c, core)
        total = own[c].astype(F32) + recv2[c].astype(F32)
        value = (base_ref[rows, cols].astype(F32) + total).astype(BF16)
        fin[c] = value
        out_ref[rows, cols] = value
        share(c).start()
        return carry
    lax.fori_loop(0, CHUNKS, final_body, 0)

    def gather_body(c, carry):
        share(c).wait_recv()
        rows, cols = place(c, 1 - core)
        out_ref[rows, cols] = recv3[c]
        return carry
    lax.fori_loop(0, CHUNKS, gather_body, 0)

    def drain_body(c, carry):
        to_sibling(c).wait_send()
        to_partner(c).wait_send()
        share(c).wait_send()
        return carry
    lax.fori_loop(0, CHUNKS, drain_body, 0)


CHUNK_SCRATCH = [pltpu.VMEM((TOKENS, HIDDEN), BF16), pltpu.SemaphoreType.DMA] + [pltpu.VMEM((CHUNKS, ROWS, COL), BF16)] * 6 + [pltpu.SemaphoreType.DMA((CHUNKS,))] * 6
OUT_RING = 3


def out_kernel(o_ref, ids_ref, gates_ref, x_ref, w_hbm, out_ref, spread, wbuf, w_sem, *chunk_refs):
    me = lax.axis_index('tp')
    core = lax.rem(me, 2)

    def copy_of(s, col):
        slot = lax.rem(s, OUT_RING)
        return pltpu.make_async_copy(w_hbm.at[:, :, pl.ds(col, COL)], wbuf.at[slot], w_sem.at[slot])

    for s in range(OUT_RING):
        half = lax.rem(core + 1 + s, 2)
        copy_of(jnp.int32(s), pl.multiple_of((half * (STEPS // 2) + s // 2) * COL, COL)).start()

    def spread_body(m, carry):
        rows = pl.ds(pl.multiple_of(m * 128, 128), 128)
        first = o_ref[rows, :QUERY_COLS].astype(F32)
        second = o_ref[rows, QUERY_COLS:].astype(F32)
        for e in range(EXPERTS):
            picked = jnp.where(ids_ref[rows, 0:1] == e, first, 0.0)
            picked = jnp.where(ids_ref[rows, 1:2] == e, second, picked)
            spread[e, rows, :] = picked.astype(BF16)
        return carry
    lax.fori_loop(0, TOKENS // 128, spread_body, 0)

    def load_step(s, column):
        @pl.when(s + OUT_RING < STEPS)
        def _():
            copy_of(s + OUT_RING, column(s + OUT_RING)).start()

    def wait_step(s, col):
        copy_of(s, col).wait()

    def partial(s, rows):
        slot = lax.rem(s, OUT_RING)
        acc = jnp.zeros((ROWS, COL), F32)
        for e in range(EXPERTS):
            acc = acc + gates_ref[rows, e:e + 1] * dot(spread[e, rows, :], wbuf[slot, e])
        return acc

    reduce_columns(load_step, wait_step, partial, x_ref, out_ref, *chunk_refs)


def out_project(o, ids, gates, x, w_out):
    vmem = pl.BlockSpec(memory_space=pltpu.VMEM)
    return pl.pallas_call(
        out_kernel,
        name='out_project',
        out_shape=jax.ShapeDtypeStruct((TOKENS, HIDDEN), BF16),
        in_specs=[vmem] * 3 + [pl.BlockSpec(memory_space=pl.ANY)] * 2,
        out_specs=vmem,
        scratch_shapes=[
            pltpu.VMEM((EXPERTS, TOKENS, QUERY_COLS), BF16),
            pltpu.VMEM((OUT_RING, EXPERTS, QUERY_COLS, COL), BF16),
            pltpu.SemaphoreType.DMA((OUT_RING,)),
        ] + CHUNK_SCRATCH,
        compiler_params=pltpu.CompilerParams(vmem_limit_bytes=VMEM_LIMIT, collective_id=0, has_side_effects=True),
    )(o, ids, gates, x, w_out)


def gate_up_kernel(x_ref, gain_ref, router_ref, idst_ref, wg_hbm, wu_hbm, a_hbm, gates_ref,
                   unorm, picked, scatter, gathered, wg, wu, act, abuf, wg_sem, wu_sem, a_sem):
    first_id = lax.axis_index('tp') * LOCAL

    def load(s):
        e = lax.div(s, F_TILES)
        cols = pl.ds(pl.multiple_of(lax.rem(s, F_TILES) * FT, FT), FT)
        slot = lax.rem(s, W_RING)
        return (pltpu.make_async_copy(wg_hbm.at[e, :, cols], wg.at[slot], wg_sem.at[slot]),
                pltpu.make_async_copy(wu_hbm.at[e, :, cols], wu.at[slot], wu_sem.at[slot]))

    def save(s):
        e = lax.div(s, F_TILES)
        cols = pl.ds(pl.multiple_of(lax.rem(s, F_TILES) * FT, FT), FT)
        slot = lax.rem(s, 2)
        return pltpu.make_async_copy(abuf.at[slot], a_hbm.at[e, :, cols], a_sem.at[slot])

    for s in range(W_RING):
        for copy in load(jnp.int32(s)):
            copy.start()

    norm_rows(x_ref, gain_ref, unorm)
    ids = turn((idst_ref[0:1, :], idst_ref[1:2, :]))
    id0 = ids[:, 0:1]
    id1 = ids[:, 1:2]
    logits = dot_nt(unorm[...], router_ref[...])
    g0, g1 = pair_gates(logits, id0, id1)
    lane8 = iota((TOKENS, EXPERTS), 1)
    local8 = lane8 + first_id
    gates_ref[...] = jnp.where(local8 == id0, g0, 0.0) + jnp.where(local8 == id1, g1, 0.0)

    before = iota((TOKENS, TOKENS), 0)
    after = iota((TOKENS, TOKENS), 1)
    lower = jnp.where(after < before, 1.0, 0.0).astype(BF16)
    upper = jnp.where(before < after, 1.0, 0.0).astype(BF16)
    lane_id = iota((TOKENS, 128), 1) + first_id
    mask_col = jnp.where((lane_id == id0) | (lane_id == id1), 1.0, 0.0)
    rank_col = dot(lower, mask_col.astype(BF16))
    sub_id = iota((8, TOKENS), 0) + first_id
    mask_row = jnp.where((sub_id == idst_ref[0:1, :]) | (sub_id == idst_ref[1:2, :]), 1.0, 0.0)
    rank_row = dot(mask_row.astype(BF16), upper)
    counts = []
    for e in range(LOCAL):
        counts.append(jnp.sum(mask_row[e:e + 1, :]).astype(jnp.int32))
        where_col = jnp.where(mask_col[:, e:e + 1] > 0.0, rank_col[:, e:e + 1], -1.0)
        where_row = jnp.where(mask_row[e:e + 1, :] > 0.0, rank_row[e:e + 1, :], -1.0)
        scatter[e] = jnp.where(after.astype(F32) == where_col, 1.0, 0.0).astype(BF16)
        picked[e] = jnp.where(before.astype(F32) == where_row, 1.0, 0.0).astype(BF16)
    blocks = [lax.div(n + (RB - 1), RB) for n in counts]

    for e in range(LOCAL):
        def gather_body(rb, carry):
            rows = pl.ds(pl.multiple_of(rb * RB, RB), RB)
            gathered[e, rows, :] = dot(picked[e, rows, :], unorm[...]).astype(BF16)
            return carry
        lax.fori_loop(0, blocks[e], gather_body, 0)

    def step_body(s, carry):
        e = lax.div(s, F_TILES)
        slot = lax.rem(s, W_RING)
        out_slot = lax.rem(s, 2)
        for copy in load(s):
            copy.wait()

        @pl.when(s >= 2)
        def _():
            save(s - 2).wait()

        def run(count):
            for n in range(FT // COL):
                cols = slice(n * COL, (n + 1) * COL)
                gate = dot(gathered[e, :count, :], wg[slot, :, cols])
                up = dot(gathered[e, :count, :], wu[slot, :, cols])
                act[:count, cols] = (gate * (1.0 / (1.0 + jnp.exp(-gate))) * up).astype(BF16)
            for m in range(TOKENS // ROWS):
                rows = slice(m * ROWS, (m + 1) * ROWS)
                abuf[out_slot, rows, :] = dot(scatter[e, rows, :count], act[:count, :]).astype(BF16)

        n_blocks = jnp.where(e == 0, blocks[0], blocks[1])
        for k in range(1, TOKENS // RB + 1):
            pl.when(n_blocks == k)(functools.partial(run, k * RB))

        @pl.when(s + W_RING < MLP_STEPS)
        def _():
            for copy in load(s + W_RING):
                copy.start()
        save(s).start()
        return carry
    lax.fori_loop(0, MLP_STEPS, step_body, 0)
    for s in (MLP_STEPS - 2, MLP_STEPS - 1):
        save(jnp.int32(s)).wait()


def gate_up(x_mid, gain, router_t, ids_t, w_gate, w_up):
    any_spec = pl.BlockSpec(memory_space=pl.ANY)
    vmem = pl.BlockSpec(memory_space=pltpu.VMEM)
    return pl.pallas_call(
        gate_up_kernel,
        name='gate_up',
        out_shape=(jax.ShapeDtypeStruct((LOCAL, TOKENS, FFN), BF16), jax.ShapeDtypeStruct((TOKENS, EXPERTS), F32)),
        in_specs=[vmem] * 4 + [any_spec] * 2,
        out_specs=(any_spec, vmem),
        scratch_shapes=[
            pltpu.VMEM((TOKENS, HIDDEN), BF16),
            pltpu.VMEM((LOCAL, TOKENS, TOKENS), BF16),
            pltpu.VMEM((LOCAL, TOKENS, TOKENS), BF16),
            pltpu.VMEM((LOCAL, TOKENS, HIDDEN), BF16),
            pltpu.VMEM((W_RING, HIDDEN, FT), BF16),
            pltpu.VMEM((W_RING, HIDDEN, FT), BF16),
            pltpu.VMEM((TOKENS, FT), BF16),
            pltpu.VMEM((2, TOKENS, FT), BF16),
            pltpu.SemaphoreType.DMA((W_RING,)),
            pltpu.SemaphoreType.DMA((W_RING,)),
            pltpu.SemaphoreType.DMA((2,)),
        ],
        compiler_params=pltpu.CompilerParams(vmem_limit_bytes=VMEM_LIMIT),
    )(x_mid, gain, router_t, ids_t, w_gate, w_up)


DOWN_RING = 2


def down_kernel(gates_ref, x_ref, a_hbm, w_hbm, out_ref, abuf, wbuf, a_sem, w_sem, *chunk_refs):
    me = lax.axis_index('tp')
    core = lax.rem(me, 2)

    def copies(s, col):
        slot = lax.rem(s, DOWN_RING)
        return [pltpu.make_async_copy(w_hbm.at[e, :, pl.ds(col, COL)], wbuf.at[slot, e], w_sem.at[slot, e]) for e in range(LOCAL)]

    a_copies = [pltpu.make_async_copy(a_hbm.at[e], abuf.at[e], a_sem.at[e]) for e in range(LOCAL)]
    for copy in a_copies:
        copy.start()
    for s in range(DOWN_RING):
        half = lax.rem(core + 1 + s, 2)
        for copy in copies(jnp.int32(s), pl.multiple_of((half * (STEPS // 2) + s // 2) * COL, COL)):
            copy.start()
    for copy in a_copies:
        copy.wait()

    def load_step(s, column):
        @pl.when(s + DOWN_RING < STEPS)
        def _():
            for copy in copies(s + DOWN_RING, column(s + DOWN_RING)):
                copy.start()

    def wait_step(s, col):
        for copy in copies(s, col):
            copy.wait()

    def partial(s, rows):
        slot = lax.rem(s, DOWN_RING)
        acc = gates_ref[rows, 0:1] * dot(abuf[0, rows, :], wbuf[slot, 0])
        return acc + gates_ref[rows, 1:2] * dot(abuf[1, rows, :], wbuf[slot, 1])

    reduce_columns(load_step, wait_step, partial, x_ref, out_ref, *chunk_refs)


def down_project(gates, x_mid, act, w_down):
    vmem = pl.BlockSpec(memory_space=pltpu.VMEM)
    any_spec = pl.BlockSpec(memory_space=pl.ANY)
    return pl.pallas_call(
        down_kernel,
        name='down_project',
        out_shape=jax.ShapeDtypeStruct((TOKENS, HIDDEN), BF16),
        in_specs=[vmem] + [any_spec] * 3,
        out_specs=vmem,
        scratch_shapes=[
            pltpu.VMEM((LOCAL, TOKENS, FFN), BF16),
            pltpu.VMEM((DOWN_RING, LOCAL, FFN, COL), BF16),
            pltpu.SemaphoreType.DMA((LOCAL,)),
            pltpu.SemaphoreType.DMA((DOWN_RING, LOCAL)),
        ] + CHUNK_SCRATCH,
        compiler_params=pltpu.CompilerParams(vmem_limit_bytes=VMEM_LIMIT, collective_id=1, has_side_effects=True),
    )(gates, x_mid, act, w_down)


def rope_table():
    half = HEAD_DIM // 2
    inv_freq = np.float32(ROPE_BASE) ** (-(np.arange(half, dtype=np.float32) * np.float32(2.0) / np.float32(HEAD_DIM)))
    angles = np.arange(SLOTS, dtype=np.float32)[:, None] * inv_freq[None, :].astype(np.float32)
    cos = np.cos(angles.astype(np.float64))
    sin = np.sin(angles.astype(np.float64))
    full = np.concatenate([cos, cos, -sin, sin], axis=1).astype(np.float32)
    parts = []
    for _ in range(3):
        part = full.astype(BF16)
        parts.append(part)
        full = full - part.astype(np.float32)
    parts.append(np.zeros_like(parts[0]))
    return np.concatenate(parts, axis=0)


def solution(mesh):
    table = rope_table()

    def local_step(x, k_cache, v_cache, positions, att_ids, mlp_ids, norm_att, w_kv, router_att, w_query, w_out, norm_mlp, router_mlp, w_gate, w_up, w_down):
        flat = (TOKENS, SLOTS * HEADS, HEAD_DIM)
        kv_rows = w_kv.reshape(HIDDEN, HEADS, 2, HEAD_DIM).transpose(0, 2, 1, 3).reshape(HIDDEN * 8, HEAD_DIM)
        k_new, v_new, o, att_gates, att_cols = attend(
            positions, x, norm_att.reshape(1, HIDDEN), jnp.asarray(table), positions.reshape(1, TOKENS), att_ids.T, router_att.T,
            kv_rows, w_query, k_cache.reshape(flat), v_cache.reshape(flat))
        x_mid = out_project(o, att_cols, att_gates, x, w_out)
        act, mlp_gates = gate_up(x_mid, norm_mlp.reshape(1, HIDDEN), router_mlp.T, mlp_ids.T, w_gate, w_up)
        x_out = down_project(mlp_gates, x_mid, act, w_down)
        return x_out, k_new.reshape(k_cache.shape), v_new.reshape(v_cache.shape)

    token_spec = P('dp', None)
    cache_spec = P('dp', None, 'tp', None)
    expert_spec = P('tp', None, None)
    in_specs = (token_spec, cache_spec, cache_spec, P('dp'), token_spec, token_spec, P(), P(None, 'tp', None), P(), P(None, None, 'tp'), P(None, 'tp', None), P(), P(), expert_spec, expert_spec, expert_spec)
    out_specs = (token_spec, cache_spec, cache_spec)
    return jax.shard_map(local_step, mesh=mesh, in_specs=in_specs, out_specs=out_specs, check_vma=False)
```

```python
import functools

import jax
import jax.numpy as jnp
import numpy as np
from jax import lax
from jax.experimental import pallas as pl
from jax.experimental.pallas import tpu as pltpu
from jax.sharding import PartitionSpec as P

NORM_EPS = 1e-6
ROPE_BASE = 10000.0
F32 = jnp.float32
BF16 = jnp.bfloat16
NEG = -1e30
MESH = pl.DeviceIdType.MESH
VMEM_LIMIT = 62 * 1024 * 1024

TOKENS = 512
HIDDEN = 2048
HEADS = 4
HEAD_DIM = 128
SLOTS = 32
QUERY_COLS = HEADS * HEAD_DIM
EXPERTS = 8
FFN = 5632
LOCAL = 2

BLOCK = 32
RING = 8
BLOCKS = TOKENS // BLOCK
GROUP = 8
WQ_RING = 3

COL = 256
ROWS = 256
STEPS = HIDDEN // COL
CHUNKS = STEPS // 2 * (TOKENS // ROWS)

FT = 512
F_TILES = FFN // FT
MLP_STEPS = LOCAL * F_TILES
W_RING = 5
RB = 128


def dot(a, b):
    return jnp.dot(a, b, preferred_element_type=F32)


def iota(shape, dim):
    return lax.broadcasted_iota(jnp.int32, shape, dim)


def norm_rows(x_ref, gain_ref, out_ref):
    def body(i, carry):
        rows = pl.ds(pl.multiple_of(i * 32, 32), 32)
        values = x_ref[rows, :].astype(F32)
        inv = lax.rsqrt(jnp.mean(values * values, axis=-1, keepdims=True) + NORM_EPS)
        out_ref[rows, :] = (values * inv * gain_ref[...]).astype(BF16)
        return carry
    lax.fori_loop(0, TOKENS // 32, body, 0)


def pair_gates(logits, id0, id1):
    lane = iota(logits.shape, 1)
    first = jnp.sum(jnp.where(lane == id0, logits, 0.0), axis=1, keepdims=True)
    second = jnp.sum(jnp.where(lane == id1, logits, 0.0), axis=1, keepdims=True)
    top = jnp.maximum(first, second)
    e0 = jnp.exp(first - top)
    e1 = jnp.exp(second - top)
    total = e0 + e1
    return e0 / total, e1 / total


def turn(rows):
    sub = iota((8, TOKENS), 0)
    stacked = jnp.zeros((8, TOKENS), F32)
    for i, row in enumerate(rows):
        stacked = jnp.where(sub == i, row.astype(F32), stacked)
    return jnp.transpose(stacked).astype(jnp.int32)


def dot_nt(a, b):
    return lax.dot_general(a, b, (((1,), (1,)), ((), ())), preferred_element_type=F32)


def project_kernel(pos_ref, x_ref, gain_ref, table_ref, posrow_ref, idst_ref, router_ref, wkv_hbm, wq_hbm, kc_hbm, vc_hbm,
                   ko_hbm, vo_hbm, qrow, gates_ref, ids_ref,
                   hid, wraw, wtmp, wkv, wq, kbuf, vbuf, qsel, knv, cos_s, sin_s,
                   wkv_sem, wq_sem, kin_sem, vin_sem, kout_sem, vout_sem):
    def block_of(ref, b):
        return ref.at[pl.ds(pl.multiple_of(b * BLOCK, BLOCK), BLOCK)]

    def load(b):
        slot = lax.rem(b, RING)
        return (pltpu.make_async_copy(block_of(kc_hbm, b), kbuf.at[slot], kin_sem.at[slot]),
                pltpu.make_async_copy(block_of(vc_hbm, b), vbuf.at[slot], vin_sem.at[slot]))

    def save(b):
        slot = lax.rem(b, RING)
        return (pltpu.make_async_copy(kbuf.at[slot], block_of(ko_hbm, b), kout_sem.at[slot]),
                pltpu.make_async_copy(vbuf.at[slot], block_of(vo_hbm, b), vout_sem.at[slot]))

    def load_wq(e):
        slot = lax.rem(e, WQ_RING)
        return pltpu.make_async_copy(wq_hbm.at[e], wq.at[slot], wq_sem.at[slot])

    kv_copy = pltpu.make_async_copy(wkv_hbm, wraw, wkv_sem)
    kv_copy.start()
    for e in range(WQ_RING):
        load_wq(jnp.int32(e)).start()

    norm_rows(x_ref, gain_ref, hid)
    ids = turn((idst_ref[0:1, :], idst_ref[1:2, :], posrow_ref[...]))
    ids_ref[...] = ids
    id0 = ids[:, 0:1]
    id1 = ids[:, 1:2]
    lane128 = iota((TOKENS, 128), 1)
    chosen = ((lane128 & 31) == ids[:, 2:3]) & (lane128 < 3 * SLOTS)
    trig = dot(jnp.where(chosen, 1.0, 0.0).astype(BF16), table_ref[...])
    cos_s[...] = trig[:, :HEAD_DIM]
    sin_s[...] = trig[:, HEAD_DIM:]
    for b in range(RING):
        for copy in load(jnp.int32(b)):
            copy.start()
    kv_copy.wait()

    def sort_body(i, carry):
        wtmp[...] = wraw[pl.ds(pl.multiple_of(i * 1024, 1024), 1024), :].astype(F32)
        rows = pl.ds(pl.multiple_of(i * 128, 128), 128)
        for j in range(8):
            wkv[rows, j * 128:(j + 1) * 128] = wtmp[pl.ds(j, 128, stride=8), :].astype(BF16)
        return carry
    lax.fori_loop(0, HIDDEN // 128, sort_body, 0)

    def kv_body(m, carry):
        rows = pl.ds(pl.multiple_of(m * ROWS, ROWS), ROWS)
        kv = dot(hid[rows, :], wkv[...])
        cos = cos_s[rows, :]
        sin = sin_s[rows, :]
        for h in range(HEADS):
            k = kv[:, h * 128:(h + 1) * 128]
            knv[pl.ds(m * (ROWS * 8) + h, ROWS, stride=8), :] = k * cos + pltpu.roll(k, 64, 1) * sin
            knv[pl.ds(m * (ROWS * 8) + h + 4, ROWS, stride=8), :] = kv[:, (h + 4) * 128:(h + 5) * 128]
        return carry
    lax.fori_loop(0, TOKENS // ROWS, kv_body, 0)

    sub16 = iota((16, HEAD_DIM), 0) >> 2
    low = iota((8, 128), 0) < 4

    def block_body(b, carry):
        e = lax.div(b, 2)
        m = lax.rem(b, 2)
        slot = lax.rem(b, RING)
        wslot = lax.rem(e, WQ_RING)

        @pl.when(m == 0)
        def _():
            load_wq(e).wait()
        for copy in load(b):
            copy.wait()
        rows = pl.ds(pl.multiple_of(m * ROWS, ROWS), ROWS)
        q = dot(hid[rows, :], wq[wslot])
        for t in range(BLOCK):
            place = pos_ref[b * BLOCK + t]
            lines = pl.ds(pl.multiple_of((place >> 2) * 16, 16), 16)
            put = sub16 == (place & 3)
            both = knv[pl.ds(pl.multiple_of((b * BLOCK + t) * 8, 8), 8), :]
            swapped = pltpu.roll(both, 4, 0)
            for n8, buf in ((jnp.where(low, both, swapped), kbuf), (jnp.where(low, swapped, both), vbuf)):
                n16 = jnp.concatenate([n8, n8], axis=0)
                old = buf[slot, t, lines, :].astype(F32)
                buf[slot, t, lines, :] = jnp.where(put, n16, old).astype(BF16)
        for k in range(2):
            picked = ids_ref[rows, k:k + 1] == e
            qsel[k, rows, :] = jnp.where(picked, q, qsel[k, rows, :])
        for copy in save(b):
            copy.start()

        @pl.when((m == 1) & (e + WQ_RING < EXPERTS))
        def _():
            load_wq(e + WQ_RING).start()

        @pl.when(b >= 2)
        def _():
            for copy in save(b - 2):
                copy.wait()

            @pl.when(b - 2 + RING < BLOCKS)
            def _():
                for copy in load(b - 2 + RING):
                    copy.start()
        return carry
    lax.fori_loop(0, BLOCKS, block_body, 0)

    logits = dot_nt(hid[...], router_ref[...])
    g0, g1 = pair_gates(logits, id0, id1)
    lane8 = iota((TOKENS, EXPERTS), 1)
    gates_ref[...] = jnp.where(lane8 == id0, g0, 0.0) + jnp.where(lane8 == id1, g1, 0.0)

    def rope_body(m, carry):
        rows = pl.ds(pl.multiple_of(m * 128, 128), 128)
        cos = cos_s[rows, :]
        sin = sin_s[rows, :]
        for k in range(2):
            for h in range(HEADS):
                q = qsel[k, rows, h * 128:(h + 1) * 128]
                qrow[pl.ds(m * 1024 + k * HEADS + h, 128, stride=8), :] = q * cos + pltpu.roll(q, 64, 1) * sin
        return carry
    lax.fori_loop(0, TOKENS // 128, rope_body, 0)
    for b in (BLOCKS - 2, BLOCKS - 1):
        for copy in save(jnp.int32(b)):
            copy.wait()


def project(positions, x, gain, table, pos_row, ids_t, router_t, w_kv, w_query, k_cache, v_cache):
    any_spec = pl.BlockSpec(memory_space=pl.ANY)
    vmem = pl.BlockSpec(memory_space=pltpu.VMEM)
    smem = pl.BlockSpec(memory_space=pltpu.SMEM)
    cache = jax.ShapeDtypeStruct(k_cache.shape, BF16)
    return pl.pallas_call(
        project_kernel,
        name='project',
        out_shape=(cache, cache, jax.ShapeDtypeStruct((TOKENS * 8, HEAD_DIM), F32),
                   jax.ShapeDtypeStruct((TOKENS, EXPERTS), F32), jax.ShapeDtypeStruct((TOKENS, EXPERTS), jnp.int32)),
        in_specs=[smem] + [vmem] * 6 + [any_spec] * 4,
        out_specs=(any_spec, any_spec, vmem, vmem, vmem),
        scratch_shapes=[
            pltpu.VMEM((TOKENS, HIDDEN), BF16),
            pltpu.VMEM((HIDDEN * 8, 128), BF16),
            pltpu.VMEM((1024, 128), F32),
            pltpu.VMEM((HIDDEN, HEADS * 256), BF16),
            pltpu.VMEM((WQ_RING, HIDDEN, QUERY_COLS), BF16),
            pltpu.VMEM((RING, BLOCK, SLOTS * HEADS, HEAD_DIM), BF16),
            pltpu.VMEM((RING, BLOCK, SLOTS * HEADS, HEAD_DIM), BF16),
            pltpu.VMEM((2, TOKENS, QUERY_COLS), F32),
            pltpu.VMEM((TOKENS * 8, HEAD_DIM), F32),
            pltpu.VMEM((TOKENS, HEAD_DIM), F32),
            pltpu.VMEM((TOKENS, HEAD_DIM), F32),
            pltpu.SemaphoreType.DMA,
            pltpu.SemaphoreType.DMA((WQ_RING,)),
            pltpu.SemaphoreType.DMA((RING,)),
            pltpu.SemaphoreType.DMA((RING,)),
            pltpu.SemaphoreType.DMA((RING,)),
            pltpu.SemaphoreType.DMA((RING,)),
        ],
        compiler_params=pltpu.CompilerParams(vmem_limit_bytes=VMEM_LIMIT),
    )(positions, x, gain, table, pos_row, ids_t, router_t, w_kv, w_query, k_cache, v_cache)


def reduce_columns(drive, partial, base_hbm, out_ref, base_ref, base_sem, send1, recv1, own, recv2, fin, recv3, s1, r1, s2, r2, s3, r3):
    me = lax.axis_index('tp')
    core = lax.rem(me, 2)
    sibling = me + 1 - 2 * core
    partner = lax.rem(me + 2, 4)
    base_copy = pltpu.make_async_copy(base_hbm, base_ref, base_sem)
    base_copy.start()
    barrier = pltpu.get_barrier_semaphore()
    for peer in (sibling, partner):
        pl.semaphore_signal(barrier, inc=1, device_id={'tp': peer}, device_id_type=MESH)
    pl.semaphore_wait(barrier, 2)

    def column(s):
        half = lax.rem(core + 1 + s, 2)
        return pl.multiple_of((half * (STEPS // 2) + lax.div(s, 2)) * COL, COL)

    def remote(src, dst, c, send, recv, peer):
        return pltpu.make_async_remote_copy(src_ref=src.at[c], dst_ref=dst.at[c], send_sem=send.at[c], recv_sem=recv.at[c],
                                            device_id={'tp': peer}, device_id_type=MESH)

    def to_sibling(c):
        return remote(send1, recv1, c, s1, r1, sibling)

    def to_partner(c):
        return remote(own, recv2, c, s2, r2, partner)

    def share(c):
        return remote(fin, recv3, c, s3, r3, sibling)

    def chunk_step(i, parity, m):
        s = 2 * i + parity
        rows = pl.ds(pl.multiple_of(m * ROWS, ROWS), ROWS)
        chunk = 2 * i + m
        acc = partial(s, rows, column(s))
        if parity == 0:
            send1[chunk] = acc.astype(BF16)
            to_sibling(chunk).start()
        else:
            to_sibling(chunk).wait_recv()
            own[chunk] = (acc + recv1[chunk].astype(F32)).astype(BF16)
            to_partner(chunk).start()

    drive(chunk_step, column)
    base_copy.wait()

    def place(c, half):
        rows = pl.ds(pl.multiple_of(lax.rem(c, 2) * ROWS, ROWS), ROWS)
        cols = pl.ds(pl.multiple_of((half * (STEPS // 2) + lax.div(c, 2)) * COL, COL), COL)
        return rows, cols

    def final_body(c, carry):
        to_partner(c).wait_recv()
        rows, cols = place(c, core)
        total = own[c].astype(F32) + recv2[c].astype(F32)
        value = (base_ref[rows, cols].astype(F32) + total).astype(BF16)
        fin[c] = value
        out_ref[rows, cols] = value
        share(c).start()
        return carry
    lax.fori_loop(0, CHUNKS, final_body, 0)

    def gather_body(c, carry):
        share(c).wait_recv()
        rows, cols = place(c, 1 - core)
        out_ref[rows, cols] = recv3[c]
        return carry
    lax.fori_loop(0, CHUNKS, gather_body, 0)

    def drain_body(c, carry):
        to_sibling(c).wait_send()
        to_partner(c).wait_send()
        share(c).wait_send()
        return carry
    lax.fori_loop(0, CHUNKS, drain_body, 0)


CHUNK_SCRATCH = [pltpu.VMEM((TOKENS, HIDDEN), BF16), pltpu.SemaphoreType.DMA] + [pltpu.VMEM((CHUNKS, ROWS, COL), BF16)] * 6 + [pltpu.SemaphoreType.DMA((CHUNKS,))] * 6
A_RING = 8
HALF_BLOCKS = ROWS // BLOCK


def attend_kernel(pos_ref, ids_ref, gates_ref, q_hbm, kc_hbm, vc_hbm, w_hbm, x_hbm, out_ref,
                  qrow, kbuf, vbuf, probs, orow, mixed, spread, wbuf, q_sem, k_sem, v_sem, w_sem, *chunk_refs):
    def load(b):
        slot = lax.rem(b, A_RING)
        rows = pl.ds(pl.multiple_of(b * BLOCK, BLOCK), BLOCK)
        return (pltpu.make_async_copy(kc_hbm.at[rows], kbuf.at[slot], k_sem.at[slot]),
                pltpu.make_async_copy(vc_hbm.at[rows], vbuf.at[slot], v_sem.at[slot]))

    q_copy = pltpu.make_async_copy(q_hbm, qrow, q_sem)
    q_copy.start()
    for b in range(A_RING):
        for copy in load(jnp.int32(b)):
            copy.start()
    w_copies = [pltpu.make_async_copy(w_hbm.at[e], wbuf.at[e], w_sem.at[e]) for e in range(EXPERTS)]
    for copy in w_copies:
        copy.start()

    scale = HEAD_DIM ** -0.5
    row8 = iota((8, 128), 0)
    lane = iota((8, 128), 1)
    same_head = (lane & 3) == (row8 & 3)
    slot_of = lane >> 2

    def attend_rows(m):
        def block_body(i, carry):
            b = m * HALF_BLOCKS + jnp.minimum(i, HALF_BLOCKS - 1)
            before = jnp.maximum(i - 1, 0)
            prev = m * HALF_BLOCKS + before
            slot = lax.rem(b, A_RING)
            prev_slot = lax.rem(prev, A_RING)
            side = lax.rem(i, 2)

            @pl.when(i < HALF_BLOCKS)
            def _():
                for copy in load(b):
                    copy.wait()

            def score(t):
                q = qrow[pl.ds(pl.multiple_of((b * BLOCK + t) * 8, 8), 8), :].astype(BF16)
                s = dot_nt(q, kbuf[slot, t]) * scale
                s = jnp.where(same_head & (slot_of <= pos_ref[b * BLOCK + t]), s, NEG)
                e = jnp.exp(s - jnp.max(s, axis=1, keepdims=True))
                probs[side, t] = e / jnp.sum(e, axis=1, keepdims=True)

            def mix(t):
                orow[t * 8:(t + 1) * 8, :] = dot(probs[1 - side, t].astype(BF16), vbuf[prev_slot, t])

            half = BLOCK // 2
            for t in range(half):
                score(t)
            for t in range(half):
                mix(t)
            for t in range(half, BLOCK):
                score(t)
            for t in range(half, BLOCK):
                mix(t)
            rows = pl.ds(pl.multiple_of(before * BLOCK, BLOCK), BLOCK)
            for r in range(8):
                mixed[rows, r * 128:(r + 1) * 128] = orow[pl.ds(r, BLOCK, stride=8), :].astype(BF16)

            @pl.when((i >= 1) & (prev + A_RING < BLOCKS))
            def _():
                for copy in load(prev + A_RING):
                    copy.start()
            return carry
        lax.fori_loop(0, HALF_BLOCKS + 1, block_body, 0)

        def spread_body(n, carry):
            rows = pl.ds(pl.multiple_of(n * 64, 64), 64)
            from_rows = pl.ds(pl.multiple_of(m * ROWS + n * 64, 64), 64)
            first = mixed[rows, :QUERY_COLS].astype(F32)
            second = mixed[rows, QUERY_COLS:].astype(F32)
            for e in range(EXPERTS):
                picked = jnp.where(ids_ref[from_rows, 0:1] == e, first, 0.0)
                picked = jnp.where(ids_ref[from_rows, 1:2] == e, second, picked)
                spread[e, rows, :] = picked.astype(BF16)
            return carry
        lax.fori_loop(0, ROWS // 64, spread_body, 0)

    def partial(s, rows, col):
        acc = jnp.zeros((ROWS, COL), F32)
        for e in range(EXPERTS):
            acc = acc + gates_ref[rows, e:e + 1] * dot(spread[e], wbuf[e, :, pl.ds(col, COL)])
        return acc

    def drive(chunk_step, column):
        q_copy.wait()

        def half_body(m, carry):
            attend_rows(m)

            @pl.when(m == 0)
            def _():
                for copy in w_copies:
                    copy.wait()

            def col_body(i, c):
                for parity in range(2):
                    chunk_step(i, parity, m)
                return c
            lax.fori_loop(0, STEPS // 2, col_body, 0)
            return carry
        lax.fori_loop(0, TOKENS // ROWS, half_body, 0)

    reduce_columns(drive, partial, x_hbm, out_ref, *chunk_refs)


def attend(positions, ids, gates, q, k_cache, v_cache, w_out, x):
    vmem = pl.BlockSpec(memory_space=pltpu.VMEM)
    any_spec = pl.BlockSpec(memory_space=pl.ANY)
    return pl.pallas_call(
        attend_kernel,
        name='attend',
        out_shape=jax.ShapeDtypeStruct((TOKENS, HIDDEN), BF16),
        in_specs=[pl.BlockSpec(memory_space=pltpu.SMEM)] + [vmem] * 2 + [any_spec] * 5,
        out_specs=vmem,
        scratch_shapes=[
            pltpu.VMEM((TOKENS * 8, HEAD_DIM), F32),
            pltpu.VMEM((A_RING, BLOCK, SLOTS * HEADS, HEAD_DIM), BF16),
            pltpu.VMEM((A_RING, BLOCK, SLOTS * HEADS, HEAD_DIM), BF16),
            pltpu.VMEM((2, BLOCK, 8, HEAD_DIM), F32),
            pltpu.VMEM((BLOCK * 8, HEAD_DIM), F32),
            pltpu.VMEM((ROWS, 2 * QUERY_COLS), BF16),
            pltpu.VMEM((EXPERTS, ROWS, QUERY_COLS), BF16),
            pltpu.VMEM((EXPERTS, QUERY_COLS, HIDDEN), BF16),
            pltpu.SemaphoreType.DMA,
            pltpu.SemaphoreType.DMA((A_RING,)),
            pltpu.SemaphoreType.DMA((A_RING,)),
            pltpu.SemaphoreType.DMA((EXPERTS,)),
        ] + CHUNK_SCRATCH,
        compiler_params=pltpu.CompilerParams(vmem_limit_bytes=VMEM_LIMIT, collective_id=0, has_side_effects=True),
    )(positions, ids, gates, q, k_cache, v_cache, w_out, x)


def gate_up_kernel(x_ref, gain_ref, router_ref, idst_ref, wg_hbm, wu_hbm, a_hbm, gates_ref,
                   unorm, picked, scatter, gathered, wg, wu, act, abuf, wg_sem, wu_sem, a_sem):
    first_id = lax.axis_index('tp') * LOCAL

    def load(s):
        e = lax.div(s, F_TILES)
        cols = pl.ds(pl.multiple_of(lax.rem(s, F_TILES) * FT, FT), FT)
        slot = lax.rem(s, W_RING)
        return (pltpu.make_async_copy(wg_hbm.at[e, :, cols], wg.at[slot], wg_sem.at[slot]),
                pltpu.make_async_copy(wu_hbm.at[e, :, cols], wu.at[slot], wu_sem.at[slot]))

    def save(s):
        e = lax.div(s, F_TILES)
        cols = pl.ds(pl.multiple_of(lax.rem(s, F_TILES) * FT, FT), FT)
        slot = lax.rem(s, 2)
        return pltpu.make_async_copy(abuf.at[slot], a_hbm.at[e, :, cols], a_sem.at[slot])

    for s in range(W_RING):
        for copy in load(jnp.int32(s)):
            copy.start()

    norm_rows(x_ref, gain_ref, unorm)
    ids = turn((idst_ref[0:1, :], idst_ref[1:2, :]))
    id0 = ids[:, 0:1]
    id1 = ids[:, 1:2]
    logits = dot_nt(unorm[...], router_ref[...])
    g0, g1 = pair_gates(logits, id0, id1)
    lane8 = iota((TOKENS, EXPERTS), 1)
    local8 = lane8 + first_id
    gates_ref[...] = jnp.where(local8 == id0, g0, 0.0) + jnp.where(local8 == id1, g1, 0.0)

    before = iota((TOKENS, TOKENS), 0)
    after = iota((TOKENS, TOKENS), 1)
    lower = jnp.where(after < before, 1.0, 0.0).astype(BF16)
    upper = jnp.where(before < after, 1.0, 0.0).astype(BF16)
    lane_id = iota((TOKENS, 128), 1) + first_id
    mask_col = jnp.where((lane_id == id0) | (lane_id == id1), 1.0, 0.0)
    rank_col = dot(lower, mask_col.astype(BF16))
    sub_id = iota((8, TOKENS), 0) + first_id
    mask_row = jnp.where((sub_id == idst_ref[0:1, :]) | (sub_id == idst_ref[1:2, :]), 1.0, 0.0)
    rank_row = dot(mask_row.astype(BF16), upper)
    counts = []
    for e in range(LOCAL):
        counts.append(jnp.sum(mask_row[e:e + 1, :]).astype(jnp.int32))
        where_col = jnp.where(mask_col[:, e:e + 1] > 0.0, rank_col[:, e:e + 1], -1.0)
        where_row = jnp.where(mask_row[e:e + 1, :] > 0.0, rank_row[e:e + 1, :], -1.0)
        scatter[e] = jnp.where(after.astype(F32) == where_col, 1.0, 0.0).astype(BF16)
        picked[e] = jnp.where(before.astype(F32) == where_row, 1.0, 0.0).astype(BF16)
    blocks = [lax.div(n + (RB - 1), RB) for n in counts]

    for e in range(LOCAL):
        def gather_body(rb, carry):
            rows = pl.ds(pl.multiple_of(rb * RB, RB), RB)
            gathered[e, rows, :] = dot(picked[e, rows, :], unorm[...]).astype(BF16)
            return carry
        lax.fori_loop(0, blocks[e], gather_body, 0)

    def step_body(s, carry):
        e = lax.div(s, F_TILES)
        slot = lax.rem(s, W_RING)
        out_slot = lax.rem(s, 2)
        for copy in load(s):
            copy.wait()

        @pl.when(s >= 2)
        def _():
            save(s - 2).wait()

        def run(count):
            for n in range(FT // COL):
                cols = slice(n * COL, (n + 1) * COL)
                gate = dot(gathered[e, :count, :], wg[slot, :, cols])
                up = dot(gathered[e, :count, :], wu[slot, :, cols])
                act[:count, cols] = (gate * (1.0 / (1.0 + jnp.exp(-gate))) * up).astype(BF16)
            for m in range(TOKENS // ROWS):
                rows = slice(m * ROWS, (m + 1) * ROWS)
                abuf[out_slot, rows, :] = dot(scatter[e, rows, :count], act[:count, :]).astype(BF16)

        n_blocks = jnp.where(e == 0, blocks[0], blocks[1])
        for k in range(1, TOKENS // RB + 1):
            pl.when(n_blocks == k)(functools.partial(run, k * RB))

        @pl.when(s + W_RING < MLP_STEPS)
        def _():
            for copy in load(s + W_RING):
                copy.start()
        save(s).start()
        return carry
    lax.fori_loop(0, MLP_STEPS, step_body, 0)
    for s in (MLP_STEPS - 2, MLP_STEPS - 1):
        save(jnp.int32(s)).wait()


def gate_up(x_mid, gain, router_t, ids_t, w_gate, w_up):
    any_spec = pl.BlockSpec(memory_space=pl.ANY)
    vmem = pl.BlockSpec(memory_space=pltpu.VMEM)
    return pl.pallas_call(
        gate_up_kernel,
        name='gate_up',
        out_shape=(jax.ShapeDtypeStruct((LOCAL, TOKENS, FFN), BF16), jax.ShapeDtypeStruct((TOKENS, EXPERTS), F32)),
        in_specs=[vmem] * 4 + [any_spec] * 2,
        out_specs=(any_spec, vmem),
        scratch_shapes=[
            pltpu.VMEM((TOKENS, HIDDEN), BF16),
            pltpu.VMEM((LOCAL, TOKENS, TOKENS), BF16),
            pltpu.VMEM((LOCAL, TOKENS, TOKENS), BF16),
            pltpu.VMEM((LOCAL, TOKENS, HIDDEN), BF16),
            pltpu.VMEM((W_RING, HIDDEN, FT), BF16),
            pltpu.VMEM((W_RING, HIDDEN, FT), BF16),
            pltpu.VMEM((TOKENS, FT), BF16),
            pltpu.VMEM((2, TOKENS, FT), BF16),
            pltpu.SemaphoreType.DMA((W_RING,)),
            pltpu.SemaphoreType.DMA((W_RING,)),
            pltpu.SemaphoreType.DMA((2,)),
        ],
        compiler_params=pltpu.CompilerParams(vmem_limit_bytes=VMEM_LIMIT),
    )(x_mid, gain, router_t, ids_t, w_gate, w_up)


DOWN_RING = 2


def down_kernel(gates_ref, x_ref, a_hbm, w_hbm, out_ref, abuf, wbuf, a_sem, w_sem, *chunk_refs):
    me = lax.axis_index('tp')
    core = lax.rem(me, 2)

    def copies(s, col):
        slot = lax.rem(s, DOWN_RING)
        return [pltpu.make_async_copy(w_hbm.at[e, :, pl.ds(col, COL)], wbuf.at[slot, e], w_sem.at[slot, e]) for e in range(LOCAL)]

    a_copies = [pltpu.make_async_copy(a_hbm.at[e], abuf.at[e], a_sem.at[e]) for e in range(LOCAL)]
    for copy in a_copies:
        copy.start()
    for s in range(DOWN_RING):
        half = lax.rem(core + 1 + s, 2)
        for copy in copies(jnp.int32(s), pl.multiple_of((half * (STEPS // 2) + s // 2) * COL, COL)):
            copy.start()
    for copy in a_copies:
        copy.wait()

    def partial(s, rows, col):
        slot = lax.rem(s, DOWN_RING)
        acc = gates_ref[rows, 0:1] * dot(abuf[0, rows, :], wbuf[slot, 0])
        return acc + gates_ref[rows, 1:2] * dot(abuf[1, rows, :], wbuf[slot, 1])

    def drive(chunk_step, column):
        def col_body(i, carry):
            for parity in range(2):
                s = 2 * i + parity
                for copy in copies(s, column(s)):
                    copy.wait()

                def row_body(m, c):
                    chunk_step(i, parity, m)
                    return c
                lax.fori_loop(0, TOKENS // ROWS, row_body, 0)

                @pl.when(s + DOWN_RING < STEPS)
                def _():
                    for copy in copies(s + DOWN_RING, column(s + DOWN_RING)):
                        copy.start()
            return carry
        lax.fori_loop(0, STEPS // 2, col_body, 0)

    reduce_columns(drive, partial, x_ref, out_ref, *chunk_refs)


def down_project(gates, x_mid, act, w_down):
    vmem = pl.BlockSpec(memory_space=pltpu.VMEM)
    any_spec = pl.BlockSpec(memory_space=pl.ANY)
    return pl.pallas_call(
        down_kernel,
        name='down_project',
        out_shape=jax.ShapeDtypeStruct((TOKENS, HIDDEN), BF16),
        in_specs=[vmem] + [any_spec] * 3,
        out_specs=vmem,
        scratch_shapes=[
            pltpu.VMEM((LOCAL, TOKENS, FFN), BF16),
            pltpu.VMEM((DOWN_RING, LOCAL, FFN, COL), BF16),
            pltpu.SemaphoreType.DMA((LOCAL,)),
            pltpu.SemaphoreType.DMA((DOWN_RING, LOCAL)),
        ] + CHUNK_SCRATCH,
        compiler_params=pltpu.CompilerParams(vmem_limit_bytes=VMEM_LIMIT, collective_id=1, has_side_effects=True),
    )(gates, x_mid, act, w_down)


def rope_table():
    half = HEAD_DIM // 2
    inv_freq = np.float32(ROPE_BASE) ** (-(np.arange(half, dtype=np.float32) * np.float32(2.0) / np.float32(HEAD_DIM)))
    angles = np.arange(SLOTS, dtype=np.float32)[:, None] * inv_freq[None, :].astype(np.float32)
    cos = np.cos(angles.astype(np.float64))
    sin = np.sin(angles.astype(np.float64))
    full = np.concatenate([cos, cos, -sin, sin], axis=1).astype(np.float32)
    parts = []
    for _ in range(3):
        part = full.astype(BF16)
        parts.append(part)
        full = full - part.astype(np.float32)
    parts.append(np.zeros_like(parts[0]))
    return np.concatenate(parts, axis=0)


def solution(mesh):
    table = rope_table()

    def local_step(x, k_cache, v_cache, positions, att_ids, mlp_ids, norm_att, w_kv, router_att, w_query, w_out, norm_mlp, router_mlp, w_gate, w_up, w_down):
        flat = (TOKENS, SLOTS * HEADS, HEAD_DIM)
        kv_rows = w_kv.reshape(HIDDEN, HEADS, 2, HEAD_DIM).transpose(0, 2, 1, 3).reshape(HIDDEN * 8, HEAD_DIM)
        k_new, v_new, q, att_gates, att_cols = project(
            positions, x, norm_att.reshape(1, HIDDEN), jnp.asarray(table), positions.reshape(1, TOKENS), att_ids.T, router_att.T,
            kv_rows, w_query, k_cache.reshape(flat), v_cache.reshape(flat))
        x_mid = attend(positions, att_cols, att_gates, q, k_new, v_new, w_out, x)
        act, mlp_gates = gate_up(x_mid, norm_mlp.reshape(1, HIDDEN), router_mlp.T, mlp_ids.T, w_gate, w_up)
        x_out = down_project(mlp_gates, x_mid, act, w_down)
        return x_out, k_new.reshape(k_cache.shape), v_new.reshape(v_cache.shape)

    token_spec = P('dp', None)
    cache_spec = P('dp', None, 'tp', None)
    expert_spec = P('tp', None, None)
    in_specs = (token_spec, cache_spec, cache_spec, P('dp'), token_spec, token_spec, P(), P(None, 'tp', None), P(), P(None, None, 'tp'), P(None, 'tp', None), P(), P(), expert_spec, expert_spec, expert_spec)
    out_specs = (token_spec, cache_spec, cache_spec)
    return jax.shard_map(local_step, mesh=mesh, in_specs=in_specs, out_specs=out_specs, check_vma=False)
```

```python
import functools

import jax
import jax.numpy as jnp
import numpy as np
from jax import lax
from jax.experimental import pallas as pl
from jax.experimental.pallas import tpu as pltpu
from jax.sharding import PartitionSpec as P

NORM_EPS = 1e-6
ROPE_BASE = 10000.0
F32 = jnp.float32
BF16 = jnp.bfloat16
NEG = -1e30
MESH = pl.DeviceIdType.MESH
VMEM_LIMIT = 62 * 1024 * 1024

TOKENS = 512
HIDDEN = 2048
HEADS = 4
HEAD_DIM = 128
SLOTS = 32
QUERY_COLS = HEADS * HEAD_DIM
EXPERTS = 8
FFN = 5632
LOCAL = 2

BLOCK = 32
RING = 8
BLOCKS = TOKENS // BLOCK
GROUP = 8
WQ_RING = 3

COL = 256
ROWS = 256
STEPS = HIDDEN // COL
CHUNKS = STEPS // 2 * (TOKENS // ROWS)

FT = 512
F_TILES = FFN // FT
MLP_STEPS = LOCAL * F_TILES
W_RING = 5
RB = 128


def dot(a, b):
    return jnp.dot(a, b, preferred_element_type=F32)


def iota(shape, dim):
    return lax.broadcasted_iota(jnp.int32, shape, dim)


def norm_rows(x_ref, gain_ref, out_ref):
    def body(i, carry):
        rows = pl.ds(pl.multiple_of(i * 32, 32), 32)
        values = x_ref[rows, :].astype(F32)
        inv = lax.rsqrt(jnp.mean(values * values, axis=-1, keepdims=True) + NORM_EPS)
        out_ref[rows, :] = (values * inv * gain_ref[...]).astype(BF16)
        return carry
    lax.fori_loop(0, TOKENS // 32, body, 0)


def pair_gates(logits, id0, id1):
    lane = iota(logits.shape, 1)
    first = jnp.sum(jnp.where(lane == id0, logits, 0.0), axis=1, keepdims=True)
    second = jnp.sum(jnp.where(lane == id1, logits, 0.0), axis=1, keepdims=True)
    top = jnp.maximum(first, second)
    e0 = jnp.exp(first - top)
    e1 = jnp.exp(second - top)
    total = e0 + e1
    return e0 / total, e1 / total


def turn(rows):
    sub = iota((8, TOKENS), 0)
    stacked = jnp.zeros((8, TOKENS), F32)
    for i, row in enumerate(rows):
        stacked = jnp.where(sub == i, row.astype(F32), stacked)
    return jnp.transpose(stacked).astype(jnp.int32)


def dot_nt(a, b):
    return lax.dot_general(a, b, (((1,), (1,)), ((), ())), preferred_element_type=F32)


def project_kernel(pos_ref, x_ref, gain_ref, table_ref, posrow_ref, idst_ref, router_ref, wkv_hbm, wq_hbm, kc_hbm, vc_hbm,
                   ko_hbm, vo_hbm, q_ref, gates_ref, ids_ref,
                   hid, wraw, wtmp, wkv, wq, kbuf, vbuf, qsel, qrow, knv, cos_s, sin_s,
                   wkv_sem, wq_sem, kin_sem, vin_sem, kout_sem, vout_sem):
    def block_of(ref, b):
        return ref.at[pl.ds(pl.multiple_of(b * BLOCK, BLOCK), BLOCK)]

    def load(b):
        slot = lax.rem(b, RING)
        return (pltpu.make_async_copy(block_of(kc_hbm, b), kbuf.at[slot], kin_sem.at[slot]),
                pltpu.make_async_copy(block_of(vc_hbm, b), vbuf.at[slot], vin_sem.at[slot]))

    def save(b):
        slot = lax.rem(b, RING)
        return (pltpu.make_async_copy(kbuf.at[slot], block_of(ko_hbm, b), kout_sem.at[slot]),
                pltpu.make_async_copy(vbuf.at[slot], block_of(vo_hbm, b), vout_sem.at[slot]))

    def load_wq(e):
        slot = lax.rem(e, WQ_RING)
        return pltpu.make_async_copy(wq_hbm.at[e], wq.at[slot], wq_sem.at[slot])

    kv_copy = pltpu.make_async_copy(wkv_hbm, wraw, wkv_sem)
    kv_copy.start()
    for e in range(WQ_RING):
        load_wq(jnp.int32(e)).start()

    norm_rows(x_ref, gain_ref, hid)
    ids = turn((idst_ref[0:1, :], idst_ref[1:2, :], posrow_ref[...]))
    ids_ref[...] = ids
    id0 = ids[:, 0:1]
    id1 = ids[:, 1:2]
    lane128 = iota((TOKENS, 128), 1)
    chosen = ((lane128 & 31) == ids[:, 2:3]) & (lane128 < 3 * SLOTS)
    trig = dot(jnp.where(chosen, 1.0, 0.0).astype(BF16), table_ref[...])
    cos_s[...] = trig[:, :HEAD_DIM]
    sin_s[...] = trig[:, HEAD_DIM:]
    for b in range(RING):
        for copy in load(jnp.int32(b)):
            copy.start()
    kv_copy.wait()

    def sort_body(i, carry):
        wtmp[...] = wraw[pl.ds(pl.multiple_of(i * 1024, 1024), 1024), :].astype(F32)
        rows = pl.ds(pl.multiple_of(i * 128, 128), 128)
        for j in range(8):
            wkv[rows, j * 128:(j + 1) * 128] = wtmp[pl.ds(j, 128, stride=8), :].astype(BF16)
        return carry
    lax.fori_loop(0, HIDDEN // 128, sort_body, 0)

    def kv_body(m, carry):
        rows = pl.ds(pl.multiple_of(m * ROWS, ROWS), ROWS)
        kv = dot(hid[rows, :], wkv[...])
        cos = cos_s[rows, :]
        sin = sin_s[rows, :]
        for h in range(HEADS):
            k = kv[:, h * 128:(h + 1) * 128]
            knv[pl.ds(m * (ROWS * 8) + h, ROWS, stride=8), :] = k * cos + pltpu.roll(k, 64, 1) * sin
            knv[pl.ds(m * (ROWS * 8) + h + 4, ROWS, stride=8), :] = kv[:, (h + 4) * 128:(h + 5) * 128]
        return carry
    lax.fori_loop(0, TOKENS // ROWS, kv_body, 0)

    sub16 = iota((16, HEAD_DIM), 0) >> 2
    low = iota((8, 128), 0) < 4

    def block_body(b, carry):
        e = lax.div(b, 2)
        m = lax.rem(b, 2)
        slot = lax.rem(b, RING)
        wslot = lax.rem(e, WQ_RING)

        @pl.when(m == 0)
        def _():
            load_wq(e).wait()
        for copy in load(b):
            copy.wait()
        rows = pl.ds(pl.multiple_of(m * ROWS, ROWS), ROWS)
        q = dot(hid[rows, :], wq[wslot])
        for t in range(BLOCK):
            place = pos_ref[b * BLOCK + t]
            lines = pl.ds(pl.multiple_of((place >> 2) * 16, 16), 16)
            put = sub16 == (place & 3)
            both = knv[pl.ds(pl.multiple_of((b * BLOCK + t) * 8, 8), 8), :]
            swapped = pltpu.roll(both, 4, 0)
            for n8, buf in ((jnp.where(low, both, swapped), kbuf), (jnp.where(low, swapped, both), vbuf)):
                n16 = jnp.concatenate([n8, n8], axis=0)
                old = buf[slot, t, lines, :].astype(F32)
                buf[slot, t, lines, :] = jnp.where(put, n16, old).astype(BF16)
        for k in range(2):
            picked = ids_ref[rows, k:k + 1] == e
            qsel[k, rows, :] = jnp.where(picked, q, qsel[k, rows, :])
        for copy in save(b):
            copy.start()

        @pl.when((m == 1) & (e + WQ_RING < EXPERTS))
        def _():
            load_wq(e + WQ_RING).start()

        @pl.when(b >= 2)
        def _():
            for copy in save(b - 2):
                copy.wait()

            @pl.when(b - 2 + RING < BLOCKS)
            def _():
                for copy in load(b - 2 + RING):
                    copy.start()
        return carry
    lax.fori_loop(0, BLOCKS, block_body, 0)

    logits = dot_nt(hid[...], router_ref[...])
    g0, g1 = pair_gates(logits, id0, id1)
    lane8 = iota((TOKENS, EXPERTS), 1)
    gates_ref[...] = jnp.where(lane8 == id0, g0, 0.0) + jnp.where(lane8 == id1, g1, 0.0)

    def rope_body(m, carry):
        rows = pl.ds(pl.multiple_of(m * 128, 128), 128)
        cos = cos_s[rows, :]
        sin = sin_s[rows, :]
        for k in range(2):
            for h in range(HEADS):
                q = qsel[k, rows, h * 128:(h + 1) * 128]
                qrow[pl.ds(k * HEADS + h, 128, stride=8), :] = q * cos + pltpu.roll(q, 64, 1) * sin
        q = qrow[...]
        even = (iota((1024, HEAD_DIM), 0) & 8) == 0
        lines = pl.ds(pl.multiple_of(m * 1024, 1024), 1024)
        q_ref[lines, :HEAD_DIM] = jnp.where(even, q, 0.0).astype(BF16)
        q_ref[lines, HEAD_DIM:] = jnp.where(even, 0.0, q).astype(BF16)
        return carry
    lax.fori_loop(0, TOKENS // 128, rope_body, 0)
    for b in (BLOCKS - 2, BLOCKS - 1):
        for copy in save(jnp.int32(b)):
            copy.wait()


def project(positions, x, gain, table, pos_row, ids_t, router_t, w_kv, w_query, k_cache, v_cache):
    any_spec = pl.BlockSpec(memory_space=pl.ANY)
    vmem = pl.BlockSpec(memory_space=pltpu.VMEM)
    smem = pl.BlockSpec(memory_space=pltpu.SMEM)
    cache = jax.ShapeDtypeStruct(k_cache.shape, BF16)
    return pl.pallas_call(
        project_kernel,
        name='project',
        out_shape=(cache, cache, jax.ShapeDtypeStruct((TOKENS * 8, 2 * HEAD_DIM), BF16),
                   jax.ShapeDtypeStruct((TOKENS, EXPERTS), F32), jax.ShapeDtypeStruct((TOKENS, EXPERTS), jnp.int32)),
        in_specs=[smem] + [vmem] * 6 + [any_spec] * 4,
        out_specs=(any_spec, any_spec, vmem, vmem, vmem),
        scratch_shapes=[
            pltpu.VMEM((TOKENS, HIDDEN), BF16),
            pltpu.VMEM((HIDDEN * 8, 128), BF16),
            pltpu.VMEM((1024, 128), F32),
            pltpu.VMEM((HIDDEN, HEADS * 256), BF16),
            pltpu.VMEM((WQ_RING, HIDDEN, QUERY_COLS), BF16),
            pltpu.VMEM((RING, BLOCK, SLOTS * HEADS, HEAD_DIM), BF16),
            pltpu.VMEM((RING, BLOCK, SLOTS * HEADS, HEAD_DIM), BF16),
            pltpu.VMEM((2, TOKENS, QUERY_COLS), F32),
            pltpu.VMEM((1024, HEAD_DIM), F32),
            pltpu.VMEM((TOKENS * 8, HEAD_DIM), F32),
            pltpu.VMEM((TOKENS, HEAD_DIM), F32),
            pltpu.VMEM((TOKENS, HEAD_DIM), F32),
            pltpu.SemaphoreType.DMA,
            pltpu.SemaphoreType.DMA((WQ_RING,)),
            pltpu.SemaphoreType.DMA((RING,)),
            pltpu.SemaphoreType.DMA((RING,)),
            pltpu.SemaphoreType.DMA((RING,)),
            pltpu.SemaphoreType.DMA((RING,)),
        ],
        compiler_params=pltpu.CompilerParams(vmem_limit_bytes=VMEM_LIMIT),
    )(positions, x, gain, table, pos_row, ids_t, router_t, w_kv, w_query, k_cache, v_cache)


def reduce_columns(drive, partial, base_hbm, out_ref, base_ref, base_sem, send1, recv1, own, recv2, fin, recv3, s1, r1, s2, r2, s3, r3):
    chunks, height, width = send1.shape
    per = TOKENS // height
    half_width = HIDDEN // 2
    me = lax.axis_index('tp')
    core = lax.rem(me, 2)
    sibling = me + 1 - 2 * core
    partner = lax.rem(me + 2, 4)
    barrier = pltpu.get_barrier_semaphore()
    for peer in (sibling, partner):
        pl.semaphore_signal(barrier, inc=1, device_id={'tp': peer}, device_id_type=MESH)
    pl.semaphore_wait(barrier, 2)

    def column(s):
        half = lax.rem(core + 1 + s, 2)
        return pl.multiple_of(half * half_width + lax.div(s, 2) * width, width)

    def remote(src, dst, c, send, recv, peer):
        return pltpu.make_async_remote_copy(src_ref=src.at[c], dst_ref=dst.at[c], send_sem=send.at[c], recv_sem=recv.at[c],
                                            device_id={'tp': peer}, device_id_type=MESH)

    def to_sibling(c):
        return remote(send1, recv1, c, s1, r1, sibling)

    def to_partner(c):
        return remote(own, recv2, c, s2, r2, partner)

    def share(c):
        return remote(fin, recv3, c, s3, r3, sibling)

    def chunk_step(i, parity, m):
        s = 2 * i + parity
        rows = pl.ds(pl.multiple_of(m * height, height), height)
        chunk = per * i + m
        acc = partial(s, rows, column(s))
        if parity == 0:
            send1[chunk] = acc.astype(BF16)
            to_sibling(chunk).start()
        else:
            to_sibling(chunk).wait_recv()
            own[chunk] = (acc + recv1[chunk].astype(F32)).astype(BF16)
            to_partner(chunk).start()

    def place(c, half):
        rows = pl.ds(pl.multiple_of(lax.rem(c, per) * height, height), height)
        cols = pl.ds(pl.multiple_of(half * half_width + lax.div(c, per) * width, width), width)
        return rows, cols

    def finish(c):
        to_partner(c).wait_recv()
        rows, cols = place(c, core)
        total = own[c].astype(F32) + recv2[c].astype(F32)
        value = (base_ref[rows, cols].astype(F32) + total).astype(BF16)
        fin[c] = value
        share(c).start()
        out_ref[rows, cols] = value

    base_copy = pltpu.make_async_copy(base_hbm, base_ref, base_sem)
    finished = drive(chunk_step, column, finish, base_copy)

    def final_body(c, carry):
        finish(c)
        return carry
    lax.fori_loop(finished, chunks, final_body, 0)

    def gather_body(c, carry):
        share(c).wait_recv()
        rows, cols = place(c, 1 - core)
        out_ref[rows, cols] = recv3[c]
        return carry
    lax.fori_loop(0, chunks, gather_body, 0)

    def drain_body(c, carry):
        to_sibling(c).wait_send()
        to_partner(c).wait_send()
        share(c).wait_send()
        return carry
    lax.fori_loop(0, chunks, drain_body, 0)


def chunk_scratch(height, width):
    chunks = TOKENS * HIDDEN // 2 // (height * width)
    return ([pltpu.VMEM((TOKENS, HIDDEN), BF16), pltpu.SemaphoreType.DMA]
            + [pltpu.VMEM((chunks, height, width), BF16)] * 6 + [pltpu.SemaphoreType.DMA((chunks,))] * 6)


A_RING = 6
A_AHEAD = 4
A_ROWS = 128
PARTS = TOKENS // A_ROWS
PART_BLOCKS = A_ROWS // BLOCK


def attend_kernel(pos_ref, ids_ref, gates_ref, q_hbm, kc_hbm, vc_hbm, w_hbm, x_hbm, out_ref,
                  qbuf, kbuf, vbuf, probs, orow, mixed, spread, wbuf, q_sem, k_sem, v_sem, w_sem, *chunk_refs):
    def load(b):
        slot = lax.rem(b, A_RING)
        rows = pl.ds(pl.multiple_of(b * BLOCK, BLOCK), BLOCK)
        return (pltpu.make_async_copy(kc_hbm.at[rows], kbuf.at[slot], k_sem.at[slot]),
                pltpu.make_async_copy(vc_hbm.at[rows], vbuf.at[slot], v_sem.at[slot]))

    q_copy = pltpu.make_async_copy(q_hbm, qbuf, q_sem)
    q_copy.start()
    for b in range(A_AHEAD):
        for copy in load(jnp.int32(b)):
            copy.start()
    w_copies = [pltpu.make_async_copy(w_hbm.at[e], wbuf.at[e], w_sem.at[e]) for e in range(EXPERTS)]

    scale = HEAD_DIM ** -0.5
    row16 = iota((16, 128), 0)
    lane = iota((16, 128), 1)
    upper = row16 < 8
    same_head = (lane & 3) == (row16 & 3)
    slot_of = lane >> 2

    def attend_rows(m):
        def block_body(i, carry):
            b = m * PART_BLOCKS + jnp.minimum(i, PART_BLOCKS - 1)
            before = jnp.maximum(i - 1, 0)
            prev = m * PART_BLOCKS + before
            slot = lax.rem(b, A_RING)
            prev_slot = lax.rem(prev, A_RING)
            side = lax.rem(i, 2)

            @pl.when(i < PART_BLOCKS)
            def _():
                for copy in load(b):
                    copy.wait()

            def score(j):
                t = b * BLOCK + 2 * j
                q = qbuf[pl.ds(pl.multiple_of(t * 8, 16), 16), :]
                keys = jnp.concatenate([kbuf[slot, 2 * j], kbuf[slot, 2 * j + 1]], axis=1)
                s = dot_nt(q, keys) * scale
                s = jnp.where(same_head & (slot_of <= jnp.where(upper, pos_ref[t], pos_ref[t + 1])), s, NEG)
                e = jnp.exp(s - jnp.max(s, axis=1, keepdims=True))
                probs[side, j] = (e / jnp.sum(e, axis=1, keepdims=True)).astype(BF16)

            def mix(j):
                values = jnp.concatenate([vbuf[prev_slot, 2 * j], vbuf[prev_slot, 2 * j + 1]], axis=1)
                o = dot(probs[1 - side, j], values)
                orow[j * 16:j * 16 + 8, :] = o[:8, :HEAD_DIM]
                orow[j * 16 + 8:j * 16 + 16, :] = o[8:, HEAD_DIM:]

            pairs = BLOCK // 2
            for j in range(pairs // 2):
                score(j)
            for j in range(pairs // 2):
                mix(j)
            for j in range(pairs // 2, pairs):
                score(j)
            for j in range(pairs // 2, pairs):
                mix(j)
            rows = pl.ds(pl.multiple_of(before * BLOCK, BLOCK), BLOCK)
            for r in range(8):
                mixed[rows, r * 128:(r + 1) * 128] = orow[pl.ds(r, BLOCK, stride=8), :].astype(BF16)

            @pl.when((i < PART_BLOCKS) & (b + A_AHEAD < BLOCKS))
            def _():
                for copy in load(b + A_AHEAD):
                    copy.start()
            return carry
        lax.fori_loop(0, PART_BLOCKS + 1, block_body, 0)

        def spread_body(n, carry):
            rows = pl.ds(pl.multiple_of(n * 64, 64), 64)
            from_rows = pl.ds(pl.multiple_of(m * A_ROWS + n * 64, 64), 64)
            first = mixed[rows, :QUERY_COLS].astype(F32)
            second = mixed[rows, QUERY_COLS:].astype(F32)
            for e in range(EXPERTS):
                picked = jnp.where(ids_ref[from_rows, 0:1] == e, first, 0.0)
                picked = jnp.where(ids_ref[from_rows, 1:2] == e, second, picked)
                spread[e, rows, :] = picked.astype(BF16)
            return carry
        lax.fori_loop(0, A_ROWS // 64, spread_body, 0)

    def partial(s, rows, col):
        acc = jnp.zeros((A_ROWS, HIDDEN // 2), F32)
        for e in range(EXPERTS):
            acc = acc + gates_ref[rows, e:e + 1] * dot(spread[e], wbuf[e, :, pl.ds(col, HIDDEN // 2)])
        return acc

    def drive(chunk_step, column, finish, base_copy):
        q_copy.wait()
        for copy in w_copies:
            copy.start()

        def part_body(m, carry):
            attend_rows(m)

            @pl.when(m == 0)
            def _():
                base_copy.start()
                for copy in w_copies:
                    copy.wait()
            for parity in range(2):
                chunk_step(0, parity, m)

            @pl.when(m == 1)
            def _():
                base_copy.wait()

            @pl.when(m >= 2)
            def _():
                finish(m - 2)
            return carry
        lax.fori_loop(0, PARTS, part_body, 0)
        return PARTS - 2

    reduce_columns(drive, partial, x_hbm, out_ref, *chunk_refs)


def attend(positions, ids, gates, q, k_cache, v_cache, w_out, x):
    vmem = pl.BlockSpec(memory_space=pltpu.VMEM)
    any_spec = pl.BlockSpec(memory_space=pl.ANY)
    return pl.pallas_call(
        attend_kernel,
        name='attend',
        out_shape=jax.ShapeDtypeStruct((TOKENS, HIDDEN), BF16),
        in_specs=[pl.BlockSpec(memory_space=pltpu.SMEM)] + [vmem] * 2 + [any_spec] * 5,
        out_specs=vmem,
        scratch_shapes=[
            pltpu.VMEM((TOKENS * 8, 2 * HEAD_DIM), BF16),
            pltpu.VMEM((A_RING, BLOCK, SLOTS * HEADS, HEAD_DIM), BF16),
            pltpu.VMEM((A_RING, BLOCK, SLOTS * HEADS, HEAD_DIM), BF16),
            pltpu.VMEM((2, BLOCK // 2, 16, HEAD_DIM), BF16),
            pltpu.VMEM((BLOCK * 8, HEAD_DIM), F32),
            pltpu.VMEM((A_ROWS, 2 * QUERY_COLS), BF16),
            pltpu.VMEM((EXPERTS, A_ROWS, QUERY_COLS), BF16),
            pltpu.VMEM((EXPERTS, QUERY_COLS, HIDDEN), BF16),
            pltpu.SemaphoreType.DMA,
            pltpu.SemaphoreType.DMA((A_RING,)),
            pltpu.SemaphoreType.DMA((A_RING,)),
            pltpu.SemaphoreType.DMA((EXPERTS,)),
        ] + chunk_scratch(A_ROWS, HIDDEN // 2),
        compiler_params=pltpu.CompilerParams(vmem_limit_bytes=VMEM_LIMIT, collective_id=0, has_side_effects=True),
    )(positions, ids, gates, q, k_cache, v_cache, w_out, x)


def gate_up_kernel(x_ref, gain_ref, router_ref, idst_ref, wg_hbm, wu_hbm, a_hbm, gates_ref,
                   unorm, picked, scatter, gathered, wg, wu, act, abuf, wg_sem, wu_sem, a_sem):
    first_id = lax.axis_index('tp') * LOCAL

    def load(s):
        e = lax.div(s, F_TILES)
        cols = pl.ds(pl.multiple_of(lax.rem(s, F_TILES) * FT, FT), FT)
        slot = lax.rem(s, W_RING)
        return (pltpu.make_async_copy(wg_hbm.at[e, :, cols], wg.at[slot], wg_sem.at[slot]),
                pltpu.make_async_copy(wu_hbm.at[e, :, cols], wu.at[slot], wu_sem.at[slot]))

    def save(s):
        e = lax.div(s, F_TILES)
        cols = pl.ds(pl.multiple_of(lax.rem(s, F_TILES) * FT, FT), FT)
        slot = lax.rem(s, 2)
        return pltpu.make_async_copy(abuf.at[slot], a_hbm.at[e, :, cols], a_sem.at[slot])

    for s in range(W_RING):
        for copy in load(jnp.int32(s)):
            copy.start()

    norm_rows(x_ref, gain_ref, unorm)
    ids = turn((idst_ref[0:1, :], idst_ref[1:2, :]))
    id0 = ids[:, 0:1]
    id1 = ids[:, 1:2]
    logits = dot_nt(unorm[...], router_ref[...])
    g0, g1 = pair_gates(logits, id0, id1)
    lane8 = iota((TOKENS, EXPERTS), 1)
    local8 = lane8 + first_id
    gates_ref[...] = jnp.where(local8 == id0, g0, 0.0) + jnp.where(local8 == id1, g1, 0.0)

    before = iota((TOKENS, TOKENS), 0)
    after = iota((TOKENS, TOKENS), 1)
    lower = jnp.where(after < before, 1.0, 0.0).astype(BF16)
    upper = jnp.where(before < after, 1.0, 0.0).astype(BF16)
    lane_id = iota((TOKENS, 128), 1) + first_id
    mask_col = jnp.where((lane_id == id0) | (lane_id == id1), 1.0, 0.0)
    rank_col = dot(lower, mask_col.astype(BF16))
    sub_id = iota((8, TOKENS), 0) + first_id
    mask_row = jnp.where((sub_id == idst_ref[0:1, :]) | (sub_id == idst_ref[1:2, :]), 1.0, 0.0)
    rank_row = dot(mask_row.astype(BF16), upper)
    counts = []
    for e in range(LOCAL):
        counts.append(jnp.sum(mask_row[e:e + 1, :]).astype(jnp.int32))
        where_col = jnp.where(mask_col[:, e:e + 1] > 0.0, rank_col[:, e:e + 1], -1.0)
        where_row = jnp.where(mask_row[e:e + 1, :] > 0.0, rank_row[e:e + 1, :], -1.0)
        scatter[e] = jnp.where(after.astype(F32) == where_col, 1.0, 0.0).astype(BF16)
        picked[e] = jnp.where(before.astype(F32) == where_row, 1.0, 0.0).astype(BF16)
    blocks = [lax.div(n + (RB - 1), RB) for n in counts]

    for e in range(LOCAL):
        def gather_body(rb, carry):
            rows = pl.ds(pl.multiple_of(rb * RB, RB), RB)
            gathered[e, rows, :] = dot(picked[e, rows, :], unorm[...]).astype(BF16)
            return carry
        lax.fori_loop(0, blocks[e], gather_body, 0)

    def step_body(s, carry):
        e = lax.div(s, F_TILES)
        slot = lax.rem(s, W_RING)
        out_slot = lax.rem(s, 2)
        for copy in load(s):
            copy.wait()

        @pl.when(s >= 2)
        def _():
            save(s - 2).wait()

        def run(count):
            for n in range(FT // COL):
                cols = slice(n * COL, (n + 1) * COL)
                gate = dot(gathered[e, :count, :], wg[slot, :, cols])
                up = dot(gathered[e, :count, :], wu[slot, :, cols])
                act[:count, cols] = (gate * (1.0 / (1.0 + jnp.exp(-gate))) * up).astype(BF16)
            for m in range(TOKENS // ROWS):
                rows = slice(m * ROWS, (m + 1) * ROWS)
                abuf[out_slot, rows, :] = dot(scatter[e, rows, :count], act[:count, :]).astype(BF16)

        n_blocks = jnp.where(e == 0, blocks[0], blocks[1])
        for k in range(1, TOKENS // RB + 1):
            pl.when(n_blocks == k)(functools.partial(run, k * RB))

        @pl.when(s + W_RING < MLP_STEPS)
        def _():
            for copy in load(s + W_RING):
                copy.start()
        save(s).start()
        return carry
    lax.fori_loop(0, MLP_STEPS, step_body, 0)
    for s in (MLP_STEPS - 2, MLP_STEPS - 1):
        save(jnp.int32(s)).wait()


def gate_up(x_mid, gain, router_t, ids_t, w_gate, w_up):
    any_spec = pl.BlockSpec(memory_space=pl.ANY)
    vmem = pl.BlockSpec(memory_space=pltpu.VMEM)
    return pl.pallas_call(
        gate_up_kernel,
        name='gate_up',
        out_shape=(jax.ShapeDtypeStruct((LOCAL, TOKENS, FFN), BF16), jax.ShapeDtypeStruct((TOKENS, EXPERTS), F32)),
        in_specs=[vmem] * 4 + [any_spec] * 2,
        out_specs=(any_spec, vmem),
        scratch_shapes=[
            pltpu.VMEM((TOKENS, HIDDEN), BF16),
            pltpu.VMEM((LOCAL, TOKENS, TOKENS), BF16),
            pltpu.VMEM((LOCAL, TOKENS, TOKENS), BF16),
            pltpu.VMEM((LOCAL, TOKENS, HIDDEN), BF16),
            pltpu.VMEM((W_RING, HIDDEN, FT), BF16),
            pltpu.VMEM((W_RING, HIDDEN, FT), BF16),
            pltpu.VMEM((TOKENS, FT), BF16),
            pltpu.VMEM((2, TOKENS, FT), BF16),
            pltpu.SemaphoreType.DMA((W_RING,)),
            pltpu.SemaphoreType.DMA((W_RING,)),
            pltpu.SemaphoreType.DMA((2,)),
        ],
        compiler_params=pltpu.CompilerParams(vmem_limit_bytes=VMEM_LIMIT),
    )(x_mid, gain, router_t, ids_t, w_gate, w_up)


DOWN_RING = 2


def down_kernel(gates_ref, x_hbm, a_hbm, w_hbm, out_ref, abuf, wbuf, first_part, a_sem, w_sem, *chunk_refs):
    me = lax.axis_index('tp')
    core = lax.rem(me, 2)

    def copy_of(s, col, e):
        slot = lax.rem(s, DOWN_RING)
        return pltpu.make_async_copy(w_hbm.at[e, :, pl.ds(col, COL)], wbuf.at[slot, e], w_sem.at[slot, e])

    def early(s, e):
        half = lax.rem(core + 1 + s, 2)
        return copy_of(jnp.int32(s), pl.multiple_of((half * (STEPS // 2) + s // 2) * COL, COL), e)

    a_copies = [pltpu.make_async_copy(a_hbm.at[e], abuf.at[e], a_sem.at[e]) for e in range(LOCAL)]
    for e in range(LOCAL):
        a_copies[e].start()
        early(0, e).start()

    def partial(s, rows, col):
        return first_part[rows, :] + gates_ref[rows, 1:2] * dot(abuf[1, rows, :], wbuf[lax.rem(s, DOWN_RING), 1])

    def drive(chunk_step, column, finish, base_copy):
        def col_body(i, carry):
            for parity in range(2):
                s = 2 * i + parity
                slot = lax.rem(s, DOWN_RING)
                copy_of(s, column(s), 0).wait()
                if parity == 0:
                    @pl.when(i == 0)
                    def _():
                        a_copies[0].wait()
                        for e in range(LOCAL):
                            early(1, e).start()
                        base_copy.start()
                first_part[...] = gates_ref[:, 0:1] * dot(abuf[0], wbuf[slot, 0])
                if parity == 0:
                    @pl.when(i == 0)
                    def _():
                        a_copies[1].wait()
                copy_of(s, column(s), 1).wait()

                def row_body(m, c):
                    chunk_step(i, parity, m)
                    return c
                lax.fori_loop(0, TOKENS // ROWS, row_body, 0)

                @pl.when(s + DOWN_RING < STEPS)
                def _():
                    for e in range(LOCAL):
                        copy_of(s + DOWN_RING, column(s + DOWN_RING), e).start()

            @pl.when(i == 1)
            def _():
                base_copy.wait()

            @pl.when(i >= 2)
            def _():
                finish(2 * (i - 2))
                finish(2 * (i - 2) + 1)
            return carry
        lax.fori_loop(0, STEPS // 2, col_body, 0)
        return CHUNKS // 2

    reduce_columns(drive, partial, x_hbm, out_ref, *chunk_refs)


def down_project(gates, x_mid, act, w_down):
    vmem = pl.BlockSpec(memory_space=pltpu.VMEM)
    any_spec = pl.BlockSpec(memory_space=pl.ANY)
    return pl.pallas_call(
        down_kernel,
        name='down_project',
        out_shape=jax.ShapeDtypeStruct((TOKENS, HIDDEN), BF16),
        in_specs=[vmem] + [any_spec] * 3,
        out_specs=vmem,
        scratch_shapes=[
            pltpu.VMEM((LOCAL, TOKENS, FFN), BF16),
            pltpu.VMEM((DOWN_RING, LOCAL, FFN, COL), BF16),
            pltpu.VMEM((TOKENS, COL), F32),
            pltpu.SemaphoreType.DMA((LOCAL,)),
            pltpu.SemaphoreType.DMA((DOWN_RING, LOCAL)),
        ] + chunk_scratch(ROWS, COL),
        compiler_params=pltpu.CompilerParams(vmem_limit_bytes=VMEM_LIMIT, collective_id=1, has_side_effects=True),
    )(gates, x_mid, act, w_down)


def rope_table():
    half = HEAD_DIM // 2
    inv_freq = np.float32(ROPE_BASE) ** (-(np.arange(half, dtype=np.float32) * np.float32(2.0) / np.float32(HEAD_DIM)))
    angles = np.arange(SLOTS, dtype=np.float32)[:, None] * inv_freq[None, :].astype(np.float32)
    cos = np.cos(angles.astype(np.float64))
    sin = np.sin(angles.astype(np.float64))
    full = np.concatenate([cos, cos, -sin, sin], axis=1).astype(np.float32)
    parts = []
    for _ in range(3):
        part = full.astype(BF16)
        parts.append(part)
        full = full - part.astype(np.float32)
    parts.append(np.zeros_like(parts[0]))
    return np.concatenate(parts, axis=0)


def solution(mesh):
    table = rope_table()

    def local_step(x, k_cache, v_cache, positions, att_ids, mlp_ids, norm_att, w_kv, router_att, w_query, w_out, norm_mlp, router_mlp, w_gate, w_up, w_down):
        flat = (TOKENS, SLOTS * HEADS, HEAD_DIM)
        kv_rows = w_kv.reshape(HIDDEN, HEADS, 2, HEAD_DIM).transpose(0, 2, 1, 3).reshape(HIDDEN * 8, HEAD_DIM)
        k_new, v_new, q, att_gates, att_cols = project(
            positions, x, norm_att.reshape(1, HIDDEN), jnp.asarray(table), positions.reshape(1, TOKENS), att_ids.T, router_att.T,
            kv_rows, w_query, k_cache.reshape(flat), v_cache.reshape(flat))
        x_mid = attend(positions, att_cols, att_gates, q, k_new, v_new, w_out, x)
        act, mlp_gates = gate_up(x_mid, norm_mlp.reshape(1, HIDDEN), router_mlp.T, mlp_ids.T, w_gate, w_up)
        x_out = down_project(mlp_gates, x_mid, act, w_down)
        return x_out, k_new.reshape(k_cache.shape), v_new.reshape(v_cache.shape)

    token_spec = P('dp', None)
    cache_spec = P('dp', None, 'tp', None)
    expert_spec = P('tp', None, None)
    in_specs = (token_spec, cache_spec, cache_spec, P('dp'), token_spec, token_spec, P(), P(None, 'tp', None), P(), P(None, None, 'tp'), P(None, 'tp', None), P(), P(), expert_spec, expert_spec, expert_spec)
    out_specs = (token_spec, cache_spec, cache_spec)
    return jax.shard_map(local_step, mesh=mesh, in_specs=in_specs, out_specs=out_specs, check_vma=False)
```

```python
import functools

import jax
import jax.numpy as jnp
import numpy as np
from jax import lax
from jax.experimental import pallas as pl
from jax.experimental.pallas import tpu as pltpu
from jax.sharding import PartitionSpec as P

NORM_EPS = 1e-6
ROPE_BASE = 10000.0
F32 = jnp.float32
BF16 = jnp.bfloat16
NEG = -1e30
MESH = pl.DeviceIdType.MESH
VMEM_LIMIT = 62 * 1024 * 1024

TOKENS = 512
HIDDEN = 2048
HEADS = 4
HEAD_DIM = 128
SLOTS = 32
QUERY_COLS = HEADS * HEAD_DIM
EXPERTS = 8
FFN = 5632
LOCAL = 2

BLOCK = 32
RING = 8
BLOCKS = TOKENS // BLOCK
GROUP = 8
WQ_RING = 3

COL = 256
ROWS = 256
STEPS = HIDDEN // COL
CHUNKS = STEPS // 2 * (TOKENS // ROWS)

FT = 512
F_TILES = FFN // FT
MLP_STEPS = LOCAL * F_TILES
W_RING = 5
RB = 128


def dot(a, b):
    return jnp.dot(a, b, preferred_element_type=F32)


def iota(shape, dim):
    return lax.broadcasted_iota(jnp.int32, shape, dim)


def norm_rows(x_ref, gain_ref, out_ref):
    def body(i, carry):
        rows = pl.ds(pl.multiple_of(i * 32, 32), 32)
        values = x_ref[rows, :].astype(F32)
        inv = lax.rsqrt(jnp.mean(values * values, axis=-1, keepdims=True) + NORM_EPS)
        out_ref[rows, :] = (values * inv * gain_ref[...]).astype(BF16)
        return carry
    lax.fori_loop(0, TOKENS // 32, body, 0)


def pair_gates(logits, id0, id1):
    lane = iota(logits.shape, 1)
    first = jnp.sum(jnp.where(lane == id0, logits, 0.0), axis=1, keepdims=True)
    second = jnp.sum(jnp.where(lane == id1, logits, 0.0), axis=1, keepdims=True)
    top = jnp.maximum(first, second)
    e0 = jnp.exp(first - top)
    e1 = jnp.exp(second - top)
    total = e0 + e1
    return e0 / total, e1 / total


def turn(rows):
    sub = iota((8, TOKENS), 0)
    stacked = jnp.zeros((8, TOKENS), F32)
    for i, row in enumerate(rows):
        stacked = jnp.where(sub == i, row.astype(F32), stacked)
    return jnp.transpose(stacked).astype(jnp.int32)


def dot_nt(a, b):
    return lax.dot_general(a, b, (((1,), (1,)), ((), ())), preferred_element_type=F32)


def project_kernel(pos_ref, x_ref, gain_ref, table_ref, posrow_ref, idst_ref, router_ref, wkv_hbm, wq_hbm, kc_hbm, vc_hbm,
                   ko_hbm, vo_hbm, q_ref, gates_ref, ids_ref,
                   hid, wraw, wtmp, wkv, wq, kbuf, vbuf, qsel, qrow, knv, cos_s, sin_s,
                   wkv_sem, wq_sem, kin_sem, vin_sem, kout_sem, vout_sem):
    def block_of(ref, b):
        return ref.at[pl.ds(pl.multiple_of(b * BLOCK, BLOCK), BLOCK)]

    def load(b):
        slot = lax.rem(b, RING)
        return (pltpu.make_async_copy(block_of(kc_hbm, b), kbuf.at[slot], kin_sem.at[slot]),
                pltpu.make_async_copy(block_of(vc_hbm, b), vbuf.at[slot], vin_sem.at[slot]))

    def save(b):
        slot = lax.rem(b, RING)
        return (pltpu.make_async_copy(kbuf.at[slot], block_of(ko_hbm, b), kout_sem.at[slot]),
                pltpu.make_async_copy(vbuf.at[slot], block_of(vo_hbm, b), vout_sem.at[slot]))

    def load_wq(e):
        slot = lax.rem(e, WQ_RING)
        return pltpu.make_async_copy(wq_hbm.at[e], wq.at[slot], wq_sem.at[slot])

    kv_copy = pltpu.make_async_copy(wkv_hbm, wraw, wkv_sem)
    kv_copy.start()
    for b in range(3):
        for copy in load(jnp.int32(b)):
            copy.start()
    load_wq(jnp.int32(0)).start()

    norm_rows(x_ref, gain_ref, hid)
    for e in range(1, WQ_RING):
        load_wq(jnp.int32(e)).start()
    for b in range(3, RING):
        for copy in load(jnp.int32(b)):
            copy.start()
    ids = turn((idst_ref[0:1, :], idst_ref[1:2, :], posrow_ref[...]))
    ids_ref[...] = ids
    id0 = ids[:, 0:1]
    id1 = ids[:, 1:2]
    lane128 = iota((TOKENS, 128), 1)
    chosen = ((lane128 & 31) == ids[:, 2:3]) & (lane128 < 3 * SLOTS)
    trig = dot(jnp.where(chosen, 1.0, 0.0).astype(BF16), table_ref[...])
    cos_s[...] = trig[:, :HEAD_DIM]
    sin_s[...] = trig[:, HEAD_DIM:]
    logits = dot_nt(hid[...], router_ref[...])
    g0, g1 = pair_gates(logits, id0, id1)
    lane8 = iota((TOKENS, EXPERTS), 1)
    gates_ref[...] = jnp.where(lane8 == id0, g0, 0.0) + jnp.where(lane8 == id1, g1, 0.0)
    kv_copy.wait()

    def sort_body(i, carry):
        wtmp[...] = wraw[pl.ds(pl.multiple_of(i * 1024, 1024), 1024), :].astype(F32)
        rows = pl.ds(pl.multiple_of(i * 128, 128), 128)
        for j in range(8):
            wkv[rows, j * 128:(j + 1) * 128] = wtmp[pl.ds(j, 128, stride=8), :].astype(BF16)
        return carry
    lax.fori_loop(0, HIDDEN // 128, sort_body, 0)

    def kv_body(m, carry):
        rows = pl.ds(pl.multiple_of(m * ROWS, ROWS), ROWS)
        kv = dot(hid[rows, :], wkv[...])
        cos = cos_s[rows, :]
        sin = sin_s[rows, :]
        for h in range(HEADS):
            k = kv[:, h * 128:(h + 1) * 128]
            knv[pl.ds(m * (ROWS * 8) + h, ROWS, stride=8), :] = k * cos + pltpu.roll(k, 64, 1) * sin
            knv[pl.ds(m * (ROWS * 8) + h + 4, ROWS, stride=8), :] = kv[:, (h + 4) * 128:(h + 5) * 128]
        return carry
    lax.fori_loop(0, TOKENS // ROWS, kv_body, 0)

    sub16 = iota((16, HEAD_DIM), 0) >> 2
    low = iota((8, 128), 0) < 4

    def block_body(b, carry):
        e = lax.div(b, 2)
        m = lax.rem(b, 2)
        slot = lax.rem(b, RING)
        wslot = lax.rem(e, WQ_RING)

        @pl.when(m == 0)
        def _():
            load_wq(e).wait()
        for copy in load(b):
            copy.wait()
        rows = pl.ds(pl.multiple_of(m * ROWS, ROWS), ROWS)
        q = dot(hid[rows, :], wq[wslot])
        for t in range(BLOCK):
            place = pos_ref[b * BLOCK + t]
            lines = pl.ds(pl.multiple_of((place >> 2) * 16, 16), 16)
            put = sub16 == (place & 3)
            both = knv[pl.ds(pl.multiple_of((b * BLOCK + t) * 8, 8), 8), :]
            swapped = pltpu.roll(both, 4, 0)
            for n8, buf in ((jnp.where(low, both, swapped), kbuf), (jnp.where(low, swapped, both), vbuf)):
                n16 = jnp.concatenate([n8, n8], axis=0)
                old = buf[slot, t, lines, :].astype(F32)
                buf[slot, t, lines, :] = jnp.where(put, n16, old).astype(BF16)
        for k in range(2):
            picked = ids_ref[rows, k:k + 1] == e
            qsel[k, rows, :] = jnp.where(picked, q, qsel[k, rows, :])
        for copy in save(b):
            copy.start()

        @pl.when((m == 1) & (e + WQ_RING < EXPERTS))
        def _():
            load_wq(e + WQ_RING).start()

        @pl.when(b >= 2)
        def _():
            for copy in save(b - 2):
                copy.wait()

            @pl.when(b - 2 + RING < BLOCKS)
            def _():
                for copy in load(b - 2 + RING):
                    copy.start()
        return carry
    lax.fori_loop(0, BLOCKS, block_body, 0)

    def rope_body(m, carry):
        rows = pl.ds(pl.multiple_of(m * 128, 128), 128)
        cos = cos_s[rows, :]
        sin = sin_s[rows, :]
        for k in range(2):
            for h in range(HEADS):
                q = qsel[k, rows, h * 128:(h + 1) * 128]
                qrow[pl.ds(k * HEADS + h, 128, stride=8), :] = q * cos + pltpu.roll(q, 64, 1) * sin
        q = qrow[...]
        even = (iota((1024, HEAD_DIM), 0) & 8) == 0
        lines = pl.ds(pl.multiple_of(m * 1024, 1024), 1024)
        q_ref[lines, :HEAD_DIM] = jnp.where(even, q, 0.0).astype(BF16)
        q_ref[lines, HEAD_DIM:] = jnp.where(even, 0.0, q).astype(BF16)
        return carry
    lax.fori_loop(0, TOKENS // 128, rope_body, 0)
    for b in (BLOCKS - 2, BLOCKS - 1):
        for copy in save(jnp.int32(b)):
            copy.wait()


def project(positions, x, gain, table, pos_row, ids_t, router_t, w_kv, w_query, k_cache, v_cache):
    any_spec = pl.BlockSpec(memory_space=pl.ANY)
    vmem = pl.BlockSpec(memory_space=pltpu.VMEM)
    smem = pl.BlockSpec(memory_space=pltpu.SMEM)
    cache = jax.ShapeDtypeStruct(k_cache.shape, BF16)
    return pl.pallas_call(
        project_kernel,
        name='project',
        out_shape=(cache, cache, jax.ShapeDtypeStruct((TOKENS * 8, 2 * HEAD_DIM), BF16),
                   jax.ShapeDtypeStruct((TOKENS, EXPERTS), F32), jax.ShapeDtypeStruct((TOKENS, EXPERTS), jnp.int32)),
        in_specs=[smem] + [vmem] * 6 + [any_spec] * 4,
        out_specs=(any_spec, any_spec, vmem, vmem, vmem),
        scratch_shapes=[
            pltpu.VMEM((TOKENS, HIDDEN), BF16),
            pltpu.VMEM((HIDDEN * 8, 128), BF16),
            pltpu.VMEM((1024, 128), F32),
            pltpu.VMEM((HIDDEN, HEADS * 256), BF16),
            pltpu.VMEM((WQ_RING, HIDDEN, QUERY_COLS), BF16),
            pltpu.VMEM((RING, BLOCK, SLOTS * HEADS, HEAD_DIM), BF16),
            pltpu.VMEM((RING, BLOCK, SLOTS * HEADS, HEAD_DIM), BF16),
            pltpu.VMEM((2, TOKENS, QUERY_COLS), F32),
            pltpu.VMEM((1024, HEAD_DIM), F32),
            pltpu.VMEM((TOKENS * 8, HEAD_DIM), F32),
            pltpu.VMEM((TOKENS, HEAD_DIM), F32),
            pltpu.VMEM((TOKENS, HEAD_DIM), F32),
            pltpu.SemaphoreType.DMA,
            pltpu.SemaphoreType.DMA((WQ_RING,)),
            pltpu.SemaphoreType.DMA((RING,)),
            pltpu.SemaphoreType.DMA((RING,)),
            pltpu.SemaphoreType.DMA((RING,)),
            pltpu.SemaphoreType.DMA((RING,)),
        ],
        compiler_params=pltpu.CompilerParams(vmem_limit_bytes=VMEM_LIMIT),
    )(positions, x, gain, table, pos_row, ids_t, router_t, w_kv, w_query, k_cache, v_cache)


def reduce_columns(drive, partial, base_hbm, out_ref, base_ref, base_sem, send1, recv1, own, recv2, fin, recv3, s1, r1, s2, r2, s3, r3):
    chunks, height, width = send1.shape
    per = TOKENS // height
    half_width = HIDDEN // 2
    me = lax.axis_index('tp')
    core = lax.rem(me, 2)
    sibling = me + 1 - 2 * core
    partner = lax.rem(me + 2, 4)
    barrier = pltpu.get_barrier_semaphore()
    for peer in (sibling, partner):
        pl.semaphore_signal(barrier, inc=1, device_id={'tp': peer}, device_id_type=MESH)
    pl.semaphore_wait(barrier, 2)

    def column(s):
        half = lax.rem(core + 1 + s, 2)
        return pl.multiple_of(half * half_width + lax.div(s, 2) * width, width)

    def remote(src, dst, c, send, recv, peer):
        return pltpu.make_async_remote_copy(src_ref=src.at[c], dst_ref=dst.at[c], send_sem=send.at[c], recv_sem=recv.at[c],
                                            device_id={'tp': peer}, device_id_type=MESH)

    def to_sibling(c):
        return remote(send1, recv1, c, s1, r1, sibling)

    def to_partner(c):
        return remote(own, recv2, c, s2, r2, partner)

    def share(c):
        return remote(fin, recv3, c, s3, r3, sibling)

    def chunk_step(i, parity, m):
        s = 2 * i + parity
        rows = pl.ds(pl.multiple_of(m * height, height), height)
        chunk = per * i + m
        acc = partial(s, rows, column(s))
        if parity == 0:
            send1[chunk] = acc.astype(BF16)
            to_sibling(chunk).start()
        else:
            to_sibling(chunk).wait_recv()
            own[chunk] = (acc + recv1[chunk].astype(F32)).astype(BF16)
            to_partner(chunk).start()

    def place(c, half):
        rows = pl.ds(pl.multiple_of(lax.rem(c, per) * height, height), height)
        cols = pl.ds(pl.multiple_of(half * half_width + lax.div(c, per) * width, width), width)
        return rows, cols

    def finish(c):
        to_partner(c).wait_recv()
        rows, cols = place(c, core)
        total = own[c].astype(F32) + recv2[c].astype(F32)
        value = (base_ref[rows, cols].astype(F32) + total).astype(BF16)
        fin[c] = value
        share(c).start()
        out_ref[rows, cols] = value

    base_copy = pltpu.make_async_copy(base_hbm, base_ref, base_sem)
    finished = drive(chunk_step, column, finish, base_copy)

    def final_body(c, carry):
        finish(c)
        return carry
    lax.fori_loop(finished, chunks, final_body, 0)

    def gather_body(c, carry):
        share(c).wait_recv()
        rows, cols = place(c, 1 - core)
        out_ref[rows, cols] = recv3[c]
        return carry
    lax.fori_loop(0, chunks, gather_body, 0)

    def drain_body(c, carry):
        to_sibling(c).wait_send()
        to_partner(c).wait_send()
        share(c).wait_send()
        return carry
    lax.fori_loop(0, chunks, drain_body, 0)


def chunk_scratch(height, width):
    chunks = TOKENS * HIDDEN // 2 // (height * width)
    return ([pltpu.VMEM((TOKENS, HIDDEN), BF16), pltpu.SemaphoreType.DMA]
            + [pltpu.VMEM((chunks, height, width), BF16)] * 6 + [pltpu.SemaphoreType.DMA((chunks,))] * 6)


A_RING = 6
A_AHEAD = 4
A_ROWS = 128
PARTS = TOKENS // A_ROWS
PART_BLOCKS = A_ROWS // BLOCK


def attend_kernel(pos_ref, ids_ref, gates_ref, q_hbm, kc_hbm, vc_hbm, w_hbm, x_hbm, out_ref,
                  qbuf, kbuf, vbuf, probs, orow, mixed, spread, wbuf, q_sem, k_sem, v_sem, w_sem, *chunk_refs):
    def load(b):
        slot = lax.rem(b, A_RING)
        rows = pl.ds(pl.multiple_of(b * BLOCK, BLOCK), BLOCK)
        return (pltpu.make_async_copy(kc_hbm.at[rows], kbuf.at[slot], k_sem.at[slot]),
                pltpu.make_async_copy(vc_hbm.at[rows], vbuf.at[slot], v_sem.at[slot]))

    q_copy = pltpu.make_async_copy(q_hbm, qbuf, q_sem)
    q_copy.start()
    for b in range(A_AHEAD):
        for copy in load(jnp.int32(b)):
            copy.start()
    w_copies = [pltpu.make_async_copy(w_hbm.at[e], wbuf.at[e], w_sem.at[e]) for e in range(EXPERTS)]

    scale = HEAD_DIM ** -0.5
    row16 = iota((16, 128), 0)
    lane = iota((16, 128), 1)
    upper = row16 < 8
    same_head = (lane & 3) == (row16 & 3)
    slot_of = lane >> 2

    def attend_rows(m):
        def block_body(i, carry):
            b = m * PART_BLOCKS + jnp.minimum(i, PART_BLOCKS - 1)
            before = jnp.maximum(i - 1, 0)
            prev = m * PART_BLOCKS + before
            slot = lax.rem(b, A_RING)
            prev_slot = lax.rem(prev, A_RING)
            side = lax.rem(i, 2)

            @pl.when(i < PART_BLOCKS)
            def _():
                for copy in load(b):
                    copy.wait()

            def score(j):
                t = b * BLOCK + 2 * j
                q = qbuf[pl.ds(pl.multiple_of(t * 8, 16), 16), :]
                keys = jnp.concatenate([kbuf[slot, 2 * j], kbuf[slot, 2 * j + 1]], axis=1)
                s = dot_nt(q, keys) * scale
                s = jnp.where(same_head & (slot_of <= jnp.where(upper, pos_ref[t], pos_ref[t + 1])), s, NEG)
                e = jnp.exp(s - jnp.max(s, axis=1, keepdims=True))
                probs[side, j] = (e / jnp.sum(e, axis=1, keepdims=True)).astype(BF16)

            def mix(j):
                values = jnp.concatenate([vbuf[prev_slot, 2 * j], vbuf[prev_slot, 2 * j + 1]], axis=1)
                o = dot(probs[1 - side, j], values)
                orow[j * 16:j * 16 + 8, :] = o[:8, :HEAD_DIM]
                orow[j * 16 + 8:j * 16 + 16, :] = o[8:, HEAD_DIM:]

            pairs = BLOCK // 2
            for j in range(pairs // 2):
                score(j)
            for j in range(pairs // 2):
                mix(j)
            for j in range(pairs // 2, pairs):
                score(j)
            for j in range(pairs // 2, pairs):
                mix(j)
            rows = pl.ds(pl.multiple_of(before * BLOCK, BLOCK), BLOCK)
            for r in range(8):
                mixed[rows, r * 128:(r + 1) * 128] = orow[pl.ds(r, BLOCK, stride=8), :].astype(BF16)

            @pl.when((i < PART_BLOCKS) & (b + A_AHEAD < BLOCKS))
            def _():
                for copy in load(b + A_AHEAD):
                    copy.start()
            return carry
        lax.fori_loop(0, PART_BLOCKS + 1, block_body, 0)

        def spread_body(n, carry):
            rows = pl.ds(pl.multiple_of(n * 64, 64), 64)
            from_rows = pl.ds(pl.multiple_of(m * A_ROWS + n * 64, 64), 64)
            first = mixed[rows, :QUERY_COLS].astype(F32)
            second = mixed[rows, QUERY_COLS:].astype(F32)
            for e in range(EXPERTS):
                picked = jnp.where(ids_ref[from_rows, 0:1] == e, first, 0.0)
                picked = jnp.where(ids_ref[from_rows, 1:2] == e, second, picked)
                spread[e, rows, :] = picked.astype(BF16)
            return carry
        lax.fori_loop(0, A_ROWS // 64, spread_body, 0)

    def partial(s, rows, col):
        acc = jnp.zeros((A_ROWS, HIDDEN // 2), F32)
        for e in range(EXPERTS):
            acc = acc + gates_ref[rows, e:e + 1] * dot(spread[e], wbuf[e, :, pl.ds(col, HIDDEN // 2)])
        return acc

    def drive(chunk_step, column, finish, base_copy):
        q_copy.wait()
        for copy in w_copies:
            copy.start()

        def part_body(m, carry):
            attend_rows(m)

            @pl.when(m == 0)
            def _():
                base_copy.start()
                for copy in w_copies:
                    copy.wait()
            for parity in range(2):
                chunk_step(0, parity, m)

            @pl.when(m == 1)
            def _():
                base_copy.wait()

            @pl.when(m >= 2)
            def _():
                finish(m - 2)
            return carry
        lax.fori_loop(0, PARTS, part_body, 0)
        return PARTS - 2

    reduce_columns(drive, partial, x_hbm, out_ref, *chunk_refs)


def attend(positions, ids, gates, q, k_cache, v_cache, w_out, x):
    vmem = pl.BlockSpec(memory_space=pltpu.VMEM)
    any_spec = pl.BlockSpec(memory_space=pl.ANY)
    return pl.pallas_call(
        attend_kernel,
        name='attend',
        out_shape=jax.ShapeDtypeStruct((TOKENS, HIDDEN), BF16),
        in_specs=[pl.BlockSpec(memory_space=pltpu.SMEM)] + [vmem] * 2 + [any_spec] * 5,
        out_specs=vmem,
        scratch_shapes=[
            pltpu.VMEM((TOKENS * 8, 2 * HEAD_DIM), BF16),
            pltpu.VMEM((A_RING, BLOCK, SLOTS * HEADS, HEAD_DIM), BF16),
            pltpu.VMEM((A_RING, BLOCK, SLOTS * HEADS, HEAD_DIM), BF16),
            pltpu.VMEM((2, BLOCK // 2, 16, HEAD_DIM), BF16),
            pltpu.VMEM((BLOCK * 8, HEAD_DIM), F32),
            pltpu.VMEM((A_ROWS, 2 * QUERY_COLS), BF16),
            pltpu.VMEM((EXPERTS, A_ROWS, QUERY_COLS), BF16),
            pltpu.VMEM((EXPERTS, QUERY_COLS, HIDDEN), BF16),
            pltpu.SemaphoreType.DMA,
            pltpu.SemaphoreType.DMA((A_RING,)),
            pltpu.SemaphoreType.DMA((A_RING,)),
            pltpu.SemaphoreType.DMA((EXPERTS,)),
        ] + chunk_scratch(A_ROWS, HIDDEN // 2),
        compiler_params=pltpu.CompilerParams(vmem_limit_bytes=VMEM_LIMIT, collective_id=0, has_side_effects=True),
    )(positions, ids, gates, q, k_cache, v_cache, w_out, x)


def gate_up_kernel(x_ref, gain_ref, router_ref, idst_ref, wg_hbm, wu_hbm, wd_hbm, a_hbm, gates_ref, early_ref,
                   unorm, picked, scatter, gathered, wg, wu, wd, act, abuf, early_rows, wg_sem, wu_sem, wd_sem, a_sem):
    first_id = lax.axis_index('tp') * LOCAL
    core = lax.rem(lax.axis_index('tp'), 2)

    def load(s):
        e = lax.div(s, F_TILES)
        cols = pl.ds(pl.multiple_of(lax.rem(s, F_TILES) * FT, FT), FT)
        slot = lax.rem(s, W_RING)
        return (pltpu.make_async_copy(wg_hbm.at[e, :, cols], wg.at[slot], wg_sem.at[slot]),
                pltpu.make_async_copy(wu_hbm.at[e, :, cols], wu.at[slot], wu_sem.at[slot]),
                down_of(e, cols, slot, 0), down_of(e, cols, slot, 1))

    def down_of(e, rows, slot, j):
        half = lax.rem(core + 1 + j, 2)
        cols = pl.ds(pl.multiple_of(half * (HIDDEN // 2), HIDDEN // 2), COL)
        return pltpu.make_async_copy(wd_hbm.at[e, rows, cols], wd.at[slot, j], wd_sem.at[slot, j])

    def save(s):
        e = lax.div(s, F_TILES)
        cols = pl.ds(pl.multiple_of(lax.rem(s, F_TILES) * FT, FT), FT)
        slot = lax.rem(s, 2)
        return pltpu.make_async_copy(abuf.at[slot], a_hbm.at[e, :, cols], a_sem.at[slot])

    for s in range(W_RING):
        for copy in load(jnp.int32(s)):
            copy.start()

    norm_rows(x_ref, gain_ref, unorm)
    ids = turn((idst_ref[0:1, :], idst_ref[1:2, :]))
    id0 = ids[:, 0:1]
    id1 = ids[:, 1:2]
    logits = dot_nt(unorm[...], router_ref[...])
    g0, g1 = pair_gates(logits, id0, id1)
    lane8 = iota((TOKENS, EXPERTS), 1)
    local8 = lane8 + first_id
    gates_ref[...] = jnp.where(local8 == id0, g0, 0.0) + jnp.where(local8 == id1, g1, 0.0)

    before = iota((TOKENS, TOKENS), 0)
    after = iota((TOKENS, TOKENS), 1)
    lower = jnp.where(after < before, 1.0, 0.0).astype(BF16)
    upper = jnp.where(before < after, 1.0, 0.0).astype(BF16)
    lane_id = iota((TOKENS, 128), 1) + first_id
    mask_col = jnp.where((lane_id == id0) | (lane_id == id1), 1.0, 0.0)
    rank_col = dot(lower, mask_col.astype(BF16))
    sub_id = iota((8, TOKENS), 0) + first_id
    mask_row = jnp.where((sub_id == idst_ref[0:1, :]) | (sub_id == idst_ref[1:2, :]), 1.0, 0.0)
    rank_row = dot(mask_row.astype(BF16), upper)
    counts = []
    for e in range(LOCAL):
        counts.append(jnp.sum(mask_row[e:e + 1, :]).astype(jnp.int32))
        where_col = jnp.where(mask_col[:, e:e + 1] > 0.0, rank_col[:, e:e + 1], -1.0)
        where_row = jnp.where(mask_row[e:e + 1, :] > 0.0, rank_row[e:e + 1, :], -1.0)
        scatter[e] = jnp.where(after.astype(F32) == where_col, 1.0, 0.0).astype(BF16)
        picked[e] = jnp.where(before.astype(F32) == where_row, 1.0, 0.0).astype(BF16)
    blocks = [lax.div(n + (RB - 1), RB) for n in counts]

    for e in range(LOCAL):
        def gather_body(rb, carry):
            rows = pl.ds(pl.multiple_of(rb * RB, RB), RB)
            gathered[e, rows, :] = dot(picked[e, rows, :], unorm[...]).astype(BF16)
            return carry
        lax.fori_loop(0, blocks[e], gather_body, 0)

    early_rows[...] = jnp.zeros_like(early_rows)

    def step_body(s, carry):
        e = lax.div(s, F_TILES)
        slot = lax.rem(s, W_RING)
        out_slot = lax.rem(s, 2)
        for copy in load(s):
            copy.wait()

        @pl.when(s >= 2)
        def _():
            save(s - 2).wait()

        def run(count):
            for n in range(FT // COL):
                cols = slice(n * COL, (n + 1) * COL)
                gate = dot(gathered[e, :count, :], wg[slot, :, cols])
                up = dot(gathered[e, :count, :], wu[slot, :, cols])
                act[:count, cols] = (gate * (1.0 / (1.0 + jnp.exp(-gate))) * up).astype(BF16)
            for j in range(2):
                cols = slice(j * COL, (j + 1) * COL)
                early_rows[e, :count, cols] += dot(act[:count, :], wd[slot, j])
            for m in range(TOKENS // ROWS):
                rows = slice(m * ROWS, (m + 1) * ROWS)
                abuf[out_slot, rows, :] = dot(scatter[e, rows, :count], act[:count, :]).astype(BF16)

        n_rows = jnp.where(e == 0, counts[0], counts[1])
        n_steps = jnp.maximum(lax.div(n_rows + 63, 64), 2)
        for k in range(2, TOKENS // 64 + 1):
            pl.when(n_steps == k)(functools.partial(run, k * 64))

        @pl.when(s + W_RING < MLP_STEPS)
        def _():
            for copy in load(s + W_RING):
                copy.start()
        save(s).start()
        return carry
    lax.fori_loop(0, MLP_STEPS, step_body, 0)

    def early_body(m, carry):
        rows = pl.ds(pl.multiple_of(m * ROWS, ROWS), ROWS)
        for j in range(2):
            total = jnp.zeros((ROWS, COL), F32)
            for e in range(LOCAL):
                z = early_rows[e, :, j * COL:(j + 1) * COL]
                high = z.astype(BF16)
                rest = (z - high.astype(F32)).astype(BF16)
                mine = dot(scatter[e, rows, :], high) + dot(scatter[e, rows, :], rest)
                total = total + gates_ref[rows, e:e + 1] * mine
            early_ref[j, rows, :] = total
        return carry
    lax.fori_loop(0, TOKENS // ROWS, early_body, 0)
    for s in (MLP_STEPS - 2, MLP_STEPS - 1):
        save(jnp.int32(s)).wait()


def gate_up(x_mid, gain, router_t, ids_t, w_gate, w_up, w_down):
    any_spec = pl.BlockSpec(memory_space=pl.ANY)
    vmem = pl.BlockSpec(memory_space=pltpu.VMEM)
    return pl.pallas_call(
        gate_up_kernel,
        name='gate_up',
        out_shape=(jax.ShapeDtypeStruct((LOCAL, TOKENS, FFN), BF16), jax.ShapeDtypeStruct((TOKENS, EXPERTS), F32),
                   jax.ShapeDtypeStruct((2, TOKENS, COL), F32)),
        in_specs=[vmem] * 4 + [any_spec] * 3,
        out_specs=(any_spec, vmem, vmem),
        scratch_shapes=[
            pltpu.VMEM((TOKENS, HIDDEN), BF16),
            pltpu.VMEM((LOCAL, TOKENS, TOKENS), BF16),
            pltpu.VMEM((LOCAL, TOKENS, TOKENS), BF16),
            pltpu.VMEM((LOCAL, TOKENS, HIDDEN), BF16),
            pltpu.VMEM((W_RING, HIDDEN, FT), BF16),
            pltpu.VMEM((W_RING, HIDDEN, FT), BF16),
            pltpu.VMEM((W_RING, 2, FT, COL), BF16),
            pltpu.VMEM((TOKENS, FT), BF16),
            pltpu.VMEM((2, TOKENS, FT), BF16),
            pltpu.VMEM((LOCAL, TOKENS, 2 * COL), F32),
            pltpu.SemaphoreType.DMA((W_RING,)),
            pltpu.SemaphoreType.DMA((W_RING,)),
            pltpu.SemaphoreType.DMA((W_RING, 2)),
            pltpu.SemaphoreType.DMA((2,)),
        ],
        compiler_params=pltpu.CompilerParams(vmem_limit_bytes=VMEM_LIMIT),
    )(x_mid, gain, router_t, ids_t, w_gate, w_up, w_down)


DOWN_RING = 2


def down_kernel(gates_ref, early_ref, x_hbm, a_hbm, w_hbm, out_ref, abuf, wbuf, first_part, a_sem, w_sem, *chunk_refs):
    me = lax.axis_index('tp')
    core = lax.rem(me, 2)

    def copy_of(s, col, e):
        slot = lax.rem(s, DOWN_RING)
        return pltpu.make_async_copy(w_hbm.at[e, :, pl.ds(col, COL)], wbuf.at[slot, e], w_sem.at[slot, e])

    def ahead(s, e):
        half = lax.rem(core + 1 + s, 2)
        return copy_of(jnp.int32(s), pl.multiple_of((half * (STEPS // 2) + s // 2) * COL, COL), e)

    a_copies = [pltpu.make_async_copy(a_hbm.at[e], abuf.at[e], a_sem.at[e]) for e in range(LOCAL)]
    for e in range(LOCAL):
        a_copies[e].start()
        ahead(2, e).start()

    def partial(s, rows, col):
        if isinstance(s, int):
            return early_ref[s, rows, :]
        return first_part[rows, :] + gates_ref[rows, 1:2] * dot(abuf[1, rows, :], wbuf[lax.rem(s, DOWN_RING), 1])

    def drive(chunk_step, column, finish, base_copy):
        for m in range(TOKENS // ROWS):
            for parity in range(2):
                chunk_step(0, parity, m)
        a_copies[0].wait()
        for e in range(LOCAL):
            ahead(3, e).start()
        base_copy.start()

        def col_body(i, carry):
            for parity in range(2):
                s = 2 * i + parity
                slot = lax.rem(s, DOWN_RING)
                copy_of(s, column(s), 0).wait()
                first_part[...] = gates_ref[:, 0:1] * dot(abuf[0], wbuf[slot, 0])
                if parity == 0:
                    @pl.when(i == 1)
                    def _():
                        a_copies[1].wait()
                copy_of(s, column(s), 1).wait()

                def row_body(m, c):
                    chunk_step(i, parity, m)
                    return c
                lax.fori_loop(0, TOKENS // ROWS, row_body, 0)

                @pl.when(s + DOWN_RING < STEPS)
                def _():
                    for e in range(LOCAL):
                        copy_of(s + DOWN_RING, column(s + DOWN_RING), e).start()

            @pl.when(i == 1)
            def _():
                base_copy.wait()

            @pl.when(i >= 2)
            def _():
                finish(2 * (i - 2))
                finish(2 * (i - 2) + 1)
            return carry
        lax.fori_loop(1, STEPS // 2, col_body, 0)
        return CHUNKS // 2

    reduce_columns(drive, partial, x_hbm, out_ref, *chunk_refs)


def down_project(gates, early, x_mid, act, w_down):
    vmem = pl.BlockSpec(memory_space=pltpu.VMEM)
    any_spec = pl.BlockSpec(memory_space=pl.ANY)
    return pl.pallas_call(
        down_kernel,
        name='down_project',
        out_shape=jax.ShapeDtypeStruct((TOKENS, HIDDEN), BF16),
        in_specs=[vmem] * 2 + [any_spec] * 3,
        out_specs=vmem,
        scratch_shapes=[
            pltpu.VMEM((LOCAL, TOKENS, FFN), BF16),
            pltpu.VMEM((DOWN_RING, LOCAL, FFN, COL), BF16),
            pltpu.VMEM((TOKENS, COL), F32),
            pltpu.SemaphoreType.DMA((LOCAL,)),
            pltpu.SemaphoreType.DMA((DOWN_RING, LOCAL)),
        ] + chunk_scratch(ROWS, COL),
        compiler_params=pltpu.CompilerParams(vmem_limit_bytes=VMEM_LIMIT, collective_id=1, has_side_effects=True),
    )(gates, early, x_mid, act, w_down)


PIECES = 8


def hand_over_kernel(x_hbm, out_hbm, buf, in_sem, out_sem):
    def rows(i):
        return pl.ds(i * (TOKENS // PIECES), TOKENS // PIECES)
    reads = [pltpu.make_async_copy(x_hbm.at[rows(i)], buf.at[i], in_sem.at[i]) for i in range(PIECES)]
    writes = [pltpu.make_async_copy(buf.at[i], out_hbm.at[rows(i)], out_sem.at[i]) for i in range(PIECES)]
    for copy in reads:
        copy.start()
    for read, write in zip(reads, writes):
        read.wait()
        write.start()
    for copy in writes:
        copy.wait()


def hand_over(x):
    any_spec = pl.BlockSpec(memory_space=pl.ANY)
    return pl.pallas_call(
        hand_over_kernel,
        name='hand_over',
        out_shape=jax.ShapeDtypeStruct(x.shape, x.dtype),
        in_specs=[any_spec],
        out_specs=any_spec,
        scratch_shapes=[pltpu.VMEM((PIECES, TOKENS // PIECES, HIDDEN), BF16), pltpu.SemaphoreType.DMA((PIECES,)), pltpu.SemaphoreType.DMA((PIECES,))],
        compiler_params=pltpu.CompilerParams(vmem_limit_bytes=VMEM_LIMIT),
    )(x)


def rope_table():
    half = HEAD_DIM // 2
    inv_freq = np.float32(ROPE_BASE) ** (-(np.arange(half, dtype=np.float32) * np.float32(2.0) / np.float32(HEAD_DIM)))
    angles = np.arange(SLOTS, dtype=np.float32)[:, None] * inv_freq[None, :].astype(np.float32)
    cos = np.cos(angles.astype(np.float64))
    sin = np.sin(angles.astype(np.float64))
    full = np.concatenate([cos, cos, -sin, sin], axis=1).astype(np.float32)
    parts = []
    for _ in range(3):
        part = full.astype(BF16)
        parts.append(part)
        full = full - part.astype(np.float32)
    parts.append(np.zeros_like(parts[0]))
    return np.concatenate(parts, axis=0)


def solution(mesh):
    table = rope_table()

    def local_step(x, k_cache, v_cache, positions, att_ids, mlp_ids, norm_att, w_kv, router_att, w_query, w_out, norm_mlp, router_mlp, w_gate, w_up, w_down):
        flat = (TOKENS, SLOTS * HEADS, HEAD_DIM)
        kv_rows = w_kv.reshape(HIDDEN, HEADS, 2, HEAD_DIM).transpose(0, 2, 1, 3).reshape(HIDDEN * 8, HEAD_DIM)
        k_new, v_new, q, att_gates, att_cols = project(
            positions, x, norm_att.reshape(1, HIDDEN), jnp.asarray(table), positions.reshape(1, TOKENS), att_ids.T, router_att.T,
            kv_rows, w_query, k_cache.reshape(flat), v_cache.reshape(flat))
        x_mid = attend(positions, att_cols, att_gates, q, k_new, v_new, w_out, x)
        act, mlp_gates, early = gate_up(x_mid, norm_mlp.reshape(1, HIDDEN), router_mlp.T, mlp_ids.T, w_gate, w_up, w_down)
        x_out = hand_over(down_project(mlp_gates, early, x_mid, act, w_down))
        return x_out, k_new.reshape(k_cache.shape), v_new.reshape(v_cache.shape)

    token_spec = P('dp', None)
    cache_spec = P('dp', None, 'tp', None)
    expert_spec = P('tp', None, None)
    in_specs = (token_spec, cache_spec, cache_spec, P('dp'), token_spec, token_spec, P(), P(None, 'tp', None), P(), P(None, None, 'tp'), P(None, 'tp', None), P(), P(), expert_spec, expert_spec, expert_spec)
    out_specs = (token_spec, cache_spec, cache_spec)
    return jax.shard_map(local_step, mesh=mesh, in_specs=in_specs, out_specs=out_specs, check_vma=False)
```

```python
import functools

import jax
import jax.numpy as jnp
import numpy as np
from jax import lax
from jax.experimental import pallas as pl
from jax.experimental.pallas import tpu as pltpu
from jax.sharding import PartitionSpec as P

NORM_EPS = 1e-6
ROPE_BASE = 10000.0
F32 = jnp.float32
BF16 = jnp.bfloat16
NEG = -1e30
MESH = pl.DeviceIdType.MESH
VMEM_LIMIT = 62 * 1024 * 1024

TOKENS = 512
HIDDEN = 2048
HEADS = 4
HEAD_DIM = 128
SLOTS = 32
QUERY_COLS = HEADS * HEAD_DIM
EXPERTS = 8
FFN = 5632
LOCAL = 2

BLOCK = 32
RING = 8
BLOCKS = TOKENS // BLOCK
GROUP = 8
WQ_RING = 3

COL = 256
ROWS = 256
STEPS = HIDDEN // COL
CHUNKS = STEPS // 2 * (TOKENS // ROWS)

FT = 512
F_TILES = FFN // FT
MLP_STEPS = LOCAL * F_TILES
W_RING = 5
RB = 128


def dot(a, b):
    return jnp.dot(a, b, preferred_element_type=F32)


def iota(shape, dim):
    return lax.broadcasted_iota(jnp.int32, shape, dim)


def norm_rows(x_ref, gain_ref, out_ref):
    def body(i, carry):
        rows = pl.ds(pl.multiple_of(i * 32, 32), 32)
        values = x_ref[rows, :].astype(F32)
        inv = lax.rsqrt(jnp.mean(values * values, axis=-1, keepdims=True) + NORM_EPS)
        out_ref[rows, :] = (values * inv * gain_ref[...]).astype(BF16)
        return carry
    lax.fori_loop(0, TOKENS // 32, body, 0)


def pair_gates(logits, id0, id1):
    lane = iota(logits.shape, 1)
    first = jnp.sum(jnp.where(lane == id0, logits, 0.0), axis=1, keepdims=True)
    second = jnp.sum(jnp.where(lane == id1, logits, 0.0), axis=1, keepdims=True)
    top = jnp.maximum(first, second)
    e0 = jnp.exp(first - top)
    e1 = jnp.exp(second - top)
    total = e0 + e1
    return e0 / total, e1 / total


def turn(rows):
    sub = iota((8, TOKENS), 0)
    stacked = jnp.zeros((8, TOKENS), F32)
    for i, row in enumerate(rows):
        stacked = jnp.where(sub == i, row.astype(F32), stacked)
    return jnp.transpose(stacked).astype(jnp.int32)


def dot_nt(a, b):
    return lax.dot_general(a, b, (((1,), (1,)), ((), ())), preferred_element_type=F32)


def project_kernel(pos_ref, x_ref, gain_ref, table_ref, posrow_ref, idst_ref, router_ref, wkv_hbm, wq_hbm, kc_hbm, vc_hbm,
                   ko_hbm, vo_hbm, q_ref, gates_ref, ids_ref,
                   hid, wraw, wtmp, wkv, wq, kbuf, vbuf, qsel, qrow, knv, cos_s, sin_s,
                   wkv_sem, wq_sem, kin_sem, vin_sem, kout_sem, vout_sem):
    def block_of(ref, b):
        return ref.at[pl.ds(pl.multiple_of(b * BLOCK, BLOCK), BLOCK)]

    def load(b):
        slot = lax.rem(b, RING)
        return (pltpu.make_async_copy(block_of(kc_hbm, b), kbuf.at[slot], kin_sem.at[slot]),
                pltpu.make_async_copy(block_of(vc_hbm, b), vbuf.at[slot], vin_sem.at[slot]))

    def save(b):
        slot = lax.rem(b, RING)
        return (pltpu.make_async_copy(kbuf.at[slot], block_of(ko_hbm, b), kout_sem.at[slot]),
                pltpu.make_async_copy(vbuf.at[slot], block_of(vo_hbm, b), vout_sem.at[slot]))

    def load_wq(e):
        slot = lax.rem(e, WQ_RING)
        return pltpu.make_async_copy(wq_hbm.at[e], wq.at[slot], wq_sem.at[slot])

    kv_copy = pltpu.make_async_copy(wkv_hbm, wraw, wkv_sem)
    kv_copy.start()
    for b in range(3):
        for copy in load(jnp.int32(b)):
            copy.start()
    load_wq(jnp.int32(0)).start()

    norm_rows(x_ref, gain_ref, hid)
    for e in range(1, WQ_RING):
        load_wq(jnp.int32(e)).start()
    for b in range(3, RING):
        for copy in load(jnp.int32(b)):
            copy.start()
    ids = turn((idst_ref[0:1, :], idst_ref[1:2, :], posrow_ref[...]))
    ids_ref[...] = ids
    id0 = ids[:, 0:1]
    id1 = ids[:, 1:2]
    lane128 = iota((TOKENS, 128), 1)
    chosen = ((lane128 & 31) == ids[:, 2:3]) & (lane128 < 3 * SLOTS)
    trig = dot(jnp.where(chosen, 1.0, 0.0).astype(BF16), table_ref[...])
    cos_s[...] = trig[:, :HEAD_DIM]
    sin_s[...] = trig[:, HEAD_DIM:]
    logits = dot_nt(hid[...], router_ref[...])
    g0, g1 = pair_gates(logits, id0, id1)
    lane8 = iota((TOKENS, EXPERTS), 1)
    gates_ref[...] = jnp.where(lane8 == id0, g0, 0.0) + jnp.where(lane8 == id1, g1, 0.0)
    kv_copy.wait()

    def sort_body(i, carry):
        wtmp[...] = wraw[pl.ds(pl.multiple_of(i * 1024, 1024), 1024), :].astype(F32)
        rows = pl.ds(pl.multiple_of(i * 128, 128), 128)
        for j in range(8):
            wkv[rows, j * 128:(j + 1) * 128] = wtmp[pl.ds(j, 128, stride=8), :].astype(BF16)
        return carry
    lax.fori_loop(0, HIDDEN // 128, sort_body, 0)

    def kv_body(m, carry):
        rows = pl.ds(pl.multiple_of(m * ROWS, ROWS), ROWS)
        kv = dot(hid[rows, :], wkv[...])
        cos = cos_s[rows, :]
        sin = sin_s[rows, :]
        for h in range(HEADS):
            k = kv[:, h * 128:(h + 1) * 128]
            knv[pl.ds(m * (ROWS * 8) + h, ROWS, stride=8), :] = k * cos + pltpu.roll(k, 64, 1) * sin
            knv[pl.ds(m * (ROWS * 8) + h + 4, ROWS, stride=8), :] = kv[:, (h + 4) * 128:(h + 5) * 128]
        return carry
    lax.fori_loop(0, TOKENS // ROWS, kv_body, 0)

    sub16 = iota((16, HEAD_DIM), 0) >> 2
    low = iota((8, 128), 0) < 4

    def block_body(b, carry):
        e = lax.div(b, 2)
        m = lax.rem(b, 2)
        slot = lax.rem(b, RING)
        wslot = lax.rem(e, WQ_RING)

        @pl.when(m == 0)
        def _():
            load_wq(e).wait()
        for copy in load(b):
            copy.wait()
        rows = pl.ds(pl.multiple_of(m * ROWS, ROWS), ROWS)
        q = dot(hid[rows, :], wq[wslot])
        for t in range(BLOCK):
            place = pos_ref[b * BLOCK + t]
            lines = pl.ds(pl.multiple_of((place >> 2) * 16, 16), 16)
            put = sub16 == (place & 3)
            both = knv[pl.ds(pl.multiple_of((b * BLOCK + t) * 8, 8), 8), :]
            swapped = pltpu.roll(both, 4, 0)
            for n8, buf in ((jnp.where(low, both, swapped), kbuf), (jnp.where(low, swapped, both), vbuf)):
                n16 = jnp.concatenate([n8, n8], axis=0)
                old = buf[slot, t, lines, :].astype(F32)
                buf[slot, t, lines, :] = jnp.where(put, n16, old).astype(BF16)
        for k in range(2):
            picked = ids_ref[rows, k:k + 1] == e
            qsel[k, rows, :] = jnp.where(picked, q, qsel[k, rows, :])
        for copy in save(b):
            copy.start()

        @pl.when((m == 1) & (e + WQ_RING < EXPERTS))
        def _():
            load_wq(e + WQ_RING).start()

        @pl.when(b >= 2)
        def _():
            for copy in save(b - 2):
                copy.wait()

            @pl.when(b - 2 + RING < BLOCKS)
            def _():
                for copy in load(b - 2 + RING):
                    copy.start()
        return carry
    lax.fori_loop(0, BLOCKS, block_body, 0)

    def rope_body(m, carry):
        rows = pl.ds(pl.multiple_of(m * 128, 128), 128)
        cos = cos_s[rows, :]
        sin = sin_s[rows, :]
        for k in range(2):
            for h in range(HEADS):
                q = qsel[k, rows, h * 128:(h + 1) * 128]
                qrow[pl.ds(k * HEADS + h, 128, stride=8), :] = q * cos + pltpu.roll(q, 64, 1) * sin
        q = qrow[...]
        even = (iota((1024, HEAD_DIM), 0) & 8) == 0
        lines = pl.ds(pl.multiple_of(m * 1024, 1024), 1024)
        q_ref[lines, :HEAD_DIM] = jnp.where(even, q, 0.0).astype(BF16)
        q_ref[lines, HEAD_DIM:] = jnp.where(even, 0.0, q).astype(BF16)
        return carry
    lax.fori_loop(0, TOKENS // 128, rope_body, 0)
    for b in (BLOCKS - 2, BLOCKS - 1):
        for copy in save(jnp.int32(b)):
            copy.wait()


def project(positions, x, gain, table, pos_row, ids_t, router_t, w_kv, w_query, k_cache, v_cache):
    any_spec = pl.BlockSpec(memory_space=pl.ANY)
    vmem = pl.BlockSpec(memory_space=pltpu.VMEM)
    smem = pl.BlockSpec(memory_space=pltpu.SMEM)
    cache = jax.ShapeDtypeStruct(k_cache.shape, BF16)
    return pl.pallas_call(
        project_kernel,
        name='project',
        out_shape=(cache, cache, jax.ShapeDtypeStruct((TOKENS * 8, 2 * HEAD_DIM), BF16),
                   jax.ShapeDtypeStruct((TOKENS, EXPERTS), F32), jax.ShapeDtypeStruct((TOKENS, EXPERTS), jnp.int32)),
        in_specs=[smem] + [vmem] * 6 + [any_spec] * 4,
        out_specs=(any_spec, any_spec, vmem, vmem, vmem),
        scratch_shapes=[
            pltpu.VMEM((TOKENS, HIDDEN), BF16),
            pltpu.VMEM((HIDDEN * 8, 128), BF16),
            pltpu.VMEM((1024, 128), F32),
            pltpu.VMEM((HIDDEN, HEADS * 256), BF16),
            pltpu.VMEM((WQ_RING, HIDDEN, QUERY_COLS), BF16),
            pltpu.VMEM((RING, BLOCK, SLOTS * HEADS, HEAD_DIM), BF16),
            pltpu.VMEM((RING, BLOCK, SLOTS * HEADS, HEAD_DIM), BF16),
            pltpu.VMEM((2, TOKENS, QUERY_COLS), F32),
            pltpu.VMEM((1024, HEAD_DIM), F32),
            pltpu.VMEM((TOKENS * 8, HEAD_DIM), F32),
            pltpu.VMEM((TOKENS, HEAD_DIM), F32),
            pltpu.VMEM((TOKENS, HEAD_DIM), F32),
            pltpu.SemaphoreType.DMA,
            pltpu.SemaphoreType.DMA((WQ_RING,)),
            pltpu.SemaphoreType.DMA((RING,)),
            pltpu.SemaphoreType.DMA((RING,)),
            pltpu.SemaphoreType.DMA((RING,)),
            pltpu.SemaphoreType.DMA((RING,)),
        ],
        compiler_params=pltpu.CompilerParams(vmem_limit_bytes=VMEM_LIMIT),
    )(positions, x, gain, table, pos_row, ids_t, router_t, w_kv, w_query, k_cache, v_cache)


def reduce_columns(drive, partial, rows_outer, base_hbm, out_hbm, base_ref, base_sem, send1, recv1, own, recv2, fin, recv3, s1, r1, s2, r2, s3, r3, o1, o2):
    chunks, height, width = send1.shape
    per = TOKENS // height
    columns = chunks // per
    half_width = HIDDEN // 2
    me = lax.axis_index('tp')
    core = lax.rem(me, 2)
    sibling = me + 1 - 2 * core
    partner = lax.rem(me + 2, 4)
    barrier = pltpu.get_barrier_semaphore()
    for peer in (sibling, partner):
        pl.semaphore_signal(barrier, inc=1, device_id={'tp': peer}, device_id_type=MESH)
    pl.semaphore_wait(barrier, 2)

    def column(s):
        half = lax.rem(core + 1 + s, 2)
        return pl.multiple_of(half * half_width + lax.div(s, 2) * width, width)

    def remote(src, dst, c, send, recv, peer):
        return pltpu.make_async_remote_copy(src_ref=src.at[c], dst_ref=dst.at[c], send_sem=send.at[c], recv_sem=recv.at[c],
                                            device_id={'tp': peer}, device_id_type=MESH)

    def to_sibling(c):
        return remote(send1, recv1, c, s1, r1, sibling)

    def to_partner(c):
        return remote(own, recv2, c, s2, r2, partner)

    def share(c):
        return remote(fin, recv3, c, s3, r3, sibling)

    def chunk_step(i, parity, m):
        s = 2 * i + parity
        rows = pl.ds(pl.multiple_of(m * height, height), height)
        chunk = columns * m + i if rows_outer else per * i + m
        acc = partial(s, rows, column(s))
        if parity == 0:
            send1[chunk] = acc.astype(BF16)
            to_sibling(chunk).start()
        else:
            to_sibling(chunk).wait_recv()
            own[chunk] = (acc + recv1[chunk].astype(F32)).astype(BF16)
            to_partner(chunk).start()

    def place(c, half):
        m, i = (lax.div(c, columns), lax.rem(c, columns)) if rows_outer else (lax.rem(c, per), lax.div(c, per))
        rows = pl.ds(pl.multiple_of(m * height, height), height)
        cols = pl.ds(pl.multiple_of(half * half_width + i * width, width), width)
        return rows, cols

    def write(src, c, half, sem):
        rows, cols = place(c, half)
        return pltpu.make_async_copy(src.at[c], out_hbm.at[rows, cols], sem.at[c])

    def finish(c):
        to_partner(c).wait_recv()
        rows, cols = place(c, core)
        total = own[c].astype(F32) + recv2[c].astype(F32)
        value = (base_ref[rows, cols].astype(F32) + total).astype(BF16)
        fin[c] = value
        share(c).start()
        write(fin, c, core, o1).start()

    base_copy = pltpu.make_async_copy(base_hbm, base_ref, base_sem)
    finished = drive(chunk_step, column, finish, base_copy)

    def final_body(c, carry):
        finish(c)
        return carry
    lax.fori_loop(finished, chunks, final_body, 0)

    def gather_body(c, carry):
        share(c).wait_recv()
        write(recv3, c, 1 - core, o2).start()
        return carry
    lax.fori_loop(0, chunks, gather_body, 0)

    def drain_body(c, carry):
        to_sibling(c).wait_send()
        to_partner(c).wait_send()
        share(c).wait_send()
        write(fin, c, core, o1).wait()
        write(recv3, c, 1 - core, o2).wait()
        return carry
    lax.fori_loop(0, chunks, drain_body, 0)


def chunk_scratch(height, width):
    chunks = TOKENS * HIDDEN // 2 // (height * width)
    return ([pltpu.VMEM((TOKENS, HIDDEN), BF16), pltpu.SemaphoreType.DMA]
            + [pltpu.VMEM((chunks, height, width), BF16)] * 6 + [pltpu.SemaphoreType.DMA((chunks,))] * 8)


A_RING = 6
A_AHEAD = 4
A_ROWS = 128
PARTS = TOKENS // A_ROWS
PART_BLOCKS = A_ROWS // BLOCK


A_COLS = 512
A_PIECES = HIDDEN // 2 // A_COLS


def attend_kernel(pos_ref, ids_ref, gates_ref, q_hbm, kc_hbm, vc_hbm, w_hbm, x_hbm, out_hbm,
                  qbuf, kbuf, vbuf, probs, orow, mixed, spread, wbuf, q_sem, k_sem, v_sem, w_sem, *chunk_refs):
    core = lax.rem(lax.axis_index('tp'), 2)

    def load(b):
        slot = lax.rem(b, A_RING)
        rows = pl.ds(pl.multiple_of(b * BLOCK, BLOCK), BLOCK)
        return (pltpu.make_async_copy(kc_hbm.at[rows], kbuf.at[slot], k_sem.at[slot]),
                pltpu.make_async_copy(vc_hbm.at[rows], vbuf.at[slot], v_sem.at[slot]))

    def load_q(part):
        rows = pl.ds(pl.multiple_of(part * A_ROWS * 8, A_ROWS * 8), A_ROWS * 8)
        return pltpu.make_async_copy(q_hbm.at[rows], qbuf.at[rows], q_sem.at[part])

    def load_w(i, parity):
        half = lax.rem(core + 1 + parity, 2)
        cols = pl.ds(pl.multiple_of(half * (HIDDEN // 2) + i * A_COLS, A_COLS), A_COLS)
        return [pltpu.make_async_copy(w_hbm.at[e, :, cols], wbuf.at[e, :, cols], w_sem.at[2 * i + parity, e]) for e in range(EXPERTS)]

    load_q(0).start()
    for b in range(2):
        for copy in load(jnp.int32(b)):
            copy.start()

    scale = HEAD_DIM ** -0.5
    row16 = iota((16, 128), 0)
    lane = iota((16, 128), 1)
    upper = row16 < 8
    same_head = (lane & 3) == (row16 & 3)
    slot_of = lane >> 2

    def block_step(g, carry):
        b = jnp.minimum(g, BLOCKS - 1)
        prev = jnp.maximum(g - 1, 0)
        slot = lax.rem(b, A_RING)
        prev_slot = lax.rem(prev, A_RING)
        side = lax.rem(g, 2)

        @pl.when(g < BLOCKS)
        def _():
            @pl.when(lax.rem(g, PART_BLOCKS) == 0)
            def _():
                load_q(lax.div(g, PART_BLOCKS)).wait()
            for copy in load(b):
                copy.wait()

            @pl.when(g == 0)
            def _():
                for n in range(2, A_AHEAD):
                    for copy in load(jnp.int32(n)):
                        copy.start()
                for parity in range(2):
                    for copy in load_w(0, parity):
                        copy.start()

            @pl.when(g == 1)
            def _():
                for i in range(1, A_PIECES):
                    for parity in range(2):
                        for copy in load_w(i, parity):
                            copy.start()
                for part in range(1, PARTS):
                    load_q(part).start()

        def score(j):
            t = b * BLOCK + 2 * j
            q = qbuf[pl.ds(pl.multiple_of(t * 8, 16), 16), :]
            keys = jnp.concatenate([kbuf[slot, 2 * j], kbuf[slot, 2 * j + 1]], axis=1)
            s = dot_nt(q, keys) * scale
            s = jnp.where(same_head & (slot_of <= jnp.where(upper, pos_ref[t], pos_ref[t + 1])), s, NEG)
            e = jnp.exp(s - jnp.max(s, axis=1, keepdims=True))
            probs[side, j] = (e / jnp.sum(e, axis=1, keepdims=True)).astype(BF16)

        def mix(j):
            values = jnp.concatenate([vbuf[prev_slot, 2 * j], vbuf[prev_slot, 2 * j + 1]], axis=1)
            o = dot(probs[1 - side, j], values)
            orow[j * 16:j * 16 + 8, :] = o[:8, :HEAD_DIM]
            orow[j * 16 + 8:j * 16 + 16, :] = o[8:, HEAD_DIM:]

        pairs = BLOCK // 2
        for j in range(pairs // 2):
            score(j)
        for j in range(pairs // 2):
            mix(j)
        for j in range(pairs // 2, pairs):
            score(j)
        for j in range(pairs // 2, pairs):
            mix(j)
        rows = pl.ds(pl.multiple_of(lax.rem(prev, PART_BLOCKS) * BLOCK, BLOCK), BLOCK)
        for r in range(8):
            mixed[rows, r * 128:(r + 1) * 128] = orow[pl.ds(r, BLOCK, stride=8), :].astype(BF16)

        @pl.when((g < BLOCKS) & (b + A_AHEAD < BLOCKS))
        def _():
            for copy in load(b + A_AHEAD):
                copy.start()
        return carry

    def spread_part(m):
        def spread_body(n, carry):
            rows = pl.ds(pl.multiple_of(n * 64, 64), 64)
            from_rows = pl.ds(pl.multiple_of(m * A_ROWS + n * 64, 64), 64)
            first = mixed[rows, :QUERY_COLS].astype(F32)
            second = mixed[rows, QUERY_COLS:].astype(F32)
            for e in range(EXPERTS):
                picked = jnp.where(ids_ref[from_rows, 0:1] == e, first, 0.0)
                picked = jnp.where(ids_ref[from_rows, 1:2] == e, second, picked)
                spread[e, rows, :] = picked.astype(BF16)
            return carry
        lax.fori_loop(0, A_ROWS // 64, spread_body, 0)

    def partial(s, rows, col):
        acc = jnp.zeros((A_ROWS, A_COLS), F32)
        for e in range(EXPERTS):
            acc = acc + gates_ref[rows, e:e + 1] * dot(spread[e], wbuf[e, :, pl.ds(col, A_COLS)])
        return acc

    def drive(chunk_step, column, finish, base_copy):
        def part_body(m, carry):
            lax.fori_loop(jnp.where(m == 0, 0, m * PART_BLOCKS + 1), (m + 1) * PART_BLOCKS + 1, block_step, 0)
            spread_part(m)
            for i in range(A_PIECES):
                for parity in range(2):
                    @pl.when(m == 0)
                    def _():
                        for copy in load_w(i, parity):
                            copy.wait()
                    chunk_step(i, parity, m)

            @pl.when(m == 0)
            def _():
                base_copy.start()

            @pl.when(m == 1)
            def _():
                base_copy.wait()

            @pl.when(m >= 2)
            def _():
                for i in range(A_PIECES):
                    finish((m - 2) * A_PIECES + i)
            return carry
        lax.fori_loop(0, PARTS, part_body, 0)
        return (PARTS - 2) * A_PIECES

    reduce_columns(drive, partial, True, x_hbm, out_hbm, *chunk_refs)


def attend(positions, ids, gates, q, k_cache, v_cache, w_out, x):
    vmem = pl.BlockSpec(memory_space=pltpu.VMEM)
    any_spec = pl.BlockSpec(memory_space=pl.ANY)
    return pl.pallas_call(
        attend_kernel,
        name='attend',
        out_shape=jax.ShapeDtypeStruct((TOKENS, HIDDEN), BF16),
        in_specs=[pl.BlockSpec(memory_space=pltpu.SMEM)] + [vmem] * 2 + [any_spec] * 5,
        out_specs=any_spec,
        scratch_shapes=[
            pltpu.VMEM((TOKENS * 8, 2 * HEAD_DIM), BF16),
            pltpu.VMEM((A_RING, BLOCK, SLOTS * HEADS, HEAD_DIM), BF16),
            pltpu.VMEM((A_RING, BLOCK, SLOTS * HEADS, HEAD_DIM), BF16),
            pltpu.VMEM((2, BLOCK // 2, 16, HEAD_DIM), BF16),
            pltpu.VMEM((BLOCK * 8, HEAD_DIM), F32),
            pltpu.VMEM((A_ROWS, 2 * QUERY_COLS), BF16),
            pltpu.VMEM((EXPERTS, A_ROWS, QUERY_COLS), BF16),
            pltpu.VMEM((EXPERTS, QUERY_COLS, HIDDEN), BF16),
            pltpu.SemaphoreType.DMA((PARTS,)),
            pltpu.SemaphoreType.DMA((A_RING,)),
            pltpu.SemaphoreType.DMA((A_RING,)),
            pltpu.SemaphoreType.DMA((2 * A_PIECES, EXPERTS)),
        ] + chunk_scratch(A_ROWS, A_COLS),
        compiler_params=pltpu.CompilerParams(vmem_limit_bytes=VMEM_LIMIT, collective_id=0, has_side_effects=True),
    )(positions, ids, gates, q, k_cache, v_cache, w_out, x)


def gate_up_kernel(x_ref, gain_ref, router_ref, idst_ref, wg_hbm, wu_hbm, wd_hbm, a_hbm, gates_ref, early_ref,
                   unorm, picked, scatter, gathered, wg, wu, wd, act, abuf, early_rows, wg_sem, wu_sem, wd_sem, a_sem):
    first_id = lax.axis_index('tp') * LOCAL
    core = lax.rem(lax.axis_index('tp'), 2)

    def load(s):
        e = lax.div(s, F_TILES)
        cols = pl.ds(pl.multiple_of(lax.rem(s, F_TILES) * FT, FT), FT)
        slot = lax.rem(s, W_RING)
        return (pltpu.make_async_copy(wg_hbm.at[e, :, cols], wg.at[slot], wg_sem.at[slot]),
                pltpu.make_async_copy(wu_hbm.at[e, :, cols], wu.at[slot], wu_sem.at[slot]),
                down_of(e, cols, slot, 0), down_of(e, cols, slot, 1))

    def down_of(e, rows, slot, j):
        half = lax.rem(core + 1 + j, 2)
        cols = pl.ds(pl.multiple_of(half * (HIDDEN // 2), HIDDEN // 2), COL)
        return pltpu.make_async_copy(wd_hbm.at[e, rows, cols], wd.at[slot, j], wd_sem.at[slot, j])

    def save(s):
        e = lax.div(s, F_TILES)
        cols = pl.ds(pl.multiple_of(lax.rem(s, F_TILES) * FT, FT), FT)
        slot = lax.rem(s, 2)
        return pltpu.make_async_copy(abuf.at[slot], a_hbm.at[e, :, cols], a_sem.at[slot])

    for s in range(W_RING):
        for copy in load(jnp.int32(s)):
            copy.start()

    norm_rows(x_ref, gain_ref, unorm)
    ids = turn((idst_ref[0:1, :], idst_ref[1:2, :]))
    id0 = ids[:, 0:1]
    id1 = ids[:, 1:2]
    logits = dot_nt(unorm[...], router_ref[...])
    g0, g1 = pair_gates(logits, id0, id1)
    lane8 = iota((TOKENS, EXPERTS), 1)
    local8 = lane8 + first_id
    gates_ref[...] = jnp.where(local8 == id0, g0, 0.0) + jnp.where(local8 == id1, g1, 0.0)

    before = iota((TOKENS, TOKENS), 0)
    after = iota((TOKENS, TOKENS), 1)
    lower = jnp.where(after < before, 1.0, 0.0).astype(BF16)
    upper = jnp.where(before < after, 1.0, 0.0).astype(BF16)
    lane_id = iota((TOKENS, 128), 1) + first_id
    mask_col = jnp.where((lane_id == id0) | (lane_id == id1), 1.0, 0.0)
    rank_col = dot(lower, mask_col.astype(BF16))
    sub_id = iota((8, TOKENS), 0) + first_id
    mask_row = jnp.where((sub_id == idst_ref[0:1, :]) | (sub_id == idst_ref[1:2, :]), 1.0, 0.0)
    rank_row = dot(mask_row.astype(BF16), upper)
    counts = []
    for e in range(LOCAL):
        counts.append(jnp.sum(mask_row[e:e + 1, :]).astype(jnp.int32))
        where_col = jnp.where(mask_col[:, e:e + 1] > 0.0, rank_col[:, e:e + 1], -1.0)
        where_row = jnp.where(mask_row[e:e + 1, :] > 0.0, rank_row[e:e + 1, :], -1.0)
        scatter[e] = jnp.where(after.astype(F32) == where_col, 1.0, 0.0).astype(BF16)
        picked[e] = jnp.where(before.astype(F32) == where_row, 1.0, 0.0).astype(BF16)
    blocks = [lax.div(n + (RB - 1), RB) for n in counts]

    for e in range(LOCAL):
        def gather_body(rb, carry):
            rows = pl.ds(pl.multiple_of(rb * RB, RB), RB)
            gathered[e, rows, :] = dot(picked[e, rows, :], unorm[...]).astype(BF16)
            return carry
        lax.fori_loop(0, blocks[e], gather_body, 0)

    early_rows[...] = jnp.zeros_like(early_rows)

    def step_body(s, carry):
        e = lax.div(s, F_TILES)
        slot = lax.rem(s, W_RING)
        out_slot = lax.rem(s, 2)
        for copy in load(s):
            copy.wait()

        @pl.when(s >= 2)
        def _():
            save(s - 2).wait()

        def run(count):
            for n in range(FT // COL):
                cols = slice(n * COL, (n + 1) * COL)
                gate = dot(gathered[e, :count, :], wg[slot, :, cols])
                up = dot(gathered[e, :count, :], wu[slot, :, cols])
                act[:count, cols] = (gate * (1.0 / (1.0 + jnp.exp(-gate))) * up).astype(BF16)
            for j in range(2):
                cols = slice(j * COL, (j + 1) * COL)
                early_rows[e, :count, cols] += dot(act[:count, :], wd[slot, j])
            for m in range(TOKENS // ROWS):
                rows = slice(m * ROWS, (m + 1) * ROWS)
                abuf[out_slot, rows, :] = dot(scatter[e, rows, :count], act[:count, :]).astype(BF16)

        n_rows = jnp.where(e == 0, counts[0], counts[1])
        n_steps = jnp.maximum(lax.div(n_rows + 63, 64), 2)
        for k in range(2, TOKENS // 64 + 1):
            pl.when(n_steps == k)(functools.partial(run, k * 64))

        @pl.when(s + W_RING < MLP_STEPS)
        def _():
            for copy in load(s + W_RING):
                copy.start()
        save(s).start()
        return carry
    lax.fori_loop(0, MLP_STEPS, step_body, 0)

    def early_body(m, carry):
        rows = pl.ds(pl.multiple_of(m * ROWS, ROWS), ROWS)
        for j in range(2):
            total = jnp.zeros((ROWS, COL), F32)
            for e in range(LOCAL):
                z = early_rows[e, :, j * COL:(j + 1) * COL]
                high = z.astype(BF16)
                rest = (z - high.astype(F32)).astype(BF16)
                mine = dot(scatter[e, rows, :], high) + dot(scatter[e, rows, :], rest)
                total = total + gates_ref[rows, e:e + 1] * mine
            early_ref[j, rows, :] = total
        return carry
    lax.fori_loop(0, TOKENS // ROWS, early_body, 0)
    for s in (MLP_STEPS - 2, MLP_STEPS - 1):
        save(jnp.int32(s)).wait()


def gate_up(x_mid, gain, router_t, ids_t, w_gate, w_up, w_down):
    any_spec = pl.BlockSpec(memory_space=pl.ANY)
    vmem = pl.BlockSpec(memory_space=pltpu.VMEM)
    return pl.pallas_call(
        gate_up_kernel,
        name='gate_up',
        out_shape=(jax.ShapeDtypeStruct((LOCAL, TOKENS, FFN), BF16), jax.ShapeDtypeStruct((TOKENS, EXPERTS), F32),
                   jax.ShapeDtypeStruct((2, TOKENS, COL), F32)),
        in_specs=[vmem] * 4 + [any_spec] * 3,
        out_specs=(any_spec, vmem, vmem),
        scratch_shapes=[
            pltpu.VMEM((TOKENS, HIDDEN), BF16),
            pltpu.VMEM((LOCAL, TOKENS, TOKENS), BF16),
            pltpu.VMEM((LOCAL, TOKENS, TOKENS), BF16),
            pltpu.VMEM((LOCAL, TOKENS, HIDDEN), BF16),
            pltpu.VMEM((W_RING, HIDDEN, FT), BF16),
            pltpu.VMEM((W_RING, HIDDEN, FT), BF16),
            pltpu.VMEM((W_RING, 2, FT, COL), BF16),
            pltpu.VMEM((TOKENS, FT), BF16),
            pltpu.VMEM((2, TOKENS, FT), BF16),
            pltpu.VMEM((LOCAL, TOKENS, 2 * COL), F32),
            pltpu.SemaphoreType.DMA((W_RING,)),
            pltpu.SemaphoreType.DMA((W_RING,)),
            pltpu.SemaphoreType.DMA((W_RING, 2)),
            pltpu.SemaphoreType.DMA((2,)),
        ],
        compiler_params=pltpu.CompilerParams(vmem_limit_bytes=VMEM_LIMIT),
    )(x_mid, gain, router_t, ids_t, w_gate, w_up, w_down)


DOWN_RING = 2


def down_kernel(gates_ref, early_ref, x_hbm, a_hbm, w_hbm, out_hbm, abuf, wbuf, first_part, a_sem, w_sem, *chunk_refs):
    me = lax.axis_index('tp')
    core = lax.rem(me, 2)

    def copy_of(s, col, e):
        slot = lax.rem(s, DOWN_RING)
        return pltpu.make_async_copy(w_hbm.at[e, :, pl.ds(col, COL)], wbuf.at[slot, e], w_sem.at[slot, e])

    def ahead(s, e):
        half = lax.rem(core + 1 + s, 2)
        return copy_of(jnp.int32(s), pl.multiple_of((half * (STEPS // 2) + s // 2) * COL, COL), e)

    a_copies = [pltpu.make_async_copy(a_hbm.at[e], abuf.at[e], a_sem.at[e]) for e in range(LOCAL)]
    a_copies[0].start()
    ahead(2, 0).start()

    def partial(s, rows, col):
        if isinstance(s, int):
            return early_ref[s, rows, :]
        return first_part[rows, :] + gates_ref[rows, 1:2] * dot(abuf[1, rows, :], wbuf[lax.rem(s, DOWN_RING), 1])

    def drive(chunk_step, column, finish, base_copy):
        for m in range(TOKENS // ROWS):
            for parity in range(2):
                chunk_step(0, parity, m)
        a_copies[0].wait()
        ahead(2, 0).wait()
        a_copies[1].start()
        ahead(2, 1).start()
        for e in range(LOCAL):
            ahead(3, e).start()
        base_copy.start()

        def col_body(i, carry):
            for parity in range(2):
                s = 2 * i + parity
                slot = lax.rem(s, DOWN_RING)
                if parity == 0:
                    @pl.when(i > 1)
                    def _():
                        copy_of(s, column(s), 0).wait()
                else:
                    copy_of(s, column(s), 0).wait()
                first_part[...] = gates_ref[:, 0:1] * dot(abuf[0], wbuf[slot, 0])
                if parity == 0:
                    @pl.when(i == 1)
                    def _():
                        a_copies[1].wait()
                copy_of(s, column(s), 1).wait()

                def row_body(m, c):
                    chunk_step(i, parity, m)
                    return c
                lax.fori_loop(0, TOKENS // ROWS, row_body, 0)

                @pl.when(s + DOWN_RING < STEPS)
                def _():
                    for e in range(LOCAL):
                        copy_of(s + DOWN_RING, column(s + DOWN_RING), e).start()

            @pl.when(i == 1)
            def _():
                base_copy.wait()

            @pl.when(i >= 2)
            def _():
                finish(2 * (i - 2))
                finish(2 * (i - 2) + 1)
            return carry
        lax.fori_loop(1, STEPS // 2, col_body, 0)
        return CHUNKS // 2

    reduce_columns(drive, partial, False, x_hbm, out_hbm, *chunk_refs)


def down_project(gates, early, x_mid, act, w_down):
    vmem = pl.BlockSpec(memory_space=pltpu.VMEM)
    any_spec = pl.BlockSpec(memory_space=pl.ANY)
    return pl.pallas_call(
        down_kernel,
        name='down_project',
        out_shape=jax.ShapeDtypeStruct((TOKENS, HIDDEN), BF16),
        in_specs=[vmem] * 2 + [any_spec] * 3,
        out_specs=any_spec,
        scratch_shapes=[
            pltpu.VMEM((LOCAL, TOKENS, FFN), BF16),
            pltpu.VMEM((DOWN_RING, LOCAL, FFN, COL), BF16),
            pltpu.VMEM((TOKENS, COL), F32),
            pltpu.SemaphoreType.DMA((LOCAL,)),
            pltpu.SemaphoreType.DMA((DOWN_RING, LOCAL)),
        ] + chunk_scratch(ROWS, COL),
        compiler_params=pltpu.CompilerParams(vmem_limit_bytes=VMEM_LIMIT, collective_id=1, has_side_effects=True),
    )(gates, early, x_mid, act, w_down)


PIECES = 8


def hand_over_kernel(x_hbm, out_hbm, buf, in_sem, out_sem):
    def rows(i):
        return pl.ds(i * (TOKENS // PIECES), TOKENS // PIECES)
    reads = [pltpu.make_async_copy(x_hbm.at[rows(i)], buf.at[i], in_sem.at[i]) for i in range(PIECES)]
    writes = [pltpu.make_async_copy(buf.at[i], out_hbm.at[rows(i)], out_sem.at[i]) for i in range(PIECES)]
    for copy in reads:
        copy.start()
    for read, write in zip(reads, writes):
        read.wait()
        write.start()
    for copy in writes:
        copy.wait()


def hand_over(x):
    any_spec = pl.BlockSpec(memory_space=pl.ANY)
    return pl.pallas_call(
        hand_over_kernel,
        name='hand_over',
        out_shape=jax.ShapeDtypeStruct(x.shape, x.dtype),
        in_specs=[any_spec],
        out_specs=any_spec,
        scratch_shapes=[pltpu.VMEM((PIECES, TOKENS // PIECES, HIDDEN), BF16), pltpu.SemaphoreType.DMA((PIECES,)), pltpu.SemaphoreType.DMA((PIECES,))],
        compiler_params=pltpu.CompilerParams(vmem_limit_bytes=VMEM_LIMIT),
    )(x)


def rope_table():
    half = HEAD_DIM // 2
    inv_freq = np.float32(ROPE_BASE) ** (-(np.arange(half, dtype=np.float32) * np.float32(2.0) / np.float32(HEAD_DIM)))
    angles = np.arange(SLOTS, dtype=np.float32)[:, None] * inv_freq[None, :].astype(np.float32)
    cos = np.cos(angles.astype(np.float64))
    sin = np.sin(angles.astype(np.float64))
    full = np.concatenate([cos, cos, -sin, sin], axis=1).astype(np.float32)
    parts = []
    for _ in range(3):
        part = full.astype(BF16)
        parts.append(part)
        full = full - part.astype(np.float32)
    parts.append(np.zeros_like(parts[0]))
    return np.concatenate(parts, axis=0)


def solution(mesh):
    table = rope_table()

    def local_step(x, k_cache, v_cache, positions, att_ids, mlp_ids, norm_att, w_kv, router_att, w_query, w_out, norm_mlp, router_mlp, w_gate, w_up, w_down):
        flat = (TOKENS, SLOTS * HEADS, HEAD_DIM)
        kv_rows = w_kv.reshape(HIDDEN, HEADS, 2, HEAD_DIM).transpose(0, 2, 1, 3).reshape(HIDDEN * 8, HEAD_DIM)
        k_new, v_new, q, att_gates, att_cols = project(
            positions, x, norm_att.reshape(1, HIDDEN), jnp.asarray(table), positions.reshape(1, TOKENS), att_ids.T, router_att.T,
            kv_rows, w_query, k_cache.reshape(flat), v_cache.reshape(flat))
        x_mid = attend(positions, att_cols, att_gates, q, k_new, v_new, w_out, x)
        act, mlp_gates, early = gate_up(x_mid, norm_mlp.reshape(1, HIDDEN), router_mlp.T, mlp_ids.T, w_gate, w_up, w_down)
        x_out = hand_over(down_project(mlp_gates, early, x_mid, act, w_down))
        return x_out, k_new.reshape(k_cache.shape), v_new.reshape(v_cache.shape)

    token_spec = P('dp', None)
    cache_spec = P('dp', None, 'tp', None)
    expert_spec = P('tp', None, None)
    in_specs = (token_spec, cache_spec, cache_spec, P('dp'), token_spec, token_spec, P(), P(None, 'tp', None), P(), P(None, None, 'tp'), P(None, 'tp', None), P(), P(), expert_spec, expert_spec, expert_spec)
    out_specs = (token_spec, cache_spec, cache_spec)
    return jax.shard_map(local_step, mesh=mesh, in_specs=in_specs, out_specs=out_specs, check_vma=False)
```

```python
import functools

import jax
import jax.numpy as jnp
import numpy as np
from jax import lax
from jax.experimental import pallas as pl
from jax.experimental.pallas import tpu as pltpu
from jax.sharding import PartitionSpec as P

NORM_EPS = 1e-6
ROPE_BASE = 10000.0
F32 = jnp.float32
BF16 = jnp.bfloat16
NEG = -1e30
MESH = pl.DeviceIdType.MESH
VMEM_LIMIT = 62 * 1024 * 1024

TOKENS = 512
HIDDEN = 2048
HEADS = 4
HEAD_DIM = 128
SLOTS = 32
QUERY_COLS = HEADS * HEAD_DIM
EXPERTS = 8
FFN = 5632
LOCAL = 2

BLOCK = 32
RING = 8
BLOCKS = TOKENS // BLOCK
GROUP = 8
WQ_RING = 3

COL = 256
ROWS = 256
STEPS = HIDDEN // COL
CHUNKS = STEPS // 2 * (TOKENS // ROWS)

FT = 512
F_TILES = FFN // FT
MLP_STEPS = LOCAL * F_TILES
W_RING = 5
RB = 128


def dot(a, b):
    return jnp.dot(a, b, preferred_element_type=F32)


def iota(shape, dim):
    return lax.broadcasted_iota(jnp.int32, shape, dim)


def norm_rows(x_ref, gain_ref, out_ref):
    def body(i, carry):
        rows = pl.ds(pl.multiple_of(i * 32, 32), 32)
        values = x_ref[rows, :].astype(F32)
        inv = lax.rsqrt(jnp.mean(values * values, axis=-1, keepdims=True) + NORM_EPS)
        out_ref[rows, :] = (values * inv * gain_ref[...]).astype(BF16)
        return carry
    lax.fori_loop(0, TOKENS // 32, body, 0)


def pair_gates(logits, id0, id1):
    lane = iota(logits.shape, 1)
    first = jnp.sum(jnp.where(lane == id0, logits, 0.0), axis=1, keepdims=True)
    second = jnp.sum(jnp.where(lane == id1, logits, 0.0), axis=1, keepdims=True)
    top = jnp.maximum(first, second)
    e0 = jnp.exp(first - top)
    e1 = jnp.exp(second - top)
    total = e0 + e1
    return e0 / total, e1 / total


def turn(rows):
    sub = iota((8, TOKENS), 0)
    stacked = jnp.zeros((8, TOKENS), F32)
    for i, row in enumerate(rows):
        stacked = jnp.where(sub == i, row.astype(F32), stacked)
    return jnp.transpose(stacked).astype(jnp.int32)


def dot_nt(a, b):
    return lax.dot_general(a, b, (((1,), (1,)), ((), ())), preferred_element_type=F32)


def attend_kernel(pos_ref, x_ref, gain_ref, table_ref, posrow_ref, idst_ref, router_ref, wkv_hbm, wq_hbm, kc_hbm, vc_hbm,
                  ko_hbm, vo_hbm, o_ref, gates_ref, ids_ref,
                  hid, wraw, wtmp, wkv, wq, kbuf, vbuf, qsel, qrow, qdiag, knv, probs, orow, cos_s, sin_s,
                  wkv_sem, wq_sem, kin_sem, vin_sem, kout_sem, vout_sem):
    def block_of(ref, b):
        return ref.at[pl.ds(pl.multiple_of(b * BLOCK, BLOCK), BLOCK)]

    def load(b):
        slot = lax.rem(b, RING)
        return (pltpu.make_async_copy(block_of(kc_hbm, b), kbuf.at[slot], kin_sem.at[slot]),
                pltpu.make_async_copy(block_of(vc_hbm, b), vbuf.at[slot], vin_sem.at[slot]))

    def save(b):
        slot = lax.rem(b, RING)
        return (pltpu.make_async_copy(kbuf.at[slot], block_of(ko_hbm, b), kout_sem.at[slot]),
                pltpu.make_async_copy(vbuf.at[slot], block_of(vo_hbm, b), vout_sem.at[slot]))

    def load_wq(e):
        slot = lax.rem(e, WQ_RING)
        return pltpu.make_async_copy(wq_hbm.at[e], wq.at[slot], wq_sem.at[slot])

    kv_copy = pltpu.make_async_copy(wkv_hbm, wraw, wkv_sem)
    kv_copy.start()
    for b in range(3):
        for copy in load(jnp.int32(b)):
            copy.start()
    load_wq(jnp.int32(0)).start()

    norm_rows(x_ref, gain_ref, hid)
    for e in range(1, WQ_RING):
        load_wq(jnp.int32(e)).start()
    ids = turn((idst_ref[0:1, :], idst_ref[1:2, :], posrow_ref[...]))
    ids_ref[...] = ids
    id0 = ids[:, 0:1]
    id1 = ids[:, 1:2]
    lane128 = iota((TOKENS, 128), 1)
    chosen = ((lane128 & 31) == ids[:, 2:3]) & (lane128 < 3 * SLOTS)
    trig = dot(jnp.where(chosen, 1.0, 0.0).astype(BF16), table_ref[...])
    cos_s[...] = trig[:, :HEAD_DIM]
    sin_s[...] = trig[:, HEAD_DIM:]
    logits = dot_nt(hid[...], router_ref[...])
    g0, g1 = pair_gates(logits, id0, id1)
    lane8 = iota((TOKENS, EXPERTS), 1)
    gates_ref[...] = jnp.where(lane8 == id0, g0, 0.0) + jnp.where(lane8 == id1, g1, 0.0)
    kv_copy.wait()

    def sort_body(i, carry):
        wtmp[...] = wraw[pl.ds(pl.multiple_of(i * 1024, 1024), 1024), :].astype(F32)
        rows = pl.ds(pl.multiple_of(i * 128, 128), 128)
        for j in range(8):
            wkv[rows, j * 128:(j + 1) * 128] = wtmp[pl.ds(j, 128, stride=8), :].astype(BF16)
        return carry
    lax.fori_loop(0, HIDDEN // 128, sort_body, 0)

    def kv_body(m, carry):
        rows = pl.ds(pl.multiple_of(m * ROWS, ROWS), ROWS)
        kv = dot(hid[rows, :], wkv[...])
        cos = cos_s[rows, :]
        sin = sin_s[rows, :]
        for h in range(HEADS):
            k = kv[:, h * 128:(h + 1) * 128]
            knv[pl.ds(m * (ROWS * 8) + h, ROWS, stride=8), :] = k * cos + pltpu.roll(k, 64, 1) * sin
            knv[pl.ds(m * (ROWS * 8) + h + 4, ROWS, stride=8), :] = kv[:, (h + 4) * 128:(h + 5) * 128]
        return carry
    lax.fori_loop(0, TOKENS // ROWS, kv_body, 0)

    def q_body(e, carry):
        @pl.when(e + 3 < RING)
        def _():
            for copy in load(e + 3):
                copy.start()
        load_wq(e).wait()
        slot = lax.rem(e, WQ_RING)

        def m_body(m, c):
            rows = pl.ds(pl.multiple_of(m * ROWS, ROWS), ROWS)
            q = dot(hid[rows, :], wq[slot])
            for k in range(2):
                picked = ids_ref[rows, k:k + 1] == e
                qsel[k, rows, :] = jnp.where(picked, q, qsel[k, rows, :])
            return c
        lax.fori_loop(0, TOKENS // ROWS, m_body, 0)

        @pl.when(e + WQ_RING < EXPERTS)
        def _():
            load_wq(e + WQ_RING).start()
        return carry
    lax.fori_loop(0, EXPERTS, q_body, 0)

    def rope_body(m, carry):
        rows = pl.ds(pl.multiple_of(m * 128, 128), 128)
        cos = cos_s[rows, :]
        sin = sin_s[rows, :]
        for k in range(2):
            for h in range(HEADS):
                q = qsel[k, rows, h * 128:(h + 1) * 128]
                qrow[pl.ds(k * HEADS + h, 128, stride=8), :] = q * cos + pltpu.roll(q, 64, 1) * sin
        q = qrow[...]
        even = (iota((1024, HEAD_DIM), 0) & 8) == 0
        lines = pl.ds(pl.multiple_of(m * 1024, 1024), 1024)
        qdiag[lines, :HEAD_DIM] = jnp.where(even, q, 0.0).astype(BF16)
        qdiag[lines, HEAD_DIM:] = jnp.where(even, 0.0, q).astype(BF16)
        return carry
    lax.fori_loop(0, TOKENS // 128, rope_body, 0)

    scale = HEAD_DIM ** -0.5
    sub16 = iota((16, HEAD_DIM), 0) >> 2
    low = iota((8, 128), 0) < 4
    row16 = iota((16, 128), 0)
    lane = iota((16, 128), 1)
    upper = row16 < 8
    same_head = (lane & 3) == (row16 & 3)
    slot_of = lane >> 2

    def block_body(i, carry):
        b = jnp.minimum(i, BLOCKS - 1)
        prev = jnp.maximum(i - 1, 0)
        slot = lax.rem(b, RING)
        prev_slot = lax.rem(prev, RING)
        side = lax.rem(i, 2)

        @pl.when(i < BLOCKS)
        def _():
            for copy in load(b):
                copy.wait()
        places = [pos_ref[b * BLOCK + t] for t in range(BLOCK)]

        def patch(t):
            rows = pl.ds(pl.multiple_of((places[t] >> 2) * 16, 16), 16)
            put = sub16 == (places[t] & 3)
            both = knv[pl.ds(pl.multiple_of((b * BLOCK + t) * 8, 8), 8), :]
            swapped = pltpu.roll(both, 4, 0)
            for n8, buf in ((jnp.where(low, both, swapped), kbuf), (jnp.where(low, swapped, both), vbuf)):
                n16 = jnp.concatenate([n8, n8], axis=0)
                old = buf[slot, t, rows, :].astype(F32)
                buf[slot, t, rows, :] = jnp.where(put, n16, old).astype(BF16)

        def score(j):
            t = b * BLOCK + 2 * j
            q = qdiag[pl.ds(pl.multiple_of(t * 8, 16), 16), :]
            keys = jnp.concatenate([kbuf[slot, 2 * j], kbuf[slot, 2 * j + 1]], axis=1)
            s = dot_nt(q, keys) * scale
            s = jnp.where(same_head & (slot_of <= jnp.where(upper, places[2 * j], places[2 * j + 1])), s, NEG)
            e = jnp.exp(s - jnp.max(s, axis=1, keepdims=True))
            probs[side, j] = (e / jnp.sum(e, axis=1, keepdims=True)).astype(BF16)

        def mix(j):
            values = jnp.concatenate([vbuf[prev_slot, 2 * j], vbuf[prev_slot, 2 * j + 1]], axis=1)
            o = dot(probs[1 - side, j], values)
            orow[j * 16:j * 16 + 8, :] = o[:8, :HEAD_DIM]
            orow[j * 16 + 8:j * 16 + 16, :] = o[8:, HEAD_DIM:]

        half = BLOCK // 2
        pairs = BLOCK // 2
        first, second = range(pairs // 2), range(pairs // 2, pairs)
        for t in range(half):
            patch(t)
        for j in first:
            score(j)
        for t in range(half, BLOCK):
            patch(t)
        for j in first:
            mix(j)
        for j in second:
            score(j)
        for j in second:
            mix(j)
        rows = pl.ds(pl.multiple_of(prev * BLOCK, BLOCK), BLOCK)
        for r in range(8):
            o_ref[rows, r * 128:(r + 1) * 128] = orow[pl.ds(r, BLOCK, stride=8), :].astype(BF16)

        @pl.when(i >= 1)
        def _():
            for copy in save(prev):
                copy.start()

        @pl.when(i >= 3)
        def _():
            for copy in save(i - 3):
                copy.wait()

            @pl.when(i - 3 + RING < BLOCKS)
            def _():
                for copy in load(i - 3 + RING):
                    copy.start()
        return carry
    lax.fori_loop(0, BLOCKS + 1, block_body, 0)
    for b in (BLOCKS - 2, BLOCKS - 1):
        for copy in save(jnp.int32(b)):
            copy.wait()


def attend(positions, x, gain, table, pos_row, ids_t, router_t, w_kv, w_query, k_cache, v_cache):
    any_spec = pl.BlockSpec(memory_space=pl.ANY)
    vmem = pl.BlockSpec(memory_space=pltpu.VMEM)
    smem = pl.BlockSpec(memory_space=pltpu.SMEM)
    cache = jax.ShapeDtypeStruct(k_cache.shape, BF16)
    return pl.pallas_call(
        attend_kernel,
        name='attend',
        out_shape=(cache, cache, jax.ShapeDtypeStruct((TOKENS, 2 * QUERY_COLS), BF16),
                   jax.ShapeDtypeStruct((TOKENS, EXPERTS), F32), jax.ShapeDtypeStruct((TOKENS, EXPERTS), jnp.int32)),
        in_specs=[smem] + [vmem] * 6 + [any_spec] * 4,
        out_specs=(any_spec, any_spec, vmem, vmem, vmem),
        scratch_shapes=[
            pltpu.VMEM((TOKENS, HIDDEN), BF16),
            pltpu.VMEM((HIDDEN * 8, 128), BF16),
            pltpu.VMEM((1024, 128), F32),
            pltpu.VMEM((HIDDEN, HEADS * 256), BF16),
            pltpu.VMEM((WQ_RING, HIDDEN, QUERY_COLS), BF16),
            pltpu.VMEM((RING, BLOCK, SLOTS * HEADS, HEAD_DIM), BF16),
            pltpu.VMEM((RING, BLOCK, SLOTS * HEADS, HEAD_DIM), BF16),
            pltpu.VMEM((2, TOKENS, QUERY_COLS), F32),
            pltpu.VMEM((1024, HEAD_DIM), F32),
            pltpu.VMEM((TOKENS * 8, 2 * HEAD_DIM), BF16),
            pltpu.VMEM((TOKENS * 8, HEAD_DIM), F32),
            pltpu.VMEM((2, BLOCK // 2, 16, HEAD_DIM), BF16),
            pltpu.VMEM((BLOCK * 8, HEAD_DIM), F32),
            pltpu.VMEM((TOKENS, HEAD_DIM), F32),
            pltpu.VMEM((TOKENS, HEAD_DIM), F32),
            pltpu.SemaphoreType.DMA,
            pltpu.SemaphoreType.DMA((WQ_RING,)),
            pltpu.SemaphoreType.DMA((RING,)),
            pltpu.SemaphoreType.DMA((RING,)),
            pltpu.SemaphoreType.DMA((RING,)),
            pltpu.SemaphoreType.DMA((RING,)),
        ],
        compiler_params=pltpu.CompilerParams(vmem_limit_bytes=VMEM_LIMIT),
    )(positions, x, gain, table, pos_row, ids_t, router_t, w_kv, w_query, k_cache, v_cache)


def reduce_columns(drive, partial, base_hbm, out_ref, base_ref, base_sem, send1, recv1, own, recv2, fin, recv3, s1, r1, s2, r2, s3, r3):
    chunks, height, width = send1.shape
    per = TOKENS // height
    half_width = HIDDEN // 2
    me = lax.axis_index('tp')
    core = lax.rem(me, 2)
    sibling = me + 1 - 2 * core
    partner = lax.rem(me + 2, 4)
    barrier = pltpu.get_barrier_semaphore()
    for peer in (sibling, partner):
        pl.semaphore_signal(barrier, inc=1, device_id={'tp': peer}, device_id_type=MESH)
    pl.semaphore_wait(barrier, 2)

    def column(s):
        half = lax.rem(core + 1 + s, 2)
        return pl.multiple_of(half * half_width + lax.div(s, 2) * width, width)

    def remote(src, dst, c, send, recv, peer):
        return pltpu.make_async_remote_copy(src_ref=src.at[c], dst_ref=dst.at[c], send_sem=send.at[c], recv_sem=recv.at[c],
                                            device_id={'tp': peer}, device_id_type=MESH)

    def to_sibling(c):
        return remote(send1, recv1, c, s1, r1, sibling)

    def to_partner(c):
        return remote(own, recv2, c, s2, r2, partner)

    def share(c):
        return remote(fin, recv3, c, s3, r3, sibling)

    def chunk_step(i, parity, m):
        s = 2 * i + parity
        rows = pl.ds(pl.multiple_of(m * height, height), height)
        chunk = per * i + m
        acc = partial(s, rows, column(s))
        if parity == 0:
            send1[chunk] = acc.astype(BF16)
            to_sibling(chunk).start()
        else:
            to_sibling(chunk).wait_recv()
            own[chunk] = (acc + recv1[chunk].astype(F32)).astype(BF16)
            to_partner(chunk).start()

    def place(c, half):
        rows = pl.ds(pl.multiple_of(lax.rem(c, per) * height, height), height)
        cols = pl.ds(pl.multiple_of(half * half_width + lax.div(c, per) * width, width), width)
        return rows, cols

    def finish(c):
        to_partner(c).wait_recv()
        rows, cols = place(c, core)
        total = own[c].astype(F32) + recv2[c].astype(F32)
        value = (base_ref[rows, cols].astype(F32) + total).astype(BF16)
        fin[c] = value
        share(c).start()
        out_ref[rows, cols] = value

    base_copy = pltpu.make_async_copy(base_hbm, base_ref, base_sem)
    finished = drive(chunk_step, column, finish, base_copy)

    def final_body(c, carry):
        finish(c)
        return carry
    lax.fori_loop(finished, chunks, final_body, 0)

    def gather_body(c, carry):
        share(c).wait_recv()
        rows, cols = place(c, 1 - core)
        out_ref[rows, cols] = recv3[c]
        return carry
    lax.fori_loop(0, chunks, gather_body, 0)

    def drain_body(c, carry):
        to_sibling(c).wait_send()
        to_partner(c).wait_send()
        share(c).wait_send()
        return carry
    lax.fori_loop(0, chunks, drain_body, 0)


def chunk_scratch(height, width):
    chunks = TOKENS * HIDDEN // 2 // (height * width)
    return ([pltpu.VMEM((TOKENS, HIDDEN), BF16), pltpu.SemaphoreType.DMA]
            + [pltpu.VMEM((chunks, height, width), BF16)] * 6 + [pltpu.SemaphoreType.DMA((chunks,))] * 6)


OUT_RING = 4


def out_kernel(o_ref, ids_ref, gates_ref, w_hbm, x_hbm, out_ref, spread, wbuf, w_sem, *chunk_refs):
    core = lax.rem(lax.axis_index('tp'), 2)

    def load_w(s):
        half = lax.rem(core + 1 + s, 2)
        cols = pl.ds(pl.multiple_of((half * (STEPS // 2) + lax.div(s, 2)) * COL, COL), COL)
        slot = lax.rem(s, OUT_RING)
        return pltpu.make_async_copy(w_hbm.at[:, :, cols], wbuf.at[slot], w_sem.at[slot])

    for s in range(OUT_RING):
        load_w(jnp.int32(s)).start()

    def spread_rows(m):
        def spread_body(n, carry):
            rows = pl.ds(pl.multiple_of(m * ROWS + n * 64, 64), 64)
            first = o_ref[rows, :QUERY_COLS].astype(F32)
            second = o_ref[rows, QUERY_COLS:].astype(F32)
            for e in range(EXPERTS):
                picked = jnp.where(ids_ref[rows, 0:1] == e, first, 0.0)
                picked = jnp.where(ids_ref[rows, 1:2] == e, second, picked)
                spread[e, rows, :] = picked.astype(BF16)
            return carry
        lax.fori_loop(0, ROWS // 64, spread_body, 0)

    def partial(s, rows, col):
        slot = lax.rem(s, OUT_RING)
        acc = jnp.zeros((ROWS, COL), F32)
        for e in range(EXPERTS):
            acc = acc + gates_ref[rows, e:e + 1] * dot(spread[e, rows, :], wbuf[slot, e])
        return acc

    def drive(chunk_step, column, finish, base_copy):
        def col_body(i, carry):
            for parity in range(2):
                load_w(2 * i + parity).wait()

            def row_body(m, c):
                @pl.when(i == 0)
                def _():
                    spread_rows(m)
                for parity in range(2):
                    chunk_step(i, parity, m)
                return c
            lax.fori_loop(0, TOKENS // ROWS, row_body, 0)

            @pl.when(2 * i + OUT_RING < STEPS)
            def _():
                for parity in range(2):
                    load_w(2 * i + OUT_RING + parity).start()

            @pl.when(i == 0)
            def _():
                base_copy.start()

            @pl.when(i == 1)
            def _():
                base_copy.wait()

            @pl.when(i >= 2)
            def _():
                finish(2 * (i - 2))
                finish(2 * (i - 2) + 1)
            return carry
        lax.fori_loop(0, STEPS // 2, col_body, 0)
        return CHUNKS // 2

    reduce_columns(drive, partial, x_hbm, out_ref, *chunk_refs)


def out_project(o, ids, gates, w_out, x):
    vmem = pl.BlockSpec(memory_space=pltpu.VMEM)
    return pl.pallas_call(
        out_kernel,
        name='out_project',
        out_shape=jax.ShapeDtypeStruct((TOKENS, HIDDEN), BF16),
        in_specs=[vmem] * 3 + [pl.BlockSpec(memory_space=pl.ANY)] * 2,
        out_specs=vmem,
        scratch_shapes=[
            pltpu.VMEM((EXPERTS, TOKENS, QUERY_COLS), BF16),
            pltpu.VMEM((OUT_RING, EXPERTS, QUERY_COLS, COL), BF16),
            pltpu.SemaphoreType.DMA((OUT_RING,)),
        ] + chunk_scratch(ROWS, COL),
        compiler_params=pltpu.CompilerParams(vmem_limit_bytes=VMEM_LIMIT, collective_id=0, has_side_effects=True),
    )(o, ids, gates, w_out, x)


def gate_up_kernel(x_ref, gain_ref, router_ref, idst_ref, wg_hbm, wu_hbm, wd_hbm, a_hbm, gates_ref, early_ref,
                   unorm, picked, scatter, gathered, wg, wu, wd, act, abuf, early_rows, wg_sem, wu_sem, wd_sem, a_sem):
    first_id = lax.axis_index('tp') * LOCAL
    core = lax.rem(lax.axis_index('tp'), 2)

    def load(s):
        e = lax.div(s, F_TILES)
        cols = pl.ds(pl.multiple_of(lax.rem(s, F_TILES) * FT, FT), FT)
        slot = lax.rem(s, W_RING)
        return (pltpu.make_async_copy(wg_hbm.at[e, :, cols], wg.at[slot], wg_sem.at[slot]),
                pltpu.make_async_copy(wu_hbm.at[e, :, cols], wu.at[slot], wu_sem.at[slot]),
                down_of(e, cols, slot, 0), down_of(e, cols, slot, 1))

    def down_of(e, rows, slot, j):
        half = lax.rem(core + 1 + j, 2)
        cols = pl.ds(pl.multiple_of(half * (HIDDEN // 2), HIDDEN // 2), COL)
        return pltpu.make_async_copy(wd_hbm.at[e, rows, cols], wd.at[slot, j], wd_sem.at[slot, j])

    def save(s):
        e = lax.div(s, F_TILES)
        cols = pl.ds(pl.multiple_of(lax.rem(s, F_TILES) * FT, FT), FT)
        slot = lax.rem(s, 2)
        return pltpu.make_async_copy(abuf.at[slot], a_hbm.at[e, :, cols], a_sem.at[slot])

    for s in range(W_RING):
        for copy in load(jnp.int32(s)):
            copy.start()

    norm_rows(x_ref, gain_ref, unorm)
    ids = turn((idst_ref[0:1, :], idst_ref[1:2, :]))
    id0 = ids[:, 0:1]
    id1 = ids[:, 1:2]
    logits = dot_nt(unorm[...], router_ref[...])
    g0, g1 = pair_gates(logits, id0, id1)
    lane8 = iota((TOKENS, EXPERTS), 1)
    local8 = lane8 + first_id
    gates_ref[...] = jnp.where(local8 == id0, g0, 0.0) + jnp.where(local8 == id1, g1, 0.0)

    before = iota((TOKENS, TOKENS), 0)
    after = iota((TOKENS, TOKENS), 1)
    lower = jnp.where(after < before, 1.0, 0.0).astype(BF16)
    upper = jnp.where(before < after, 1.0, 0.0).astype(BF16)
    lane_id = iota((TOKENS, 128), 1) + first_id
    mask_col = jnp.where((lane_id == id0) | (lane_id == id1), 1.0, 0.0)
    rank_col = dot(lower, mask_col.astype(BF16))
    sub_id = iota((8, TOKENS), 0) + first_id
    mask_row = jnp.where((sub_id == idst_ref[0:1, :]) | (sub_id == idst_ref[1:2, :]), 1.0, 0.0)
    rank_row = dot(mask_row.astype(BF16), upper)
    counts = []
    for e in range(LOCAL):
        counts.append(jnp.sum(mask_row[e:e + 1, :]).astype(jnp.int32))
        where_col = jnp.where(mask_col[:, e:e + 1] > 0.0, rank_col[:, e:e + 1], -1.0)
        where_row = jnp.where(mask_row[e:e + 1, :] > 0.0, rank_row[e:e + 1, :], -1.0)
        scatter[e] = jnp.where(after.astype(F32) == where_col, 1.0, 0.0).astype(BF16)
        picked[e] = jnp.where(before.astype(F32) == where_row, 1.0, 0.0).astype(BF16)
    blocks = [lax.div(n + (RB - 1), RB) for n in counts]

    for e in range(LOCAL):
        def gather_body(rb, carry):
            rows = pl.ds(pl.multiple_of(rb * RB, RB), RB)
            gathered[e, rows, :] = dot(picked[e, rows, :], unorm[...]).astype(BF16)
            return carry
        lax.fori_loop(0, blocks[e], gather_body, 0)

    early_rows[...] = jnp.zeros_like(early_rows)

    def step_body(s, carry):
        e = lax.div(s, F_TILES)
        slot = lax.rem(s, W_RING)
        out_slot = lax.rem(s, 2)
        for copy in load(s):
            copy.wait()

        @pl.when(s >= 2)
        def _():
            save(s - 2).wait()

        def run(count):
            for n in range(FT // COL):
                cols = slice(n * COL, (n + 1) * COL)
                gate = dot(gathered[e, :count, :], wg[slot, :, cols])
                up = dot(gathered[e, :count, :], wu[slot, :, cols])
                act[:count, cols] = (gate * (1.0 / (1.0 + jnp.exp(-gate))) * up).astype(BF16)
            for j in range(2):
                cols = slice(j * COL, (j + 1) * COL)
                early_rows[e, :count, cols] += dot(act[:count, :], wd[slot, j])
            for m in range(TOKENS // ROWS):
                rows = slice(m * ROWS, (m + 1) * ROWS)
                abuf[out_slot, rows, :] = dot(scatter[e, rows, :count], act[:count, :]).astype(BF16)

        n_rows = jnp.where(e == 0, counts[0], counts[1])
        n_steps = jnp.maximum(lax.div(n_rows + 63, 64), 2)
        for k in range(2, TOKENS // 64 + 1):
            pl.when(n_steps == k)(functools.partial(run, k * 64))

        @pl.when(s + W_RING < MLP_STEPS)
        def _():
            for copy in load(s + W_RING):
                copy.start()
        save(s).start()
        return carry
    lax.fori_loop(0, MLP_STEPS, step_body, 0)

    def early_body(m, carry):
        rows = pl.ds(pl.multiple_of(m * ROWS, ROWS), ROWS)
        for j in range(2):
            total = jnp.zeros((ROWS, COL), F32)
            for e in range(LOCAL):
                z = early_rows[e, :, j * COL:(j + 1) * COL]
                high = z.astype(BF16)
                rest = (z - high.astype(F32)).astype(BF16)
                mine = dot(scatter[e, rows, :], high) + dot(scatter[e, rows, :], rest)
                total = total + gates_ref[rows, e:e + 1] * mine
            early_ref[j, rows, :] = total
        return carry
    lax.fori_loop(0, TOKENS // ROWS, early_body, 0)
    for s in (MLP_STEPS - 2, MLP_STEPS - 1):
        save(jnp.int32(s)).wait()


def gate_up(x_mid, gain, router_t, ids_t, w_gate, w_up, w_down):
    any_spec = pl.BlockSpec(memory_space=pl.ANY)
    vmem = pl.BlockSpec(memory_space=pltpu.VMEM)
    return pl.pallas_call(
        gate_up_kernel,
        name='gate_up',
        out_shape=(jax.ShapeDtypeStruct((LOCAL, TOKENS, FFN), BF16), jax.ShapeDtypeStruct((TOKENS, EXPERTS), F32),
                   jax.ShapeDtypeStruct((2, TOKENS, COL), F32)),
        in_specs=[vmem] * 4 + [any_spec] * 3,
        out_specs=(any_spec, vmem, vmem),
        scratch_shapes=[
            pltpu.VMEM((TOKENS, HIDDEN), BF16),
            pltpu.VMEM((LOCAL, TOKENS, TOKENS), BF16),
            pltpu.VMEM((LOCAL, TOKENS, TOKENS), BF16),
            pltpu.VMEM((LOCAL, TOKENS, HIDDEN), BF16),
            pltpu.VMEM((W_RING, HIDDEN, FT), BF16),
            pltpu.VMEM((W_RING, HIDDEN, FT), BF16),
            pltpu.VMEM((W_RING, 2, FT, COL), BF16),
            pltpu.VMEM((TOKENS, FT), BF16),
            pltpu.VMEM((2, TOKENS, FT), BF16),
            pltpu.VMEM((LOCAL, TOKENS, 2 * COL), F32),
            pltpu.SemaphoreType.DMA((W_RING,)),
            pltpu.SemaphoreType.DMA((W_RING,)),
            pltpu.SemaphoreType.DMA((W_RING, 2)),
            pltpu.SemaphoreType.DMA((2,)),
        ],
        compiler_params=pltpu.CompilerParams(vmem_limit_bytes=VMEM_LIMIT),
    )(x_mid, gain, router_t, ids_t, w_gate, w_up, w_down)


DOWN_RING = 2


def down_kernel(gates_ref, early_ref, x_hbm, a_hbm, w_hbm, out_ref, abuf, wbuf, first_part, a_sem, w_sem, *chunk_refs):
    me = lax.axis_index('tp')
    core = lax.rem(me, 2)

    def copy_of(s, col, e):
        slot = lax.rem(s, DOWN_RING)
        return pltpu.make_async_copy(w_hbm.at[e, :, pl.ds(col, COL)], wbuf.at[slot, e], w_sem.at[slot, e])

    def ahead(s, e):
        half = lax.rem(core + 1 + s, 2)
        return copy_of(jnp.int32(s), pl.multiple_of((half * (STEPS // 2) + s // 2) * COL, COL), e)

    a_copies = [pltpu.make_async_copy(a_hbm.at[e], abuf.at[e], a_sem.at[e]) for e in range(LOCAL)]
    for e in range(LOCAL):
        a_copies[e].start()
        ahead(2, e).start()

    def partial(s, rows, col):
        if isinstance(s, int):
            return early_ref[s, rows, :]
        return first_part[rows, :] + gates_ref[rows, 1:2] * dot(abuf[1, rows, :], wbuf[lax.rem(s, DOWN_RING), 1])

    def drive(chunk_step, column, finish, base_copy):
        for m in range(TOKENS // ROWS):
            for parity in range(2):
                chunk_step(0, parity, m)
        a_copies[0].wait()
        for e in range(LOCAL):
            ahead(3, e).start()
        base_copy.start()

        def col_body(i, carry):
            for parity in range(2):
                s = 2 * i + parity
                slot = lax.rem(s, DOWN_RING)
                copy_of(s, column(s), 0).wait()
                first_part[...] = gates_ref[:, 0:1] * dot(abuf[0], wbuf[slot, 0])
                if parity == 0:
                    @pl.when(i == 1)
                    def _():
                        a_copies[1].wait()
                copy_of(s, column(s), 1).wait()

                def row_body(m, c):
                    chunk_step(i, parity, m)
                    return c
                lax.fori_loop(0, TOKENS // ROWS, row_body, 0)

                @pl.when(s + DOWN_RING < STEPS)
                def _():
                    for e in range(LOCAL):
                        copy_of(s + DOWN_RING, column(s + DOWN_RING), e).start()

            @pl.when(i == 1)
            def _():
                base_copy.wait()

            @pl.when(i >= 2)
            def _():
                finish(2 * (i - 2))
                finish(2 * (i - 2) + 1)
            return carry
        lax.fori_loop(1, STEPS // 2, col_body, 0)
        return CHUNKS // 2

    reduce_columns(drive, partial, x_hbm, out_ref, *chunk_refs)


def down_project(gates, early, x_mid, act, w_down):
    vmem = pl.BlockSpec(memory_space=pltpu.VMEM)
    any_spec = pl.BlockSpec(memory_space=pl.ANY)
    return pl.pallas_call(
        down_kernel,
        name='down_project',
        out_shape=jax.ShapeDtypeStruct((TOKENS, HIDDEN), BF16),
        in_specs=[vmem] * 2 + [any_spec] * 3,
        out_specs=vmem,
        scratch_shapes=[
            pltpu.VMEM((LOCAL, TOKENS, FFN), BF16),
            pltpu.VMEM((DOWN_RING, LOCAL, FFN, COL), BF16),
            pltpu.VMEM((TOKENS, COL), F32),
            pltpu.SemaphoreType.DMA((LOCAL,)),
            pltpu.SemaphoreType.DMA((DOWN_RING, LOCAL)),
        ] + chunk_scratch(ROWS, COL),
        compiler_params=pltpu.CompilerParams(vmem_limit_bytes=VMEM_LIMIT, collective_id=1, has_side_effects=True),
    )(gates, early, x_mid, act, w_down)


PIECES = 8


def hand_over_kernel(x_hbm, out_hbm, buf, in_sem, out_sem):
    def rows(i):
        return pl.ds(i * (TOKENS // PIECES), TOKENS // PIECES)
    reads = [pltpu.make_async_copy(x_hbm.at[rows(i)], buf.at[i], in_sem.at[i]) for i in range(PIECES)]
    writes = [pltpu.make_async_copy(buf.at[i], out_hbm.at[rows(i)], out_sem.at[i]) for i in range(PIECES)]
    for copy in reads:
        copy.start()
    for read, write in zip(reads, writes):
        read.wait()
        write.start()
    for copy in writes:
        copy.wait()


def hand_over(x):
    any_spec = pl.BlockSpec(memory_space=pl.ANY)
    return pl.pallas_call(
        hand_over_kernel,
        name='hand_over',
        out_shape=jax.ShapeDtypeStruct(x.shape, x.dtype),
        in_specs=[any_spec],
        out_specs=any_spec,
        scratch_shapes=[pltpu.VMEM((PIECES, TOKENS // PIECES, HIDDEN), BF16), pltpu.SemaphoreType.DMA((PIECES,)), pltpu.SemaphoreType.DMA((PIECES,))],
        compiler_params=pltpu.CompilerParams(vmem_limit_bytes=VMEM_LIMIT),
    )(x)


def rope_table():
    half = HEAD_DIM // 2
    inv_freq = np.float32(ROPE_BASE) ** (-(np.arange(half, dtype=np.float32) * np.float32(2.0) / np.float32(HEAD_DIM)))
    angles = np.arange(SLOTS, dtype=np.float32)[:, None] * inv_freq[None, :].astype(np.float32)
    cos = np.cos(angles.astype(np.float64))
    sin = np.sin(angles.astype(np.float64))
    full = np.concatenate([cos, cos, -sin, sin], axis=1).astype(np.float32)
    parts = []
    for _ in range(3):
        part = full.astype(BF16)
        parts.append(part)
        full = full - part.astype(np.float32)
    parts.append(np.zeros_like(parts[0]))
    return np.concatenate(parts, axis=0)


def solution(mesh):
    table = rope_table()

    def local_step(x, k_cache, v_cache, positions, att_ids, mlp_ids, norm_att, w_kv, router_att, w_query, w_out, norm_mlp, router_mlp, w_gate, w_up, w_down):
        flat = (TOKENS, SLOTS * HEADS, HEAD_DIM)
        kv_rows = w_kv.reshape(HIDDEN, HEADS, 2, HEAD_DIM).transpose(0, 2, 1, 3).reshape(HIDDEN * 8, HEAD_DIM)
        k_new, v_new, o, att_gates, att_cols = attend(
            positions, x, norm_att.reshape(1, HIDDEN), jnp.asarray(table), positions.reshape(1, TOKENS), att_ids.T, router_att.T,
            kv_rows, w_query, k_cache.reshape(flat), v_cache.reshape(flat))
        x_mid = out_project(o, att_cols, att_gates, w_out, x)
        act, mlp_gates, early = gate_up(x_mid, norm_mlp.reshape(1, HIDDEN), router_mlp.T, mlp_ids.T, w_gate, w_up, w_down)
        x_out = hand_over(down_project(mlp_gates, early, x_mid, act, w_down))
        return x_out, k_new.reshape(k_cache.shape), v_new.reshape(v_cache.shape)

    token_spec = P('dp', None)
    cache_spec = P('dp', None, 'tp', None)
    expert_spec = P('tp', None, None)
    in_specs = (token_spec, cache_spec, cache_spec, P('dp'), token_spec, token_spec, P(), P(None, 'tp', None), P(), P(None, None, 'tp'), P(None, 'tp', None), P(), P(), expert_spec, expert_spec, expert_spec)
    out_specs = (token_spec, cache_spec, cache_spec)
    return jax.shard_map(local_step, mesh=mesh, in_specs=in_specs, out_specs=out_specs, check_vma=False)
```

```python
import functools

import jax
import jax.numpy as jnp
import numpy as np
from jax import lax
from jax.experimental import pallas as pl
from jax.experimental.pallas import tpu as pltpu
from jax.sharding import PartitionSpec as P

NORM_EPS = 1e-6
ROPE_BASE = 10000.0
F32 = jnp.float32
BF16 = jnp.bfloat16
NEG = -1e30
MESH = pl.DeviceIdType.MESH
VMEM_LIMIT = 62 * 1024 * 1024

TOKENS = 512
HIDDEN = 2048
HEADS = 4
HEAD_DIM = 128
SLOTS = 32
QUERY_COLS = HEADS * HEAD_DIM
EXPERTS = 8
FFN = 5632
LOCAL = 2

BLOCK = 32
RING = 8
BLOCKS = TOKENS // BLOCK
GROUP = 8
WQ_RING = 3

COL = 256
ROWS = 256
STEPS = HIDDEN // COL
CHUNKS = STEPS // 2 * (TOKENS // ROWS)

FT = 512
F_TILES = FFN // FT
MLP_STEPS = LOCAL * F_TILES
W_RING = 5
RB = 128


def dot(a, b):
    return jnp.dot(a, b, preferred_element_type=F32)


def iota(shape, dim):
    return lax.broadcasted_iota(jnp.int32, shape, dim)


def norm_rows(x_ref, gain_ref, out_ref):
    def body(i, carry):
        rows = pl.ds(pl.multiple_of(i * 32, 32), 32)
        values = x_ref[rows, :].astype(F32)
        inv = lax.rsqrt(jnp.mean(values * values, axis=-1, keepdims=True) + NORM_EPS)
        out_ref[rows, :] = (values * inv * gain_ref[...]).astype(BF16)
        return carry
    lax.fori_loop(0, TOKENS // 32, body, 0)


def pair_gates(logits, id0, id1):
    lane = iota(logits.shape, 1)
    first = jnp.sum(jnp.where(lane == id0, logits, 0.0), axis=1, keepdims=True)
    second = jnp.sum(jnp.where(lane == id1, logits, 0.0), axis=1, keepdims=True)
    top = jnp.maximum(first, second)
    e0 = jnp.exp(first - top)
    e1 = jnp.exp(second - top)
    total = e0 + e1
    return e0 / total, e1 / total


def turn(rows):
    sub = iota((8, TOKENS), 0)
    stacked = jnp.zeros((8, TOKENS), F32)
    for i, row in enumerate(rows):
        stacked = jnp.where(sub == i, row.astype(F32), stacked)
    return jnp.transpose(stacked).astype(jnp.int32)


def dot_nt(a, b):
    return lax.dot_general(a, b, (((1,), (1,)), ((), ())), preferred_element_type=F32)


def attend_kernel(pos_ref, gain_ref, table_ref, posrow_ref, idst_ref, router_ref, x_hbm, wkv_hbm, wq_hbm, kc_hbm, vc_hbm,
                  ko_hbm, vo_hbm, o_ref, gates_ref, ids_ref,
                  xbuf, hid, wraw, wtmp, wkv, wq, kbuf, vbuf, qsel, qrow, qdiag, knv, probs, orow, cos_s, sin_s,
                  x_sem, wkv_sem, wq_sem, kin_sem, vin_sem, kout_sem, vout_sem):
    def block_of(ref, b):
        return ref.at[pl.ds(pl.multiple_of(b * BLOCK, BLOCK), BLOCK)]

    def load(b):
        slot = lax.rem(b, RING)
        return (pltpu.make_async_copy(block_of(kc_hbm, b), kbuf.at[slot], kin_sem.at[slot]),
                pltpu.make_async_copy(block_of(vc_hbm, b), vbuf.at[slot], vin_sem.at[slot]))

    def save(b):
        slot = lax.rem(b, RING)
        return (pltpu.make_async_copy(kbuf.at[slot], block_of(ko_hbm, b), kout_sem.at[slot]),
                pltpu.make_async_copy(vbuf.at[slot], block_of(vo_hbm, b), vout_sem.at[slot]))

    def load_wq(e):
        slot = lax.rem(e, WQ_RING)
        return pltpu.make_async_copy(wq_hbm.at[e], wq.at[slot], wq_sem.at[slot])

    x_copy = pltpu.make_async_copy(x_hbm, xbuf, x_sem)
    x_copy.start()
    kv_copy = pltpu.make_async_copy(wkv_hbm, wraw, wkv_sem)
    kv_copy.start()
    for b in range(3):
        for copy in load(jnp.int32(b)):
            copy.start()
    load_wq(jnp.int32(0)).start()

    x_copy.wait()
    norm_rows(xbuf, gain_ref, hid)
    for e in range(1, WQ_RING):
        load_wq(jnp.int32(e)).start()
    ids = turn((idst_ref[0:1, :], idst_ref[1:2, :], posrow_ref[...]))
    ids_ref[...] = ids
    id0 = ids[:, 0:1]
    id1 = ids[:, 1:2]
    lane128 = iota((TOKENS, 128), 1)
    chosen = ((lane128 & 31) == ids[:, 2:3]) & (lane128 < 3 * SLOTS)
    trig = dot(jnp.where(chosen, 1.0, 0.0).astype(BF16), table_ref[...])
    cos_s[...] = trig[:, :HEAD_DIM]
    sin_s[...] = trig[:, HEAD_DIM:]
    logits = dot_nt(hid[...], router_ref[...])
    g0, g1 = pair_gates(logits, id0, id1)
    lane8 = iota((TOKENS, EXPERTS), 1)
    gates_ref[...] = jnp.where(lane8 == id0, g0, 0.0) + jnp.where(lane8 == id1, g1, 0.0)
    kv_copy.wait()

    def sort_body(i, carry):
        wtmp[...] = wraw[pl.ds(pl.multiple_of(i * 1024, 1024), 1024), :].astype(F32)
        rows = pl.ds(pl.multiple_of(i * 128, 128), 128)
        for j in range(8):
            wkv[rows, j * 128:(j + 1) * 128] = wtmp[pl.ds(j, 128, stride=8), :].astype(BF16)
        return carry
    lax.fori_loop(0, HIDDEN // 128, sort_body, 0)

    keys_new = dot(hid[...], wkv[:, :QUERY_COLS])
    for h in range(HEADS):
        k = keys_new[:, h * 128:(h + 1) * 128]
        knv[pl.ds(h, TOKENS, stride=8), :] = k * cos_s[...] + pltpu.roll(k, 64, 1) * sin_s[...]
    values_new = dot(hid[...], wkv[:, QUERY_COLS:])
    for h in range(HEADS):
        knv[pl.ds(h + 4, TOKENS, stride=8), :] = values_new[:, h * 128:(h + 1) * 128]

    def q_body(e, carry):
        @pl.when(e + 3 < RING)
        def _():
            for copy in load(e + 3):
                copy.start()
        load_wq(e).wait()
        slot = lax.rem(e, WQ_RING)

        q = dot(hid[...], wq[slot])
        for k in range(2):
            qsel[k] = jnp.where(ids_ref[:, k:k + 1] == e, q, qsel[k])

        @pl.when(e + WQ_RING < EXPERTS)
        def _():
            load_wq(e + WQ_RING).start()
        return carry
    lax.fori_loop(0, EXPERTS, q_body, 0)

    def rope_body(m, carry):
        rows = pl.ds(pl.multiple_of(m * 128, 128), 128)
        cos = cos_s[rows, :]
        sin = sin_s[rows, :]
        for k in range(2):
            for h in range(HEADS):
                q = qsel[k, rows, h * 128:(h + 1) * 128]
                qrow[pl.ds(k * HEADS + h, 128, stride=8), :] = q * cos + pltpu.roll(q, 64, 1) * sin
        q = qrow[...]
        even = (iota((1024, HEAD_DIM), 0) & 8) == 0
        lines = pl.ds(pl.multiple_of(m * 1024, 1024), 1024)
        qdiag[lines, :HEAD_DIM] = jnp.where(even, q, 0.0).astype(BF16)
        qdiag[lines, HEAD_DIM:] = jnp.where(even, 0.0, q).astype(BF16)
        return carry
    lax.fori_loop(0, TOKENS // 128, rope_body, 0)

    scale = HEAD_DIM ** -0.5
    sub16 = iota((16, HEAD_DIM), 0) >> 2
    low = iota((8, 128), 0) < 4
    row16 = iota((16, 128), 0)
    lane = iota((16, 128), 1)
    upper = row16 < 8
    same_head = (lane & 3) == (row16 & 3)
    slot_of = lane >> 2

    def block_body(i, carry):
        b = jnp.minimum(i, BLOCKS - 1)
        prev = jnp.maximum(i - 1, 0)
        slot = lax.rem(b, RING)
        prev_slot = lax.rem(prev, RING)
        side = lax.rem(i, 2)

        @pl.when(i < BLOCKS)
        def _():
            for copy in load(b):
                copy.wait()
        places = [pos_ref[b * BLOCK + t] for t in range(BLOCK)]

        def patch(t):
            rows = pl.ds(pl.multiple_of((places[t] >> 2) * 16, 16), 16)
            put = sub16 == (places[t] & 3)
            both = knv[pl.ds(pl.multiple_of((b * BLOCK + t) * 8, 8), 8), :]
            swapped = pltpu.roll(both, 4, 0)
            for n8, buf in ((jnp.where(low, both, swapped), kbuf), (jnp.where(low, swapped, both), vbuf)):
                n16 = jnp.concatenate([n8, n8], axis=0)
                old = buf[slot, t, rows, :].astype(F32)
                buf[slot, t, rows, :] = jnp.where(put, n16, old).astype(BF16)

        def score(j):
            t = b * BLOCK + 2 * j
            q = qdiag[pl.ds(pl.multiple_of(t * 8, 16), 16), :]
            keys = jnp.concatenate([kbuf[slot, 2 * j], kbuf[slot, 2 * j + 1]], axis=1)
            s = dot_nt(q, keys) * scale
            s = jnp.where(same_head & (slot_of <= jnp.where(upper, places[2 * j], places[2 * j + 1])), s, NEG)
            e = jnp.exp(s - jnp.max(s, axis=1, keepdims=True))
            probs[side, j] = (e / jnp.sum(e, axis=1, keepdims=True)).astype(BF16)

        def mix(j):
            values = jnp.concatenate([vbuf[prev_slot, 2 * j], vbuf[prev_slot, 2 * j + 1]], axis=1)
            o = dot(probs[1 - side, j], values)
            orow[j * 16:j * 16 + 8, :] = o[:8, :HEAD_DIM]
            orow[j * 16 + 8:j * 16 + 16, :] = o[8:, HEAD_DIM:]

        half = BLOCK // 2
        pairs = BLOCK // 2
        first, second = range(pairs // 2), range(pairs // 2, pairs)
        for t in range(half):
            patch(t)
        for j in first:
            score(j)
        for t in range(half, BLOCK):
            patch(t)
        for j in first:
            mix(j)
        for j in second:
            score(j)
        for j in second:
            mix(j)
        rows = pl.ds(pl.multiple_of(prev * BLOCK, BLOCK), BLOCK)
        for r in range(8):
            o_ref[rows, r * 128:(r + 1) * 128] = orow[pl.ds(r, BLOCK, stride=8), :].astype(BF16)

        @pl.when(i >= 1)
        def _():
            for copy in save(prev):
                copy.start()

        @pl.when(i >= 3)
        def _():
            for copy in save(i - 3):
                copy.wait()

            @pl.when(i - 3 + RING < BLOCKS)
            def _():
                for copy in load(i - 3 + RING):
                    copy.start()
        return carry
    lax.fori_loop(0, BLOCKS + 1, block_body, 0)
    for b in (BLOCKS - 2, BLOCKS - 1):
        for copy in save(jnp.int32(b)):
            copy.wait()


def attend(positions, gain, table, pos_row, ids_t, router_t, x, w_kv, w_query, k_cache, v_cache):
    any_spec = pl.BlockSpec(memory_space=pl.ANY)
    vmem = pl.BlockSpec(memory_space=pltpu.VMEM)
    smem = pl.BlockSpec(memory_space=pltpu.SMEM)
    cache = jax.ShapeDtypeStruct(k_cache.shape, BF16)
    return pl.pallas_call(
        attend_kernel,
        name='attend',
        out_shape=(cache, cache, jax.ShapeDtypeStruct((TOKENS, 2 * QUERY_COLS), BF16),
                   jax.ShapeDtypeStruct((TOKENS, EXPERTS), F32), jax.ShapeDtypeStruct((TOKENS, EXPERTS), jnp.int32)),
        in_specs=[smem] + [vmem] * 5 + [any_spec] * 5,
        out_specs=(any_spec, any_spec, vmem, vmem, vmem),
        scratch_shapes=[
            pltpu.VMEM((TOKENS, HIDDEN), BF16),
            pltpu.VMEM((TOKENS, HIDDEN), BF16),
            pltpu.VMEM((HIDDEN * 8, 128), BF16),
            pltpu.VMEM((1024, 128), F32),
            pltpu.VMEM((HIDDEN, HEADS * 256), BF16),
            pltpu.VMEM((WQ_RING, HIDDEN, QUERY_COLS), BF16),
            pltpu.VMEM((RING, BLOCK, SLOTS * HEADS, HEAD_DIM), BF16),
            pltpu.VMEM((RING, BLOCK, SLOTS * HEADS, HEAD_DIM), BF16),
            pltpu.VMEM((2, TOKENS, QUERY_COLS), F32),
            pltpu.VMEM((1024, HEAD_DIM), F32),
            pltpu.VMEM((TOKENS * 8, 2 * HEAD_DIM), BF16),
            pltpu.VMEM((TOKENS * 8, HEAD_DIM), F32),
            pltpu.VMEM((2, BLOCK // 2, 16, HEAD_DIM), BF16),
            pltpu.VMEM((BLOCK * 8, HEAD_DIM), F32),
            pltpu.VMEM((TOKENS, HEAD_DIM), F32),
            pltpu.VMEM((TOKENS, HEAD_DIM), F32),
            pltpu.SemaphoreType.DMA,
            pltpu.SemaphoreType.DMA,
            pltpu.SemaphoreType.DMA((WQ_RING,)),
            pltpu.SemaphoreType.DMA((RING,)),
            pltpu.SemaphoreType.DMA((RING,)),
            pltpu.SemaphoreType.DMA((RING,)),
            pltpu.SemaphoreType.DMA((RING,)),
        ],
        compiler_params=pltpu.CompilerParams(vmem_limit_bytes=VMEM_LIMIT),
    )(positions, gain, table, pos_row, ids_t, router_t, x, w_kv, w_query, k_cache, v_cache)


def reduce_columns(drive, partial, base_hbm, out_ref, base_ref, base_sem, send1, recv1, own, recv2, fin, recv3, s1, r1, s2, r2, s3, r3):
    chunks, height, width = send1.shape
    per = TOKENS // height
    half_width = HIDDEN // 2
    me = lax.axis_index('tp')
    core = lax.rem(me, 2)
    sibling = me + 1 - 2 * core
    partner = lax.rem(me + 2, 4)
    barrier = pltpu.get_barrier_semaphore()
    for peer in (sibling, partner):
        pl.semaphore_signal(barrier, inc=1, device_id={'tp': peer}, device_id_type=MESH)
    pl.semaphore_wait(barrier, 2)

    def column(s):
        half = lax.rem(core + 1 + s, 2)
        return pl.multiple_of(half * half_width + lax.div(s, 2) * width, width)

    def remote(src, dst, c, send, recv, peer):
        return pltpu.make_async_remote_copy(src_ref=src.at[c], dst_ref=dst.at[c], send_sem=send.at[c], recv_sem=recv.at[c],
                                            device_id={'tp': peer}, device_id_type=MESH)

    def to_sibling(c):
        return remote(send1, recv1, c, s1, r1, sibling)

    def to_partner(c):
        return remote(own, recv2, c, s2, r2, partner)

    def share(c):
        return remote(fin, recv3, c, s3, r3, sibling)

    def chunk_step(i, parity, m):
        s = 2 * i + parity
        rows = pl.ds(pl.multiple_of(m * height, height), height)
        chunk = per * i + m
        acc = partial(s, rows, column(s))
        if parity == 0:
            send1[chunk] = acc.astype(BF16)
            to_sibling(chunk).start()
        else:
            to_sibling(chunk).wait_recv()
            own[chunk] = (acc + recv1[chunk].astype(F32)).astype(BF16)
            to_partner(chunk).start()

    def place(c, half):
        rows = pl.ds(pl.multiple_of(lax.rem(c, per) * height, height), height)
        cols = pl.ds(pl.multiple_of(half * half_width + lax.div(c, per) * width, width), width)
        return rows, cols

    def finish(c):
        to_partner(c).wait_recv()
        rows, cols = place(c, core)
        total = own[c].astype(F32) + recv2[c].astype(F32)
        value = (base_ref[rows, cols].astype(F32) + total).astype(BF16)
        fin[c] = value
        share(c).start()
        out_ref[rows, cols] = value

    base_copy = pltpu.make_async_copy(base_hbm, base_ref, base_sem)
    finished = drive(chunk_step, column, finish, base_copy)

    def final_body(c, carry):
        finish(c)
        return carry
    lax.fori_loop(finished, chunks, final_body, 0)

    def gather_body(c, carry):
        share(c).wait_recv()
        rows, cols = place(c, 1 - core)
        out_ref[rows, cols] = recv3[c]
        return carry
    lax.fori_loop(0, chunks, gather_body, 0)

    def drain_body(c, carry):
        to_sibling(c).wait_send()
        to_partner(c).wait_send()
        share(c).wait_send()
        return carry
    lax.fori_loop(0, chunks, drain_body, 0)


def chunk_scratch(height, width):
    chunks = TOKENS * HIDDEN // 2 // (height * width)
    return ([pltpu.VMEM((TOKENS, HIDDEN), BF16), pltpu.SemaphoreType.DMA]
            + [pltpu.VMEM((chunks, height, width), BF16)] * 6 + [pltpu.SemaphoreType.DMA((chunks,))] * 6)


OUT_RING = 4


def out_kernel(o_ref, ids_ref, gates_ref, w_hbm, x_hbm, out_ref, spread, wbuf, w_sem, *chunk_refs):
    core = lax.rem(lax.axis_index('tp'), 2)

    def load_w(s):
        half = lax.rem(core + 1 + s, 2)
        cols = pl.ds(pl.multiple_of((half * (STEPS // 2) + lax.div(s, 2)) * COL, COL), COL)
        slot = lax.rem(s, OUT_RING)
        return pltpu.make_async_copy(w_hbm.at[:, :, cols], wbuf.at[slot], w_sem.at[slot])

    for s in range(OUT_RING):
        load_w(jnp.int32(s)).start()

    def spread_rows(m):
        def spread_body(n, carry):
            rows = pl.ds(pl.multiple_of(m * ROWS + n * 64, 64), 64)
            first = o_ref[rows, :QUERY_COLS].astype(F32)
            second = o_ref[rows, QUERY_COLS:].astype(F32)
            for e in range(EXPERTS):
                picked = jnp.where(ids_ref[rows, 0:1] == e, first, 0.0)
                picked = jnp.where(ids_ref[rows, 1:2] == e, second, picked)
                spread[e, rows, :] = picked.astype(BF16)
            return carry
        lax.fori_loop(0, ROWS // 64, spread_body, 0)

    def partial(s, rows, col):
        slot = lax.rem(s, OUT_RING)
        acc = jnp.zeros((ROWS, COL), F32)
        for e in range(EXPERTS):
            acc = acc + gates_ref[rows, e:e + 1] * dot(spread[e, rows, :], wbuf[slot, e])
        return acc

    def drive(chunk_step, column, finish, base_copy):
        def col_body(i, carry):
            for parity in range(2):
                load_w(2 * i + parity).wait()

            def row_body(m, c):
                @pl.when(i == 0)
                def _():
                    spread_rows(m)
                for parity in range(2):
                    chunk_step(i, parity, m)
                return c
            lax.fori_loop(0, TOKENS // ROWS, row_body, 0)

            @pl.when(2 * i + OUT_RING < STEPS)
            def _():
                for parity in range(2):
                    load_w(2 * i + OUT_RING + parity).start()

            @pl.when(i == 0)
            def _():
                base_copy.start()

            @pl.when(i == 1)
            def _():
                base_copy.wait()

            @pl.when(i >= 2)
            def _():
                finish(2 * (i - 2))
                finish(2 * (i - 2) + 1)
            return carry
        lax.fori_loop(0, STEPS // 2, col_body, 0)
        return CHUNKS // 2

    reduce_columns(drive, partial, x_hbm, out_ref, *chunk_refs)


def out_project(o, ids, gates, w_out, x):
    vmem = pl.BlockSpec(memory_space=pltpu.VMEM)
    return pl.pallas_call(
        out_kernel,
        name='out_project',
        out_shape=jax.ShapeDtypeStruct((TOKENS, HIDDEN), BF16),
        in_specs=[vmem] * 3 + [pl.BlockSpec(memory_space=pl.ANY)] * 2,
        out_specs=vmem,
        scratch_shapes=[
            pltpu.VMEM((EXPERTS, TOKENS, QUERY_COLS), BF16),
            pltpu.VMEM((OUT_RING, EXPERTS, QUERY_COLS, COL), BF16),
            pltpu.SemaphoreType.DMA((OUT_RING,)),
        ] + chunk_scratch(ROWS, COL),
        compiler_params=pltpu.CompilerParams(vmem_limit_bytes=VMEM_LIMIT, collective_id=0, has_side_effects=True),
    )(o, ids, gates, w_out, x)


def gate_up_kernel(gain_ref, router_ref, idst_ref, x_hbm, wg_hbm, wu_hbm, wd_hbm, a_hbm, gates_ref, early_ref,
                   xbuf, unorm, picked, scatter, gathered, wg, wu, wd, act, abuf, early_rows, x_sem, wg_sem, wu_sem, wd_sem, a_sem):
    first_id = lax.axis_index('tp') * LOCAL
    core = lax.rem(lax.axis_index('tp'), 2)

    def load(s):
        e = lax.div(s, F_TILES)
        cols = pl.ds(pl.multiple_of(lax.rem(s, F_TILES) * FT, FT), FT)
        slot = lax.rem(s, W_RING)
        return (pltpu.make_async_copy(wg_hbm.at[e, :, cols], wg.at[slot], wg_sem.at[slot]),
                pltpu.make_async_copy(wu_hbm.at[e, :, cols], wu.at[slot], wu_sem.at[slot]),
                down_of(e, cols, slot, 0), down_of(e, cols, slot, 1))

    def down_of(e, rows, slot, j):
        half = lax.rem(core + 1 + j, 2)
        cols = pl.ds(pl.multiple_of(half * (HIDDEN // 2), HIDDEN // 2), COL)
        return pltpu.make_async_copy(wd_hbm.at[e, rows, cols], wd.at[slot, j], wd_sem.at[slot, j])

    def save(s):
        e = lax.div(s, F_TILES)
        cols = pl.ds(pl.multiple_of(lax.rem(s, F_TILES) * FT, FT), FT)
        slot = lax.rem(s, 2)
        return pltpu.make_async_copy(abuf.at[slot], a_hbm.at[e, :, cols], a_sem.at[slot])

    x_copy = pltpu.make_async_copy(x_hbm, xbuf, x_sem)
    x_copy.start()
    for s in range(W_RING):
        for copy in load(jnp.int32(s)):
            copy.start()

    x_copy.wait()
    norm_rows(xbuf, gain_ref, unorm)
    ids = turn((idst_ref[0:1, :], idst_ref[1:2, :]))
    id0 = ids[:, 0:1]
    id1 = ids[:, 1:2]
    logits = dot_nt(unorm[...], router_ref[...])
    g0, g1 = pair_gates(logits, id0, id1)
    lane8 = iota((TOKENS, EXPERTS), 1)
    local8 = lane8 + first_id
    gates_ref[...] = jnp.where(local8 == id0, g0, 0.0) + jnp.where(local8 == id1, g1, 0.0)

    before = iota((TOKENS, TOKENS), 0)
    after = iota((TOKENS, TOKENS), 1)
    lower = jnp.where(after < before, 1.0, 0.0).astype(BF16)
    upper = jnp.where(before < after, 1.0, 0.0).astype(BF16)
    lane_id = iota((TOKENS, 128), 1) + first_id
    mask_col = jnp.where((lane_id == id0) | (lane_id == id1), 1.0, 0.0)
    rank_col = dot(lower, mask_col.astype(BF16))
    sub_id = iota((8, TOKENS), 0) + first_id
    mask_row = jnp.where((sub_id == idst_ref[0:1, :]) | (sub_id == idst_ref[1:2, :]), 1.0, 0.0)
    rank_row = dot(mask_row.astype(BF16), upper)
    counts = []
    for e in range(LOCAL):
        counts.append(jnp.sum(mask_row[e:e + 1, :]).astype(jnp.int32))
        where_col = jnp.where(mask_col[:, e:e + 1] > 0.0, rank_col[:, e:e + 1], -1.0)
        where_row = jnp.where(mask_row[e:e + 1, :] > 0.0, rank_row[e:e + 1, :], -1.0)
        scatter[e] = jnp.where(after.astype(F32) == where_col, 1.0, 0.0).astype(BF16)
        picked[e] = jnp.where(before.astype(F32) == where_row, 1.0, 0.0).astype(BF16)
    blocks = [lax.div(n + (RB - 1), RB) for n in counts]

    for e in range(LOCAL):
        def gather_body(rb, carry):
            rows = pl.ds(pl.multiple_of(rb * RB, RB), RB)
            gathered[e, rows, :] = dot(picked[e, rows, :], unorm[...]).astype(BF16)
            return carry
        lax.fori_loop(0, blocks[e], gather_body, 0)

    early_rows[...] = jnp.zeros_like(early_rows)

    def step_body(s, carry):
        e = lax.div(s, F_TILES)
        slot = lax.rem(s, W_RING)
        out_slot = lax.rem(s, 2)
        for copy in load(s):
            copy.wait()

        @pl.when(s >= 2)
        def _():
            save(s - 2).wait()

        def run(count):
            for n in range(FT // COL):
                cols = slice(n * COL, (n + 1) * COL)
                gate = dot(gathered[e, :count, :], wg[slot, :, cols])
                up = dot(gathered[e, :count, :], wu[slot, :, cols])
                act[:count, cols] = (gate * (1.0 / (1.0 + jnp.exp(-gate))) * up).astype(BF16)
            for j in range(2):
                cols = slice(j * COL, (j + 1) * COL)
                early_rows[e, :count, cols] += dot(act[:count, :], wd[slot, j])
            for m in range(TOKENS // ROWS):
                rows = slice(m * ROWS, (m + 1) * ROWS)
                abuf[out_slot, rows, :] = dot(scatter[e, rows, :count], act[:count, :]).astype(BF16)

        n_rows = jnp.where(e == 0, counts[0], counts[1])
        n_steps = jnp.maximum(lax.div(n_rows + 63, 64), 2)
        for k in range(2, TOKENS // 64 + 1):
            pl.when(n_steps == k)(functools.partial(run, k * 64))

        @pl.when(s + W_RING < MLP_STEPS)
        def _():
            for copy in load(s + W_RING):
                copy.start()
        save(s).start()
        return carry
    lax.fori_loop(0, MLP_STEPS, step_body, 0)

    def early_body(m, carry):
        rows = pl.ds(pl.multiple_of(m * ROWS, ROWS), ROWS)
        for j in range(2):
            total = jnp.zeros((ROWS, COL), F32)
            for e in range(LOCAL):
                z = early_rows[e, :, j * COL:(j + 1) * COL]
                high = z.astype(BF16)
                rest = (z - high.astype(F32)).astype(BF16)
                mine = dot(scatter[e, rows, :], high) + dot(scatter[e, rows, :], rest)
                total = total + gates_ref[rows, e:e + 1] * mine
            early_ref[j, rows, :] = total
        return carry
    lax.fori_loop(0, TOKENS // ROWS, early_body, 0)
    for s in (MLP_STEPS - 2, MLP_STEPS - 1):
        save(jnp.int32(s)).wait()


def gate_up(gain, router_t, ids_t, x_mid, w_gate, w_up, w_down):
    any_spec = pl.BlockSpec(memory_space=pl.ANY)
    vmem = pl.BlockSpec(memory_space=pltpu.VMEM)
    return pl.pallas_call(
        gate_up_kernel,
        name='gate_up',
        out_shape=(jax.ShapeDtypeStruct((LOCAL, TOKENS, FFN), BF16), jax.ShapeDtypeStruct((TOKENS, EXPERTS), F32),
                   jax.ShapeDtypeStruct((2, TOKENS, COL), F32)),
        in_specs=[vmem] * 3 + [any_spec] * 4,
        out_specs=(any_spec, vmem, vmem),
        scratch_shapes=[
            pltpu.VMEM((TOKENS, HIDDEN), BF16),
            pltpu.VMEM((TOKENS, HIDDEN), BF16),
            pltpu.VMEM((LOCAL, TOKENS, TOKENS), BF16),
            pltpu.VMEM((LOCAL, TOKENS, TOKENS), BF16),
            pltpu.VMEM((LOCAL, TOKENS, HIDDEN), BF16),
            pltpu.VMEM((W_RING, HIDDEN, FT), BF16),
            pltpu.VMEM((W_RING, HIDDEN, FT), BF16),
            pltpu.VMEM((W_RING, 2, FT, COL), BF16),
            pltpu.VMEM((TOKENS, FT), BF16),
            pltpu.VMEM((2, TOKENS, FT), BF16),
            pltpu.VMEM((LOCAL, TOKENS, 2 * COL), F32),
            pltpu.SemaphoreType.DMA,
            pltpu.SemaphoreType.DMA((W_RING,)),
            pltpu.SemaphoreType.DMA((W_RING,)),
            pltpu.SemaphoreType.DMA((W_RING, 2)),
            pltpu.SemaphoreType.DMA((2,)),
        ],
        compiler_params=pltpu.CompilerParams(vmem_limit_bytes=VMEM_LIMIT),
    )(gain, router_t, ids_t, x_mid, w_gate, w_up, w_down)


DOWN_RING = 2


def down_kernel(gates_ref, early_ref, x_hbm, a_hbm, w_hbm, out_ref, abuf, wbuf, first_part, a_sem, w_sem, *chunk_refs):
    me = lax.axis_index('tp')
    core = lax.rem(me, 2)

    def copy_of(s, col, e):
        slot = lax.rem(s, DOWN_RING)
        return pltpu.make_async_copy(w_hbm.at[e, :, pl.ds(col, COL)], wbuf.at[slot, e], w_sem.at[slot, e])

    def ahead(s, e):
        half = lax.rem(core + 1 + s, 2)
        return copy_of(jnp.int32(s), pl.multiple_of((half * (STEPS // 2) + s // 2) * COL, COL), e)

    a_copies = [pltpu.make_async_copy(a_hbm.at[e], abuf.at[e], a_sem.at[e]) for e in range(LOCAL)]
    for e in range(LOCAL):
        a_copies[e].start()
        ahead(2, e).start()

    def partial(s, rows, col):
        if isinstance(s, int):
            return early_ref[s, rows, :]
        return first_part[rows, :] + gates_ref[rows, 1:2] * dot(abuf[1, rows, :], wbuf[lax.rem(s, DOWN_RING), 1])

    def drive(chunk_step, column, finish, base_copy):
        for m in range(TOKENS // ROWS):
            for parity in range(2):
                chunk_step(0, parity, m)
        a_copies[0].wait()
        for e in range(LOCAL):
            ahead(3, e).start()
        base_copy.start()

        def col_body(i, carry):
            for parity in range(2):
                s = 2 * i + parity
                slot = lax.rem(s, DOWN_RING)
                copy_of(s, column(s), 0).wait()
                first_part[...] = gates_ref[:, 0:1] * dot(abuf[0], wbuf[slot, 0])
                if parity == 0:
                    @pl.when(i == 1)
                    def _():
                        a_copies[1].wait()
                copy_of(s, column(s), 1).wait()

                def row_body(m, c):
                    chunk_step(i, parity, m)
                    return c
                lax.fori_loop(0, TOKENS // ROWS, row_body, 0)

                @pl.when(s + DOWN_RING < STEPS)
                def _():
                    for e in range(LOCAL):
                        copy_of(s + DOWN_RING, column(s + DOWN_RING), e).start()

            @pl.when(i == 1)
            def _():
                base_copy.wait()

            @pl.when(i >= 2)
            def _():
                finish(2 * (i - 2))
                finish(2 * (i - 2) + 1)
            return carry
        lax.fori_loop(1, STEPS // 2, col_body, 0)
        return CHUNKS // 2

    reduce_columns(drive, partial, x_hbm, out_ref, *chunk_refs)


def down_project(gates, early, x_mid, act, w_down):
    vmem = pl.BlockSpec(memory_space=pltpu.VMEM)
    any_spec = pl.BlockSpec(memory_space=pl.ANY)
    return pl.pallas_call(
        down_kernel,
        name='down_project',
        out_shape=jax.ShapeDtypeStruct((TOKENS, HIDDEN), BF16),
        in_specs=[vmem] * 2 + [any_spec] * 3,
        out_specs=vmem,
        scratch_shapes=[
            pltpu.VMEM((LOCAL, TOKENS, FFN), BF16),
            pltpu.VMEM((DOWN_RING, LOCAL, FFN, COL), BF16),
            pltpu.VMEM((TOKENS, COL), F32),
            pltpu.SemaphoreType.DMA((LOCAL,)),
            pltpu.SemaphoreType.DMA((DOWN_RING, LOCAL)),
        ] + chunk_scratch(ROWS, COL),
        compiler_params=pltpu.CompilerParams(vmem_limit_bytes=VMEM_LIMIT, collective_id=1, has_side_effects=True),
    )(gates, early, x_mid, act, w_down)


PIECES = 8


def hand_over_kernel(x_hbm, out_hbm, buf, in_sem, out_sem):
    def rows(i):
        return pl.ds(i * (TOKENS // PIECES), TOKENS // PIECES)
    reads = [pltpu.make_async_copy(x_hbm.at[rows(i)], buf.at[i], in_sem.at[i]) for i in range(PIECES)]
    writes = [pltpu.make_async_copy(buf.at[i], out_hbm.at[rows(i)], out_sem.at[i]) for i in range(PIECES)]
    for copy in reads:
        copy.start()
    for read, write in zip(reads, writes):
        read.wait()
        write.start()
    for copy in writes:
        copy.wait()


def hand_over(x):
    any_spec = pl.BlockSpec(memory_space=pl.ANY)
    return pl.pallas_call(
        hand_over_kernel,
        name='hand_over',
        out_shape=jax.ShapeDtypeStruct(x.shape, x.dtype),
        in_specs=[any_spec],
        out_specs=any_spec,
        scratch_shapes=[pltpu.VMEM((PIECES, TOKENS // PIECES, HIDDEN), BF16), pltpu.SemaphoreType.DMA((PIECES,)), pltpu.SemaphoreType.DMA((PIECES,))],
        compiler_params=pltpu.CompilerParams(vmem_limit_bytes=VMEM_LIMIT),
    )(x)


def rope_table():
    half = HEAD_DIM // 2
    inv_freq = np.float32(ROPE_BASE) ** (-(np.arange(half, dtype=np.float32) * np.float32(2.0) / np.float32(HEAD_DIM)))
    angles = np.arange(SLOTS, dtype=np.float32)[:, None] * inv_freq[None, :].astype(np.float32)
    cos = np.cos(angles.astype(np.float64))
    sin = np.sin(angles.astype(np.float64))
    full = np.concatenate([cos, cos, -sin, sin], axis=1).astype(np.float32)
    parts = []
    for _ in range(3):
        part = full.astype(BF16)
        parts.append(part)
        full = full - part.astype(np.float32)
    parts.append(np.zeros_like(parts[0]))
    return np.concatenate(parts, axis=0)


def solution(mesh):
    table = rope_table()

    def local_step(x, k_cache, v_cache, positions, att_ids, mlp_ids, norm_att, w_kv, router_att, w_query, w_out, norm_mlp, router_mlp, w_gate, w_up, w_down):
        flat = (TOKENS, SLOTS * HEADS, HEAD_DIM)
        kv_rows = w_kv.reshape(HIDDEN, HEADS, 2, HEAD_DIM).transpose(0, 2, 1, 3).reshape(HIDDEN * 8, HEAD_DIM)
        k_new, v_new, o, att_gates, att_cols = attend(
            positions, norm_att.reshape(1, HIDDEN), jnp.asarray(table), positions.reshape(1, TOKENS), att_ids.T, router_att.T,
            x, kv_rows, w_query, k_cache.reshape(flat), v_cache.reshape(flat))
        x_mid = out_project(o, att_cols, att_gates, w_out, x)
        act, mlp_gates, early = gate_up(norm_mlp.reshape(1, HIDDEN), router_mlp.T, mlp_ids.T, x_mid, w_gate, w_up, w_down)
        x_out = hand_over(down_project(mlp_gates, early, x_mid, act, w_down))
        return x_out, k_new.reshape(k_cache.shape), v_new.reshape(v_cache.shape)

    token_spec = P('dp', None)
    cache_spec = P('dp', None, 'tp', None)
    expert_spec = P('tp', None, None)
    in_specs = (token_spec, cache_spec, cache_spec, P('dp'), token_spec, token_spec, P(), P(None, 'tp', None), P(), P(None, None, 'tp'), P(None, 'tp', None), P(), P(), expert_spec, expert_spec, expert_spec)
    out_specs = (token_spec, cache_spec, cache_spec)
    return jax.shard_map(local_step, mesh=mesh, in_specs=in_specs, out_specs=out_specs, check_vma=False)
```

```python
import functools

import jax
import jax.numpy as jnp
import numpy as np
from jax import lax
from jax.experimental import pallas as pl
from jax.experimental.pallas import tpu as pltpu
from jax.sharding import PartitionSpec as P

NORM_EPS = 1e-6
ROPE_BASE = 10000.0
F32 = jnp.float32
BF16 = jnp.bfloat16
NEG = -1e30
MESH = pl.DeviceIdType.MESH
VMEM_LIMIT = 62 * 1024 * 1024

TOKENS = 512
HIDDEN = 2048
HEADS = 4
HEAD_DIM = 128
SLOTS = 32
QUERY_COLS = HEADS * HEAD_DIM
EXPERTS = 8
FFN = 5632
LOCAL = 2

BLOCK = 32
RING = 8
BLOCKS = TOKENS // BLOCK
GROUP = 8
WQ_RING = 3

COL = 256
ROWS = 256
STEPS = HIDDEN // COL
CHUNKS = STEPS // 2 * (TOKENS // ROWS)

FT = 512
F_TILES = FFN // FT
MLP_STEPS = LOCAL * F_TILES
W_RING = 5
RB = 128


def dot(a, b):
    return jnp.dot(a, b, preferred_element_type=F32)


def iota(shape, dim):
    return lax.broadcasted_iota(jnp.int32, shape, dim)


def norm_rows(x_ref, gain_ref, out_ref):
    def body(i, carry):
        rows = pl.ds(pl.multiple_of(i * 32, 32), 32)
        values = x_ref[rows, :].astype(F32)
        inv = lax.rsqrt(jnp.mean(values * values, axis=-1, keepdims=True) + NORM_EPS)
        out_ref[rows, :] = (values * inv * gain_ref[...]).astype(BF16)
        return carry
    lax.fori_loop(0, TOKENS // 32, body, 0)


def pair_gates(logits, id0, id1):
    lane = iota(logits.shape, 1)
    first = jnp.sum(jnp.where(lane == id0, logits, 0.0), axis=1, keepdims=True)
    second = jnp.sum(jnp.where(lane == id1, logits, 0.0), axis=1, keepdims=True)
    top = jnp.maximum(first, second)
    e0 = jnp.exp(first - top)
    e1 = jnp.exp(second - top)
    total = e0 + e1
    return e0 / total, e1 / total


def turn(rows):
    sub = iota((8, TOKENS), 0)
    stacked = jnp.zeros((8, TOKENS), F32)
    for i, row in enumerate(rows):
        stacked = jnp.where(sub == i, row.astype(F32), stacked)
    return jnp.transpose(stacked).astype(jnp.int32)


def dot_nt(a, b):
    return lax.dot_general(a, b, (((1,), (1,)), ((), ())), preferred_element_type=F32)


def attend_kernel(pos_ref, x_ref, gain_ref, table_ref, posrow_ref, idst_ref, router_ref, wkv_hbm, wq_hbm, kc_hbm, vc_hbm,
                  ko_hbm, vo_hbm, o_ref, gates_ref, ids_ref,
                  hid, wraw, wtmp, wkv, wq, kbuf, vbuf, qsel, qrow, qdiag, knv, probs, orow, cos_s, sin_s,
                  wkv_sem, wq_sem, kin_sem, vin_sem, kout_sem, vout_sem):
    def block_of(ref, b):
        return ref.at[pl.ds(pl.multiple_of(b * BLOCK, BLOCK), BLOCK)]

    def load(b):
        slot = lax.rem(b, RING)
        return (pltpu.make_async_copy(block_of(kc_hbm, b), kbuf.at[slot], kin_sem.at[slot]),
                pltpu.make_async_copy(block_of(vc_hbm, b), vbuf.at[slot], vin_sem.at[slot]))

    def save(b):
        slot = lax.rem(b, RING)
        return (pltpu.make_async_copy(kbuf.at[slot], block_of(ko_hbm, b), kout_sem.at[slot]),
                pltpu.make_async_copy(vbuf.at[slot], block_of(vo_hbm, b), vout_sem.at[slot]))

    def load_wq(e):
        slot = lax.rem(e, WQ_RING)
        return pltpu.make_async_copy(wq_hbm.at[e], wq.at[slot], wq_sem.at[slot])

    kv_copy = pltpu.make_async_copy(wkv_hbm, wraw, wkv_sem)
    kv_copy.start()
    for b in range(3):
        for copy in load(jnp.int32(b)):
            copy.start()
    load_wq(jnp.int32(0)).start()

    norm_rows(x_ref, gain_ref, hid)
    for e in range(1, WQ_RING):
        load_wq(jnp.int32(e)).start()
    ids = turn((idst_ref[0:1, :], idst_ref[1:2, :], posrow_ref[...]))
    ids_ref[...] = ids
    id0 = ids[:, 0:1]
    id1 = ids[:, 1:2]
    lane128 = iota((TOKENS, 128), 1)
    chosen = ((lane128 & 31) == ids[:, 2:3]) & (lane128 < 3 * SLOTS)
    trig = dot(jnp.where(chosen, 1.0, 0.0).astype(BF16), table_ref[...])
    cos_s[...] = trig[:, :HEAD_DIM]
    sin_s[...] = trig[:, HEAD_DIM:]
    logits = dot_nt(hid[...], router_ref[...])
    g0, g1 = pair_gates(logits, id0, id1)
    lane8 = iota((TOKENS, EXPERTS), 1)
    gates_ref[...] = jnp.where(lane8 == id0, g0, 0.0) + jnp.where(lane8 == id1, g1, 0.0)
    kv_copy.wait()

    def sort_body(i, carry):
        wtmp[...] = wraw[pl.ds(pl.multiple_of(i * 1024, 1024), 1024), :].astype(F32)
        rows = pl.ds(pl.multiple_of(i * 128, 128), 128)
        for j in range(8):
            wkv[rows, j * 128:(j + 1) * 128] = wtmp[pl.ds(j, 128, stride=8), :].astype(BF16)
        return carry
    lax.fori_loop(0, HIDDEN // 128, sort_body, 0)

    keys_new = dot(hid[...], wkv[:, :QUERY_COLS])
    for h in range(HEADS):
        k = keys_new[:, h * 128:(h + 1) * 128]
        knv[pl.ds(h, TOKENS, stride=8), :] = k * cos_s[...] + pltpu.roll(k, 64, 1) * sin_s[...]
    values_new = dot(hid[...], wkv[:, QUERY_COLS:])
    for h in range(HEADS):
        knv[pl.ds(h + 4, TOKENS, stride=8), :] = values_new[:, h * 128:(h + 1) * 128]

    def q_body(e, carry):
        @pl.when(e + 3 < RING)
        def _():
            for copy in load(e + 3):
                copy.start()
        load_wq(e).wait()
        slot = lax.rem(e, WQ_RING)

        q = dot(hid[...], wq[slot])
        for k in range(2):
            qsel[k] = jnp.where(ids_ref[:, k:k + 1] == e, q, qsel[k])

        @pl.when(e + WQ_RING < EXPERTS)
        def _():
            load_wq(e + WQ_RING).start()
        return carry
    lax.fori_loop(0, EXPERTS, q_body, 0)

    def rope_body(m, carry):
        rows = pl.ds(pl.multiple_of(m * 128, 128), 128)
        cos = cos_s[rows, :]
        sin = sin_s[rows, :]
        for k in range(2):
            for h in range(HEADS):
                q = qsel[k, rows, h * 128:(h + 1) * 128]
                qrow[pl.ds(k * HEADS + h, 128, stride=8), :] = q * cos + pltpu.roll(q, 64, 1) * sin
        q = qrow[...]
        even = (iota((1024, HEAD_DIM), 0) & 8) == 0
        lines = pl.ds(pl.multiple_of(m * 1024, 1024), 1024)
        qdiag[lines, :HEAD_DIM] = jnp.where(even, q, 0.0).astype(BF16)
        qdiag[lines, HEAD_DIM:] = jnp.where(even, 0.0, q).astype(BF16)
        return carry
    lax.fori_loop(0, TOKENS // 128, rope_body, 0)

    scale = HEAD_DIM ** -0.5
    sub16 = iota((16, HEAD_DIM), 0) >> 2
    low = iota((8, 128), 0) < 4
    row16 = iota((16, 128), 0)
    lane = iota((16, 128), 1)
    upper = row16 < 8
    same_head = (lane & 3) == (row16 & 3)
    slot_of = lane >> 2

    def block_body(i, carry):
        b = jnp.minimum(i, BLOCKS - 1)
        prev = jnp.maximum(i - 1, 0)
        slot = lax.rem(b, RING)
        prev_slot = lax.rem(prev, RING)
        side = lax.rem(i, 2)

        @pl.when(i < BLOCKS)
        def _():
            for copy in load(b):
                copy.wait()
        places = [pos_ref[b * BLOCK + t] for t in range(BLOCK)]

        def patch(t):
            rows = pl.ds(pl.multiple_of((places[t] >> 2) * 16, 16), 16)
            put = sub16 == (places[t] & 3)
            both = knv[pl.ds(pl.multiple_of((b * BLOCK + t) * 8, 8), 8), :]
            swapped = pltpu.roll(both, 4, 0)
            for n8, buf in ((jnp.where(low, both, swapped), kbuf), (jnp.where(low, swapped, both), vbuf)):
                n16 = jnp.concatenate([n8, n8], axis=0)
                old = buf[slot, t, rows, :].astype(F32)
                buf[slot, t, rows, :] = jnp.where(put, n16, old).astype(BF16)

        def score(j):
            t = b * BLOCK + 2 * j
            q = qdiag[pl.ds(pl.multiple_of(t * 8, 16), 16), :]
            keys = jnp.concatenate([kbuf[slot, 2 * j], kbuf[slot, 2 * j + 1]], axis=1)
            s = dot_nt(q, keys) * scale
            s = jnp.where(same_head & (slot_of <= jnp.where(upper, places[2 * j], places[2 * j + 1])), s, NEG)
            e = jnp.exp(s - jnp.max(s, axis=1, keepdims=True))
            probs[side, j] = (e / jnp.sum(e, axis=1, keepdims=True)).astype(BF16)

        def mix(j):
            values = jnp.concatenate([vbuf[prev_slot, 2 * j], vbuf[prev_slot, 2 * j + 1]], axis=1)
            o = dot(probs[1 - side, j], values)
            orow[j * 16:j * 16 + 8, :] = o[:8, :HEAD_DIM]
            orow[j * 16 + 8:j * 16 + 16, :] = o[8:, HEAD_DIM:]

        half = BLOCK // 2
        pairs = BLOCK // 2
        first, second = range(pairs // 2), range(pairs // 2, pairs)
        for t in range(half):
            patch(t)
        for j in first:
            score(j)
        for t in range(half, BLOCK):
            patch(t)
        for j in first:
            mix(j)
        for j in second:
            score(j)
        for j in second:
            mix(j)
        rows = pl.ds(pl.multiple_of(prev * BLOCK, BLOCK), BLOCK)
        for r in range(8):
            o_ref[rows, r * 128:(r + 1) * 128] = orow[pl.ds(r, BLOCK, stride=8), :].astype(BF16)

        @pl.when(i >= 1)
        def _():
            for copy in save(prev):
                copy.start()

        @pl.when(i >= 3)
        def _():
            for copy in save(i - 3):
                copy.wait()

            @pl.when(i - 3 + RING < BLOCKS)
            def _():
                for copy in load(i - 3 + RING):
                    copy.start()
        return carry
    lax.fori_loop(0, BLOCKS + 1, block_body, 0)
    for b in (BLOCKS - 2, BLOCKS - 1):
        for copy in save(jnp.int32(b)):
            copy.wait()


def attend(positions, x, gain, table, pos_row, ids_t, router_t, w_kv, w_query, k_cache, v_cache):
    any_spec = pl.BlockSpec(memory_space=pl.ANY)
    vmem = pl.BlockSpec(memory_space=pltpu.VMEM)
    smem = pl.BlockSpec(memory_space=pltpu.SMEM)
    cache = jax.ShapeDtypeStruct(k_cache.shape, BF16)
    return pl.pallas_call(
        attend_kernel,
        name='attend',
        out_shape=(cache, cache, jax.ShapeDtypeStruct((TOKENS, 2 * QUERY_COLS), BF16),
                   jax.ShapeDtypeStruct((TOKENS, EXPERTS), F32), jax.ShapeDtypeStruct((TOKENS, EXPERTS), jnp.int32)),
        in_specs=[smem] + [vmem] * 6 + [any_spec] * 4,
        out_specs=(any_spec, any_spec, vmem, vmem, vmem),
        scratch_shapes=[
            pltpu.VMEM((TOKENS, HIDDEN), BF16),
            pltpu.VMEM((HIDDEN * 8, 128), BF16),
            pltpu.VMEM((1024, 128), F32),
            pltpu.VMEM((HIDDEN, HEADS * 256), BF16),
            pltpu.VMEM((WQ_RING, HIDDEN, QUERY_COLS), BF16),
            pltpu.VMEM((RING, BLOCK, SLOTS * HEADS, HEAD_DIM), BF16),
            pltpu.VMEM((RING, BLOCK, SLOTS * HEADS, HEAD_DIM), BF16),
            pltpu.VMEM((2, TOKENS, QUERY_COLS), F32),
            pltpu.VMEM((1024, HEAD_DIM), F32),
            pltpu.VMEM((TOKENS * 8, 2 * HEAD_DIM), BF16),
            pltpu.VMEM((TOKENS * 8, HEAD_DIM), F32),
            pltpu.VMEM((2, BLOCK // 2, 16, HEAD_DIM), BF16),
            pltpu.VMEM((BLOCK * 8, HEAD_DIM), F32),
            pltpu.VMEM((TOKENS, HEAD_DIM), F32),
            pltpu.VMEM((TOKENS, HEAD_DIM), F32),
            pltpu.SemaphoreType.DMA,
            pltpu.SemaphoreType.DMA((WQ_RING,)),
            pltpu.SemaphoreType.DMA((RING,)),
            pltpu.SemaphoreType.DMA((RING,)),
            pltpu.SemaphoreType.DMA((RING,)),
            pltpu.SemaphoreType.DMA((RING,)),
        ],
        compiler_params=pltpu.CompilerParams(vmem_limit_bytes=VMEM_LIMIT),
    )(positions, x, gain, table, pos_row, ids_t, router_t, w_kv, w_query, k_cache, v_cache)


def reduce_columns(drive, partial, base_hbm, out_ref, base_ref, base_sem, send1, recv1, own, recv2, fin, recv3, s1, r1, s2, r2, s3, r3):
    chunks, height, width = send1.shape
    per = TOKENS // height
    half_width = HIDDEN // 2
    me = lax.axis_index('tp')
    core = lax.rem(me, 2)
    sibling = me + 1 - 2 * core
    partner = lax.rem(me + 2, 4)
    barrier = pltpu.get_barrier_semaphore()
    for peer in (sibling, partner):
        pl.semaphore_signal(barrier, inc=1, device_id={'tp': peer}, device_id_type=MESH)
    pl.semaphore_wait(barrier, 2)

    def column(s):
        half = lax.rem(core + 1 + s, 2)
        return pl.multiple_of(half * half_width + lax.div(s, 2) * width, width)

    def remote(src, dst, c, send, recv, peer):
        return pltpu.make_async_remote_copy(src_ref=src.at[c], dst_ref=dst.at[c], send_sem=send.at[c], recv_sem=recv.at[c],
                                            device_id={'tp': peer}, device_id_type=MESH)

    def to_sibling(c):
        return remote(send1, recv1, c, s1, r1, sibling)

    def to_partner(c):
        return remote(own, recv2, c, s2, r2, partner)

    def share(c):
        return remote(fin, recv3, c, s3, r3, sibling)

    def chunk_step(i, parity, m):
        s = 2 * i + parity
        rows = pl.ds(pl.multiple_of(m * height, height), height)
        chunk = per * i + m
        acc = partial(s, rows, column(s))
        if parity == 0:
            send1[chunk] = acc.astype(BF16)
            to_sibling(chunk).start()
        else:
            to_sibling(chunk).wait_recv()
            own[chunk] = (acc + recv1[chunk].astype(F32)).astype(BF16)
            to_partner(chunk).start()

    def place(c, half):
        rows = pl.ds(pl.multiple_of(lax.rem(c, per) * height, height), height)
        cols = pl.ds(pl.multiple_of(half * half_width + lax.div(c, per) * width, width), width)
        return rows, cols

    def finish(c):
        to_partner(c).wait_recv()
        rows, cols = place(c, core)
        total = own[c].astype(F32) + recv2[c].astype(F32)
        value = (base_ref[rows, cols].astype(F32) + total).astype(BF16)
        fin[c] = value
        share(c).start()
        out_ref[rows, cols] = value

    base_copy = pltpu.make_async_copy(base_hbm, base_ref, base_sem)
    finished = drive(chunk_step, column, finish, base_copy)

    def final_body(c, carry):
        finish(c)
        return carry
    lax.fori_loop(finished, chunks, final_body, 0)

    def gather_body(c, carry):
        share(c).wait_recv()
        rows, cols = place(c, 1 - core)
        out_ref[rows, cols] = recv3[c]
        return carry
    lax.fori_loop(0, chunks, gather_body, 0)

    def drain_body(c, carry):
        to_sibling(c).wait_send()
        to_partner(c).wait_send()
        share(c).wait_send()
        return carry
    lax.fori_loop(0, chunks, drain_body, 0)


def chunk_scratch(height, width):
    chunks = TOKENS * HIDDEN // 2 // (height * width)
    return ([pltpu.VMEM((TOKENS, HIDDEN), BF16), pltpu.SemaphoreType.DMA]
            + [pltpu.VMEM((chunks, height, width), BF16)] * 6 + [pltpu.SemaphoreType.DMA((chunks,))] * 6)


OUT_RING = 4


def out_kernel(o_ref, ids_ref, gates_ref, w_hbm, x_hbm, out_ref, spread, wbuf, w_sem, *chunk_refs):
    core = lax.rem(lax.axis_index('tp'), 2)

    def load_w(s):
        half = lax.rem(core + 1 + s, 2)
        cols = pl.ds(pl.multiple_of((half * (STEPS // 2) + lax.div(s, 2)) * COL, COL), COL)
        slot = lax.rem(s, OUT_RING)
        return pltpu.make_async_copy(w_hbm.at[:, :, cols], wbuf.at[slot], w_sem.at[slot])

    for s in range(OUT_RING):
        load_w(jnp.int32(s)).start()

    def spread_rows(m):
        def spread_body(n, carry):
            rows = pl.ds(pl.multiple_of(m * ROWS + n * 64, 64), 64)
            first = o_ref[rows, :QUERY_COLS].astype(F32)
            second = o_ref[rows, QUERY_COLS:].astype(F32)
            for e in range(EXPERTS):
                picked = jnp.where(ids_ref[rows, 0:1] == e, first, 0.0)
                picked = jnp.where(ids_ref[rows, 1:2] == e, second, picked)
                spread[e, rows, :] = picked.astype(BF16)
            return carry
        lax.fori_loop(0, ROWS // 64, spread_body, 0)

    def partial(s, rows, col):
        slot = lax.rem(s, OUT_RING)
        acc = jnp.zeros((ROWS, COL), F32)
        for e in range(EXPERTS):
            acc = acc + gates_ref[rows, e:e + 1] * dot(spread[e, rows, :], wbuf[slot, e])
        return acc

    def drive(chunk_step, column, finish, base_copy):
        def col_body(i, carry):
            for parity in range(2):
                load_w(2 * i + parity).wait()

            def row_body(m, c):
                @pl.when(i == 0)
                def _():
                    spread_rows(m)
                for parity in range(2):
                    chunk_step(i, parity, m)
                return c
            lax.fori_loop(0, TOKENS // ROWS, row_body, 0)

            @pl.when(2 * i + OUT_RING < STEPS)
            def _():
                for parity in range(2):
                    load_w(2 * i + OUT_RING + parity).start()

            @pl.when(i == 0)
            def _():
                base_copy.start()

            @pl.when(i == 1)
            def _():
                base_copy.wait()

            @pl.when(i >= 2)
            def _():
                finish(2 * (i - 2))
                finish(2 * (i - 2) + 1)
            return carry
        lax.fori_loop(0, STEPS // 2, col_body, 0)
        return CHUNKS // 2

    reduce_columns(drive, partial, x_hbm, out_ref, *chunk_refs)


def out_project(o, ids, gates, w_out, x):
    vmem = pl.BlockSpec(memory_space=pltpu.VMEM)
    return pl.pallas_call(
        out_kernel,
        name='out_project',
        out_shape=jax.ShapeDtypeStruct((TOKENS, HIDDEN), BF16),
        in_specs=[vmem] * 3 + [pl.BlockSpec(memory_space=pl.ANY)] * 2,
        out_specs=vmem,
        scratch_shapes=[
            pltpu.VMEM((EXPERTS, TOKENS, QUERY_COLS), BF16),
            pltpu.VMEM((OUT_RING, EXPERTS, QUERY_COLS, COL), BF16),
            pltpu.SemaphoreType.DMA((OUT_RING,)),
        ] + chunk_scratch(ROWS, COL),
        compiler_params=pltpu.CompilerParams(vmem_limit_bytes=VMEM_LIMIT, collective_id=0, has_side_effects=True),
    )(o, ids, gates, w_out, x)


def gate_up_kernel(x_ref, gain_ref, router_ref, idst_ref, wg_hbm, wu_hbm, wd_hbm, a_hbm, gates_ref, early_ref,
                   unorm, picked, scatter, gathered, wg, wu, wd, act, abuf, early_rows, wg_sem, wu_sem, wd_sem, a_sem):
    first_id = lax.axis_index('tp') * LOCAL
    core = lax.rem(lax.axis_index('tp'), 2)

    def load(s):
        e = lax.div(s, F_TILES)
        cols = pl.ds(pl.multiple_of(lax.rem(s, F_TILES) * FT, FT), FT)
        slot = lax.rem(s, W_RING)
        return (pltpu.make_async_copy(wg_hbm.at[e, :, cols], wg.at[slot], wg_sem.at[slot]),
                pltpu.make_async_copy(wu_hbm.at[e, :, cols], wu.at[slot], wu_sem.at[slot]),
                down_of(e, cols, slot, 0), down_of(e, cols, slot, 1))

    def down_of(e, rows, slot, j):
        half = lax.rem(core + 1 + j, 2)
        cols = pl.ds(pl.multiple_of(half * (HIDDEN // 2), HIDDEN // 2), COL)
        return pltpu.make_async_copy(wd_hbm.at[e, rows, cols], wd.at[slot, j], wd_sem.at[slot, j])

    def save(s):
        e = lax.div(s, F_TILES)
        cols = pl.ds(pl.multiple_of(lax.rem(s, F_TILES) * FT, FT), FT)
        slot = lax.rem(s, 2)
        return pltpu.make_async_copy(abuf.at[slot], a_hbm.at[e, :, cols], a_sem.at[slot])

    for s in range(W_RING):
        for copy in load(jnp.int32(s)):
            copy.start()

    norm_rows(x_ref, gain_ref, unorm)
    ids = turn((idst_ref[0:1, :], idst_ref[1:2, :]))
    id0 = ids[:, 0:1]
    id1 = ids[:, 1:2]
    logits = dot_nt(unorm[...], router_ref[...])
    g0, g1 = pair_gates(logits, id0, id1)
    lane8 = iota((TOKENS, EXPERTS), 1)
    local8 = lane8 + first_id
    gates_ref[...] = jnp.where(local8 == id0, g0, 0.0) + jnp.where(local8 == id1, g1, 0.0)

    before = iota((TOKENS, TOKENS), 0)
    after = iota((TOKENS, TOKENS), 1)
    lower = jnp.where(after < before, 1.0, 0.0).astype(BF16)
    upper = jnp.where(before < after, 1.0, 0.0).astype(BF16)
    lane_id = iota((TOKENS, 128), 1) + first_id
    mask_col = jnp.where((lane_id == id0) | (lane_id == id1), 1.0, 0.0)
    rank_col = dot(lower, mask_col.astype(BF16))
    sub_id = iota((8, TOKENS), 0) + first_id
    mask_row = jnp.where((sub_id == idst_ref[0:1, :]) | (sub_id == idst_ref[1:2, :]), 1.0, 0.0)
    rank_row = dot(mask_row.astype(BF16), upper)
    counts = []
    for e in range(LOCAL):
        counts.append(jnp.sum(mask_row[e:e + 1, :]).astype(jnp.int32))
        where_col = jnp.where(mask_col[:, e:e + 1] > 0.0, rank_col[:, e:e + 1], -1.0)
        where_row = jnp.where(mask_row[e:e + 1, :] > 0.0, rank_row[e:e + 1, :], -1.0)
        scatter[e] = jnp.where(after.astype(F32) == where_col, 1.0, 0.0).astype(BF16)
        picked[e] = jnp.where(before.astype(F32) == where_row, 1.0, 0.0).astype(BF16)
    blocks = [lax.div(n + (RB - 1), RB) for n in counts]

    for e in range(LOCAL):
        def gather_body(rb, carry):
            rows = pl.ds(pl.multiple_of(rb * RB, RB), RB)
            gathered[e, rows, :] = dot(picked[e, rows, :], unorm[...]).astype(BF16)
            return carry
        lax.fori_loop(0, blocks[e], gather_body, 0)

    early_rows[...] = jnp.zeros_like(early_rows)

    def step_body(s, carry):
        e = lax.div(s, F_TILES)
        slot = lax.rem(s, W_RING)
        out_slot = lax.rem(s, 2)
        for copy in load(s):
            copy.wait()

        @pl.when(s >= 2)
        def _():
            save(s - 2).wait()

        def run(count):
            for n in range(FT // COL):
                cols = slice(n * COL, (n + 1) * COL)
                gate = dot(gathered[e, :count, :], wg[slot, :, cols])
                up = dot(gathered[e, :count, :], wu[slot, :, cols])
                act[:count, cols] = (gate * (1.0 / (1.0 + jnp.exp(-gate))) * up).astype(BF16)
            for j in range(2):
                cols = slice(j * COL, (j + 1) * COL)
                early_rows[e, :count, cols] += dot(act[:count, :], wd[slot, j])
            for m in range(TOKENS // ROWS):
                rows = slice(m * ROWS, (m + 1) * ROWS)
                abuf[out_slot, rows, :] = dot(scatter[e, rows, :count], act[:count, :]).astype(BF16)

        n_rows = jnp.where(e == 0, counts[0], counts[1])
        n_steps = jnp.maximum(lax.div(n_rows + 63, 64), 2)
        for k in range(2, TOKENS // 64 + 1):
            pl.when(n_steps == k)(functools.partial(run, k * 64))

        @pl.when(s + W_RING < MLP_STEPS)
        def _():
            for copy in load(s + W_RING):
                copy.start()
        save(s).start()
        return carry
    lax.fori_loop(0, MLP_STEPS, step_body, 0)

    def early_body(m, carry):
        rows = pl.ds(pl.multiple_of(m * ROWS, ROWS), ROWS)
        for j in range(2):
            total = jnp.zeros((ROWS, COL), F32)
            for e in range(LOCAL):
                z = early_rows[e, :, j * COL:(j + 1) * COL]
                high = z.astype(BF16)
                rest = (z - high.astype(F32)).astype(BF16)
                mine = dot(scatter[e, rows, :], high) + dot(scatter[e, rows, :], rest)
                total = total + gates_ref[rows, e:e + 1] * mine
            early_ref[j, rows, :] = total
        return carry
    lax.fori_loop(0, TOKENS // ROWS, early_body, 0)
    for s in (MLP_STEPS - 2, MLP_STEPS - 1):
        save(jnp.int32(s)).wait()


def gate_up(x_mid, gain, router_t, ids_t, w_gate, w_up, w_down):
    any_spec = pl.BlockSpec(memory_space=pl.ANY)
    vmem = pl.BlockSpec(memory_space=pltpu.VMEM)
    return pl.pallas_call(
        gate_up_kernel,
        name='gate_up',
        out_shape=(jax.ShapeDtypeStruct((LOCAL, TOKENS, FFN), BF16), jax.ShapeDtypeStruct((TOKENS, EXPERTS), F32),
                   jax.ShapeDtypeStruct((2, TOKENS, COL), F32)),
        in_specs=[vmem] * 4 + [any_spec] * 3,
        out_specs=(any_spec, vmem, vmem),
        scratch_shapes=[
            pltpu.VMEM((TOKENS, HIDDEN), BF16),
            pltpu.VMEM((LOCAL, TOKENS, TOKENS), BF16),
            pltpu.VMEM((LOCAL, TOKENS, TOKENS), BF16),
            pltpu.VMEM((LOCAL, TOKENS, HIDDEN), BF16),
            pltpu.VMEM((W_RING, HIDDEN, FT), BF16),
            pltpu.VMEM((W_RING, HIDDEN, FT), BF16),
            pltpu.VMEM((W_RING, 2, FT, COL), BF16),
            pltpu.VMEM((TOKENS, FT), BF16),
            pltpu.VMEM((2, TOKENS, FT), BF16),
            pltpu.VMEM((LOCAL, TOKENS, 2 * COL), F32),
            pltpu.SemaphoreType.DMA((W_RING,)),
            pltpu.SemaphoreType.DMA((W_RING,)),
            pltpu.SemaphoreType.DMA((W_RING, 2)),
            pltpu.SemaphoreType.DMA((2,)),
        ],
        compiler_params=pltpu.CompilerParams(vmem_limit_bytes=VMEM_LIMIT),
    )(x_mid, gain, router_t, ids_t, w_gate, w_up, w_down)


DOWN_RING = 2


def down_kernel(gates_ref, early_ref, x_hbm, a_hbm, w_hbm, out_ref, abuf, wbuf, first_part, a_sem, w_sem, *chunk_refs):
    me = lax.axis_index('tp')
    core = lax.rem(me, 2)

    def copy_of(s, col, e):
        slot = lax.rem(s, DOWN_RING)
        return pltpu.make_async_copy(w_hbm.at[e, :, pl.ds(col, COL)], wbuf.at[slot, e], w_sem.at[slot, e])

    def ahead(s, e):
        half = lax.rem(core + 1 + s, 2)
        return copy_of(jnp.int32(s), pl.multiple_of((half * (STEPS // 2) + s // 2) * COL, COL), e)

    a_copies = [pltpu.make_async_copy(a_hbm.at[e], abuf.at[e], a_sem.at[e]) for e in range(LOCAL)]
    for e in range(LOCAL):
        a_copies[e].start()
        ahead(2, e).start()

    def partial(s, rows, col):
        if isinstance(s, int):
            return early_ref[s, rows, :]
        return first_part[rows, :] + gates_ref[rows, 1:2] * dot(abuf[1, rows, :], wbuf[lax.rem(s, DOWN_RING), 1])

    def drive(chunk_step, column, finish, base_copy):
        for m in range(TOKENS // ROWS):
            for parity in range(2):
                chunk_step(0, parity, m)
        a_copies[0].wait()
        for e in range(LOCAL):
            ahead(3, e).start()
        base_copy.start()

        def col_body(i, carry):
            for parity in range(2):
                s = 2 * i + parity
                slot = lax.rem(s, DOWN_RING)
                copy_of(s, column(s), 0).wait()
                first_part[...] = gates_ref[:, 0:1] * dot(abuf[0], wbuf[slot, 0])
                if parity == 0:
                    @pl.when(i == 1)
                    def _():
                        a_copies[1].wait()
                copy_of(s, column(s), 1).wait()

                def row_body(m, c):
                    chunk_step(i, parity, m)
                    return c
                lax.fori_loop(0, TOKENS // ROWS, row_body, 0)

                @pl.when(s + DOWN_RING < STEPS)
                def _():
                    for e in range(LOCAL):
                        copy_of(s + DOWN_RING, column(s + DOWN_RING), e).start()

            @pl.when(i == 1)
            def _():
                base_copy.wait()

            @pl.when(i >= 2)
            def _():
                finish(2 * (i - 2))
                finish(2 * (i - 2) + 1)
            return carry
        lax.fori_loop(1, STEPS // 2, col_body, 0)
        return CHUNKS // 2

    reduce_columns(drive, partial, x_hbm, out_ref, *chunk_refs)


def down_project(gates, early, x_mid, act, w_down):
    vmem = pl.BlockSpec(memory_space=pltpu.VMEM)
    any_spec = pl.BlockSpec(memory_space=pl.ANY)
    return pl.pallas_call(
        down_kernel,
        name='down_project',
        out_shape=jax.ShapeDtypeStruct((TOKENS, HIDDEN), BF16),
        in_specs=[vmem] * 2 + [any_spec] * 3,
        out_specs=vmem,
        scratch_shapes=[
            pltpu.VMEM((LOCAL, TOKENS, FFN), BF16),
            pltpu.VMEM((DOWN_RING, LOCAL, FFN, COL), BF16),
            pltpu.VMEM((TOKENS, COL), F32),
            pltpu.SemaphoreType.DMA((LOCAL,)),
            pltpu.SemaphoreType.DMA((DOWN_RING, LOCAL)),
        ] + chunk_scratch(ROWS, COL),
        compiler_params=pltpu.CompilerParams(vmem_limit_bytes=VMEM_LIMIT, collective_id=1, has_side_effects=True),
    )(gates, early, x_mid, act, w_down)


PIECES = 8


def hand_over_kernel(x_hbm, out_hbm, buf, in_sem, out_sem):
    def rows(i):
        return pl.ds(i * (TOKENS // PIECES), TOKENS // PIECES)
    reads = [pltpu.make_async_copy(x_hbm.at[rows(i)], buf.at[i], in_sem.at[i]) for i in range(PIECES)]
    writes = [pltpu.make_async_copy(buf.at[i], out_hbm.at[rows(i)], out_sem.at[i]) for i in range(PIECES)]
    for copy in reads:
        copy.start()
    for read, write in zip(reads, writes):
        read.wait()
        write.start()
    for copy in writes:
        copy.wait()


def hand_over(x):
    any_spec = pl.BlockSpec(memory_space=pl.ANY)
    return pl.pallas_call(
        hand_over_kernel,
        name='hand_over',
        out_shape=jax.ShapeDtypeStruct(x.shape, x.dtype),
        in_specs=[any_spec],
        out_specs=any_spec,
        scratch_shapes=[pltpu.VMEM((PIECES, TOKENS // PIECES, HIDDEN), BF16), pltpu.SemaphoreType.DMA((PIECES,)), pltpu.SemaphoreType.DMA((PIECES,))],
        compiler_params=pltpu.CompilerParams(vmem_limit_bytes=VMEM_LIMIT),
    )(x)


def rope_table():
    half = HEAD_DIM // 2
    inv_freq = np.float32(ROPE_BASE) ** (-(np.arange(half, dtype=np.float32) * np.float32(2.0) / np.float32(HEAD_DIM)))
    angles = np.arange(SLOTS, dtype=np.float32)[:, None] * inv_freq[None, :].astype(np.float32)
    cos = np.cos(angles.astype(np.float64))
    sin = np.sin(angles.astype(np.float64))
    full = np.concatenate([cos, cos, -sin, sin], axis=1).astype(np.float32)
    parts = []
    for _ in range(3):
        part = full.astype(BF16)
        parts.append(part)
        full = full - part.astype(np.float32)
    parts.append(np.zeros_like(parts[0]))
    return np.concatenate(parts, axis=0)


def solution(mesh):
    table = rope_table()

    def local_step(x, k_cache, v_cache, positions, att_ids, mlp_ids, norm_att, w_kv, router_att, w_query, w_out, norm_mlp, router_mlp, w_gate, w_up, w_down):
        flat = (TOKENS, SLOTS * HEADS, HEAD_DIM)
        kv_rows = w_kv.reshape(HIDDEN, HEADS, 2, HEAD_DIM).transpose(0, 2, 1, 3).reshape(HIDDEN * 8, HEAD_DIM)
        k_new, v_new, o, att_gates, att_cols = attend(
            positions, x, norm_att.reshape(1, HIDDEN), jnp.asarray(table), positions.reshape(1, TOKENS), att_ids.T, router_att.T,
            kv_rows, w_query, k_cache.reshape(flat), v_cache.reshape(flat))
        x_mid = out_project(o, att_cols, att_gates, w_out, x)
        act, mlp_gates, early = gate_up(x_mid, norm_mlp.reshape(1, HIDDEN), router_mlp.T, mlp_ids.T, w_gate, w_up, w_down)
        x_out = hand_over(down_project(mlp_gates, early, x_mid, act, w_down))
        return x_out, k_new.reshape(k_cache.shape), v_new.reshape(v_cache.shape)

    token_spec = P('dp', None)
    cache_spec = P('dp', None, 'tp', None)
    expert_spec = P('tp', None, None)
    in_specs = (token_spec, cache_spec, cache_spec, P('dp'), token_spec, token_spec, P(), P(None, 'tp', None), P(), P(None, None, 'tp'), P(None, 'tp', None), P(), P(), expert_spec, expert_spec, expert_spec)
    out_specs = (token_spec, cache_spec, cache_spec)
    return jax.shard_map(local_step, mesh=mesh, in_specs=in_specs, out_specs=out_specs, check_vma=False)
```
